8 devices in a mesh: dp: 1 (over z), tp: 8 (over y, x, core).
Axes of the slice: x: 2, y: 2, z: 1, core: 2. Of those that a mesh axis runs over, the one named last changes fastest.
Arguments:
- tokens: int32 [1, 2048], P('dp')
- embed_table: bfloat16 [102400, 2048], P('tp')
- w_q: bfloat16 [2048, 16, 192], P(None, 'tp')
- w_dkv: bfloat16 [2048, 576], replicated
- g_kv: float32 [512], replicated
- w_uk: bfloat16 [512, 16, 128], P(None, 'tp')
- w_uv: bfloat16 [512, 16, 128], P(None, 'tp')
- w_o: bfloat16 [16, 128, 2048], P('tp')
- g_attn: float32 [2048], replicated
- g_mlp: float32 [2048], replicated
- w_gate: bfloat16 [2048, 10944], P(None, 'tp')
- w_up: bfloat16 [2048, 10944], P(None, 'tp')
- w_down: bfloat16 [10944, 2048], P('tp')
- d_out: bfloat16 [1, 2048, 2048], P('dp', 'tp')
Outputs:
- output 1: bfloat16 [1, 2048, 2048], P('dp', 'tp')
- output 2: bfloat16 [102400, 2048], P(('dp', 'tp'))
- output 3: float32 [2048, 16, 192], P('dp', 'tp')
- output 4: float32 [2048, 576], P('dp')
- output 5: float32 [512], P('dp')
- output 6: float32 [512, 16, 128], P('dp', 'tp')
- output 7: float32 [512, 16, 128], P('dp', 'tp')
- output 8: float32 [16, 128, 2048], P(('dp', 'tp'))
- output 9: float32 [2048], P('dp')
- output 10: float32 [2048], P('dp')
- output 11: float32 [2048, 10944], P('dp', 'tp')
- output 12: float32 [2048, 10944], P('dp', 'tp')
- output 13: float32 [10944, 2048], P(('dp', 'tp'))
All inputs are finite; a program needn't handle non-finite values.
Results may differ from the reference program's by a relative error of at most 0.02.
Values are sent between devices in bfloat16 or wider.
A program may use at most 1 GiB of HBM per device.

```python
import jax
import jax.numpy as jnp
import numpy as np
from jax import lax

VOCAB_SIZE = 102400
MODEL_DIM = 2048
NUM_HEADS = 16
NOPE_DIM = 128
ROPE_DIM = 64
VALUE_DIM = 128
KV_LORA = 512
FFN_DIM = 10944
BATCH_SIZE = 1
SEQ_LEN = 2048


def draw_tokens(tok_key):
    num_tokens = BATCH_SIZE * SEQ_LEN
    pool_size = num_tokens // 4
    bounds = jnp.asarray(np.arange(pool_size + 1, dtype=np.int64) * VOCAB_SIZE // pool_size, dtype=jnp.int32)
    key_list = jax.random.split(tok_key, 3)
    pool_ids = bounds[:-1] + jax.random.randint(key_list[0], (pool_size,), 0, bounds[1:] - bounds[:-1], dtype=jnp.int32)
    extra_picks = jax.random.randint(key_list[1], (num_tokens - pool_size,), 0, pool_size, dtype=jnp.int32)
    pick_idx = jax.random.permutation(key_list[2], jnp.concatenate([jnp.arange(pool_size, dtype=jnp.int32), extra_picks]))
    return pool_ids[pick_idx].reshape(BATCH_SIZE, SEQ_LEN)


def setup_inputs(seed: int = 0, part: int = 0) -> dict:
    base_key = jax.random.key(seed)
    part_key = jax.random.fold_in(base_key, part)
    key_list = jax.random.split(base_key, 12)
    part_list = jax.random.split(part_key, 2)
    qk_dim = NOPE_DIM + ROPE_DIM

    def normal_bf(idx, shape, scale):
        return (jax.random.normal(key_list[idx], shape, jnp.float32) * scale).astype(jnp.bfloat16)

    def gain_vec(idx, size):
        return 1.0 + 0.3 * jax.random.normal(key_list[idx], (size,), jnp.float32)

    return {
        'tokens': draw_tokens(part_list[0]),
        'embed_table': normal_bf(0, (VOCAB_SIZE, MODEL_DIM), 0.5),
        'w_q': normal_bf(1, (MODEL_DIM, NUM_HEADS, qk_dim), MODEL_DIM ** -0.5),
        'w_dkv': normal_bf(2, (MODEL_DIM, KV_LORA + ROPE_DIM), MODEL_DIM ** -0.5),
        'g_kv': gain_vec(3, KV_LORA),
        'w_uk': normal_bf(4, (KV_LORA, NUM_HEADS, NOPE_DIM), KV_LORA ** -0.5),
        'w_uv': normal_bf(5, (KV_LORA, NUM_HEADS, VALUE_DIM), KV_LORA ** -0.5),
        'w_o': normal_bf(6, (NUM_HEADS, VALUE_DIM, MODEL_DIM), (NUM_HEADS * VALUE_DIM) ** -0.5),
        'g_attn': gain_vec(7, MODEL_DIM),
        'g_mlp': gain_vec(8, MODEL_DIM),
        'w_gate': normal_bf(9, (MODEL_DIM, FFN_DIM), MODEL_DIM ** -0.5),
        'w_up': normal_bf(10, (MODEL_DIM, FFN_DIM), MODEL_DIM ** -0.5),
        'w_down': normal_bf(11, (FFN_DIM, MODEL_DIM), FFN_DIM ** -0.5),
        'd_out': jax.random.normal(part_list[1], (BATCH_SIZE, SEQ_LEN, MODEL_DIM), jnp.float32).astype(jnp.bfloat16),
    }


def to_bf(x_in):
    return x_in.astype(jnp.bfloat16).astype(jnp.float32)


def rms_scale(x_in, gain):
    return x_in * lax.rsqrt(jnp.mean(x_in * x_in, axis=-1, keepdims=True) + 1e-6) * gain


def rope_tables(seq_len, rope_dim):
    inv_freq = 10000.0 ** (-jnp.arange(0, rope_dim, 2, dtype=jnp.float32) / rope_dim)
    angles = jnp.arange(seq_len, dtype=jnp.float32)[:, None] * inv_freq[None, :]
    return jnp.cos(angles), jnp.sin(angles)


def apply_rope(x_in, cos_t, sin_t):
    half_dim = x_in.shape[-1] // 2
    x_lo = x_in[..., :half_dim]
    x_hi = x_in[..., half_dim:]
    return jnp.concatenate([x_lo * cos_t - x_hi * sin_t, x_hi * cos_t + x_lo * sin_t], axis=-1)


def attention(q_nope, q_pe, k_nope, k_pe, value):
    seq_len = q_nope.shape[1]
    scale = (NOPE_DIM + ROPE_DIM) ** -0.5
    causal = jnp.arange(seq_len)[:, None] >= jnp.arange(seq_len)[None, :]

    def one_head(head_in):
        head_qn, head_qp, head_kn, head_val = head_in
        scores = (jnp.einsum('bqn,bkn->bqk', head_qn, head_kn) + jnp.einsum('bqr,bkr->bqk', head_qp, k_pe)) * scale
        scores = jnp.where(causal[None], scores, -1e30)
        attn_prob = to_bf(jax.nn.softmax(scores, axis=-1))
        return to_bf(jnp.einsum('bqk,bkv->bqv', attn_prob, head_val))

    per_head = lax.map(one_head, (jnp.moveaxis(q_nope, 2, 0), jnp.moveaxis(q_pe, 2, 0), jnp.moveaxis(k_nope, 2, 0), jnp.moveaxis(value, 2, 0)))
    return jnp.moveaxis(per_head, 0, 2)


def layer_fwd(embedded, w_q, w_dkv, g_kv, w_uk, w_uv, w_o, g_attn, g_mlp, w_gate, w_up, w_down):
    cos_t, sin_t = rope_tables(embedded.shape[1], ROPE_DIM)
    x_attn = to_bf(rms_scale(embedded, g_attn))
    query = to_bf(jnp.einsum('bsd,dhe->bshe', x_attn, w_q))
    latent = jnp.einsum('bsd,dc->bsc', x_attn, w_dkv)
    c_kv = to_bf(rms_scale(latent[..., :KV_LORA], g_kv))
    k_pe = to_bf(apply_rope(latent[..., KV_LORA:], cos_t, sin_t))
    q_pe = to_bf(apply_rope(query[..., NOPE_DIM:], cos_t[:, None, :], sin_t[:, None, :]))
    k_nope = to_bf(jnp.einsum('bsc,che->bshe', c_kv, w_uk))
    value = to_bf(jnp.einsum('bsc,chv->bshv', c_kv, w_uv))
    attn_out = attention(query[..., :NOPE_DIM], q_pe, k_nope, k_pe, value)
    residual = to_bf(embedded + to_bf(jnp.einsum('bshv,hvd->bsd', attn_out, w_o)))
    x_mlp = to_bf(rms_scale(residual, g_mlp))
    gate = jnp.einsum('bsd,df->bsf', x_mlp, w_gate)
    up_proj = jnp.einsum('bsd,df->bsf', x_mlp, w_up)
    hidden = to_bf(jax.nn.silu(gate) * up_proj)
    mlp_out = to_bf(jnp.einsum('bsf,fd->bsd', hidden, w_down))
    return to_bf(residual + mlp_out)


def reference(tokens, embed_table, w_q, w_dkv, g_kv, w_uk, w_uv, w_o, g_attn, g_mlp, w_gate, w_up, w_down, d_out):
    embedded = jnp.take(embed_table, tokens, axis=0).astype(jnp.float32)
    layer_out, pullback = jax.vjp(layer_fwd, embedded, w_q.astype(jnp.float32), w_dkv.astype(jnp.float32), g_kv, w_uk.astype(jnp.float32), w_uv.astype(jnp.float32), w_o.astype(jnp.float32), g_attn, g_mlp, w_gate.astype(jnp.float32), w_up.astype(jnp.float32), w_down.astype(jnp.float32))
    grad_list = pullback(d_out.astype(jnp.float32))
    d_embed = to_bf(grad_list[0]).reshape(-1, MODEL_DIM)
    d_table = jax.ops.segment_sum(d_embed, tokens.reshape(-1), num_segments=VOCAB_SIZE).astype(jnp.bfloat16)
    return (layer_out.astype(jnp.bfloat16), d_table, grad_list[1], grad_list[2], grad_list[3], grad_list[4], grad_list[5], grad_list[6], grad_list[7], grad_list[8], grad_list[9], grad_list[10], grad_list[11])
```

```python
import functools

import jax
import jax.numpy as jnp
from jax import lax
from jax.experimental import pallas as pl
from jax.experimental.pallas import tpu as pltpu
from jax.sharding import PartitionSpec as P

EPSILON = 1e-6
ROPE_BASE = 10000.0
LOG2E = 1.4426950408889634
BLK = 256
RING = 16
F32 = jnp.float32
BF16 = jnp.bfloat16


def matmul_f32(form, lhs, rhs):
    return jnp.einsum(form, lhs, rhs, preferred_element_type=jnp.float32)


def dot_nn(a, b):
    return lax.dot_general(a, b, (((1,), (0,)), ((), ())), preferred_element_type=F32)


def dot_nt(a, b):
    return lax.dot_general(a, b, (((1,), (1,)), ((), ())), preferred_element_type=F32)


def rope_tables(seq_len, rope_dim):
    inv_freq = ROPE_BASE ** (-jnp.arange(0, rope_dim, 2, dtype=jnp.float32) / rope_dim)
    angles = jnp.arange(seq_len, dtype=jnp.float32)[:, None] * inv_freq[None, :]
    return jnp.cos(angles), jnp.sin(angles)


def apply_rope(x_in, cos_t, sin_t):
    half_dim = x_in.shape[-1] // 2
    x_lo = x_in[..., :half_dim]
    x_hi = x_in[..., half_dim:]
    return jnp.concatenate([x_lo * cos_t - x_hi * sin_t, x_hi * cos_t + x_lo * sin_t], axis=-1)


def unapply_rope(x_in, cos_t, sin_t):
    half_dim = x_in.shape[-1] // 2
    x_lo = x_in[..., :half_dim]
    x_hi = x_in[..., half_dim:]
    return jnp.concatenate([x_lo * cos_t + x_hi * sin_t, x_hi * cos_t - x_lo * sin_t], axis=-1)


def rms_norm(x_in, gain):
    inv_rms = lax.rsqrt(jnp.mean(x_in * x_in, axis=-1, keepdims=True) + EPSILON)
    return (x_in * inv_rms * gain).astype(jnp.bfloat16)


def kv_prep(latent, g_kv):
    value_a7 = g_kv.shape[0]
    cos_t, sin_t = rope_tables(latent.shape[0], latent.shape[-1] - value_a7)
    k_pe = apply_rope(latent[..., value_a7:], cos_t, sin_t).astype(jnp.bfloat16)
    return rms_norm(latent[..., :value_a7], g_kv), k_pe


def gather_body(slot_ref, pos_ref, cnt_ref, tab_ref, out_ref, buf, acc, sems):
    seq = acc.shape[0]
    cnt = cnt_ref[0]

    def fetch(k):
        blk = pl.multiple_of((slot_ref[k] // 8) * 8, 8)
        return pltpu.make_async_copy(tab_ref.at[pl.ds(blk, 8), :], buf.at[k % RING], sems.at[k % RING])

    def prime(k, c):
        fetch(k).start()
        return c

    lax.fori_loop(0, jnp.minimum(cnt, RING), prime, 0)

    def clear(i, c):
        acc[pl.ds(pl.multiple_of(i * 64, 64), 64), :] = jnp.zeros((64, acc.shape[1]), F32)
        return c

    lax.fori_loop(0, seq // 64, clear, 0)
    rows = lax.broadcasted_iota(jnp.int32, (8, acc.shape[1]), 0)

    def step(k, c):
        fetch(k).wait()
        blk = buf[k % RING].astype(F32)
        row = jnp.sum(jnp.where(rows == slot_ref[k] % 8, blk, 0.0), axis=0, keepdims=True)
        acc[pl.ds(pos_ref[k], 1), :] = row

        @pl.when(k + RING < cnt)
        def _():
            fetch(k + RING).start()

        return c

    lax.fori_loop(0, cnt, step, 0)

    def emit(i, c):
        at = pl.ds(pl.multiple_of(i * 64, 64), 64)
        out_ref[at, :] = acc[at, :].astype(BF16)
        return c

    lax.fori_loop(0, seq // 64, emit, 0)


def gather_rows(slots, pos, cnt, table, seq):
    dim = table.shape[1]
    return pl.pallas_call(
        gather_body,
        grid_spec=pltpu.PrefetchScalarGridSpec(
            num_scalar_prefetch=3,
            grid=(1,),
            in_specs=[pl.BlockSpec(memory_space=pl.ANY)],
            out_specs=pl.BlockSpec((seq, dim), lambda i, *_: (0, 0)),
            scratch_shapes=[pltpu.VMEM((RING, 8, dim), BF16), pltpu.VMEM((seq, dim), F32), pltpu.SemaphoreType.DMA((RING,))],
        ),
        out_shape=jax.ShapeDtypeStruct((seq, dim), BF16),
        compiler_params=pltpu.CompilerParams(vmem_limit_bytes=60 * 1024 * 1024),
        cost_estimate=pl.CostEstimate(flops=20_000_000_000, bytes_accessed=24_000_000, transcendentals=0),
        name="gather_rows",
    )(slots, pos, cnt, table)


def scatter_body(slot_ref, pos_ref, cnt_ref, de_ref, zero_ref, out_ref, wide, acc, stage, sems):
    seq = wide.shape[0]
    cnt = cnt_ref[0]

    def widen(i, c):
        at = pl.ds(pl.multiple_of(i * 64, 64), 64)
        wide[at, :] = de_ref[at, :].astype(F32)
        return c

    lax.fori_loop(0, seq // 64, widen, 0)

    def put(slot_blk, n):
        at = pl.multiple_of(slot_blk * 8, 8)
        return pltpu.make_async_copy(stage.at[n % RING], out_ref.at[pl.ds(at, 8), :], sems.at[n % RING])

    def step(k, carry):
        prev, n = carry
        slot = slot_ref[k]
        blk = slot // 8

        @pl.when(blk != prev)
        def _():
            acc[...] = jnp.zeros_like(acc)

        at = pl.ds(slot % 8, 1)
        acc[at, :] = acc[at, :] + wide[pl.ds(pos_ref[k], 1), :]
        last = slot_ref[k + 1] // 8 != blk

        @pl.when(last)
        def _():
            @pl.when(n >= RING)
            def _():
                put(blk, n).wait()

            stage[n % RING] = acc[...].astype(BF16)
            put(blk, n).start()

        return blk, n + last.astype(jnp.int32)

    _, total = lax.fori_loop(0, cnt, step, (jnp.int32(-1), jnp.int32(0)))

    def drain(i, c):
        put(0, i).wait()
        return c

    lax.fori_loop(jnp.maximum(total - RING, 0), total, drain, 0)


def scatter_rows(slots, pos, cnt, de, zeros):
    seq, dim = de.shape
    return pl.pallas_call(
        scatter_body,
        grid_spec=pltpu.PrefetchScalarGridSpec(
            num_scalar_prefetch=3,
            grid=(1,),
            in_specs=[pl.BlockSpec((seq, dim), lambda i, *_: (0, 0)), pl.BlockSpec(memory_space=pl.ANY)],
            out_specs=pl.BlockSpec(memory_space=pl.ANY),
            scratch_shapes=[pltpu.VMEM((seq, dim), F32), pltpu.VMEM((8, dim), F32), pltpu.VMEM((RING, 8, dim), BF16), pltpu.SemaphoreType.DMA((RING,))],
        ),
        out_shape=jax.ShapeDtypeStruct(zeros.shape, BF16),
        input_output_aliases={4: 0},
        compiler_params=pltpu.CompilerParams(vmem_limit_bytes=60 * 1024 * 1024),
        cost_estimate=pl.CostEstimate(flops=20_000_000_000, bytes_accessed=24_000_000, transcendentals=0),
        name="scatter_rows",
    )(slots, pos, cnt, de, zeros)


def attn_fwd_body(scale2, q_ref, k_ref, vt_ref, o_ref, lse_ref, s_scr):
    seq = q_ref.shape[1]
    tri = lax.broadcasted_iota(jnp.int32, (BLK, BLK), 0) <= lax.broadcasted_iota(jnp.int32, (BLK, BLK), 1)
    for i in range(seq // BLK):
        q_i = q_ref[0, i * BLK:(i + 1) * BLK, :]
        top = None
        for j in range(i + 1):
            s = dot_nt(k_ref[0, j * BLK:(j + 1) * BLK, :], q_i) * scale2
            if j == i:
                s = jnp.where(tri, s, -1e30)
            s_scr[j * BLK:(j + 1) * BLK, :] = s
            part = jnp.max(s.reshape(BLK // 8, 8, BLK), axis=0)
            top = part if top is None else jnp.maximum(top, part)
        top = jnp.max(top, axis=0, keepdims=True)
        den = None
        for j in range(i + 1):
            e = jnp.exp2(s_scr[j * BLK:(j + 1) * BLK, :] - top)
            s_scr[j * BLK:(j + 1) * BLK, :] = e
            part = jnp.sum(e.reshape(BLK // 8, 8, BLK), axis=0)
            den = part if den is None else den + part
        den = jnp.sum(den, axis=0, keepdims=True)
        inv = 1.0 / den
        out = None
        for j in range(i + 1):
            prob = (s_scr[j * BLK:(j + 1) * BLK, :] * inv).astype(BF16)
            part = dot_nn(vt_ref[0, :, j * BLK:(j + 1) * BLK], prob)
            out = part if out is None else out + part
        o_ref[i * BLK:(i + 1) * BLK, :] = out.T.astype(BF16)
        lse_ref[0, :, i * BLK:(i + 1) * BLK] = top + jnp.log2(den)


def attn_fwd(q, k, vt, scale):
    heads, seq, qk = q.shape
    vdim = vt.shape[1]
    return pl.pallas_call(
        functools.partial(attn_fwd_body, scale * LOG2E),
        grid=(heads,),
        in_specs=[pl.BlockSpec((1, seq, qk), lambda h: (h, 0, 0)), pl.BlockSpec((1, seq, qk), lambda h: (h, 0, 0)), pl.BlockSpec((1, vdim, seq), lambda h: (h, 0, 0))],
        out_specs=[pl.BlockSpec((seq, vdim), lambda h: (0, h)), pl.BlockSpec((1, 1, seq), lambda h: (h, 0, 0))],
        out_shape=[jax.ShapeDtypeStruct((seq, heads * vdim), BF16), jax.ShapeDtypeStruct((heads, 1, seq), F32)],
        scratch_shapes=[pltpu.VMEM((seq, BLK), F32)],
        compiler_params=pltpu.CompilerParams(vmem_limit_bytes=40 * 1024 * 1024),
        cost_estimate=pl.CostEstimate(flops=20_000_000_000, bytes_accessed=10_000_000, transcendentals=0),
        name="attn_fwd",
    )(q, k, vt)


def attn_bwd_body(scale2, scale, q_ref, k_ref, kt_ref, v_ref, do_ref, lse_ref, dlt_ref, dqt_ref, dk_ref, dv_ref, p_scr, ds_scr):
    seq = q_ref.shape[1]
    n = seq // BLK
    tri = lax.broadcasted_iota(jnp.int32, (BLK, BLK), 0) <= lax.broadcasted_iota(jnp.int32, (BLK, BLK), 1)
    for j in range(n):
        at_j = slice(j * BLK, (j + 1) * BLK)
        k_j = k_ref[0, at_j, :]
        v_j = v_ref[0, at_j, :]
        for i in range(j, n):
            at_i = slice(i * BLK, (i + 1) * BLK)
            s = dot_nt(k_j, q_ref[0, at_i, :])
            prob = jnp.exp2(s * scale2 - lse_ref[0, :, at_i])
            if i == j:
                prob = jnp.where(tri, prob, 0.0)
            dp = dot_nt(v_j, do_ref[at_i, :])
            p_scr[:, at_i] = prob.astype(BF16)
            ds_scr[at_j, at_i] = (prob * (dp - dlt_ref[0, :, at_i])).astype(BF16)
        dv_ref[0, at_j, :] = dot_nn(p_scr[:, j * BLK:], do_ref[j * BLK:, :]).astype(BF16)
        dk_ref[0, at_j, :] = dot_nn(ds_scr[at_j, j * BLK:], q_ref[0, j * BLK:, :]) * scale
    for i in range(n):
        at_i = slice(i * BLK, (i + 1) * BLK)
        dqt_ref[0, :, at_i] = dot_nn(kt_ref[0, :, :(i + 1) * BLK], ds_scr[:(i + 1) * BLK, at_i]) * scale


def attn_bwd(q, k, kt, v, do, lse, dlt, scale):
    heads, seq, qk = q.shape
    vdim = v.shape[2]
    per_head = lambda h: (h, 0, 0)
    return pl.pallas_call(
        functools.partial(attn_bwd_body, scale * LOG2E, scale),
        grid=(heads,),
        in_specs=[
            pl.BlockSpec((1, seq, qk), per_head),
            pl.BlockSpec((1, seq, qk), per_head),
            pl.BlockSpec((1, qk, seq), per_head),
            pl.BlockSpec((1, seq, vdim), per_head),
            pl.BlockSpec((seq, vdim), lambda h: (0, h)),
            pl.BlockSpec((1, 1, seq), per_head),
            pl.BlockSpec((1, 1, seq), per_head),
        ],
        out_specs=[pl.BlockSpec((1, qk, seq), per_head), pl.BlockSpec((1, seq, qk), per_head), pl.BlockSpec((1, seq, vdim), per_head)],
        out_shape=[jax.ShapeDtypeStruct((heads, qk, seq), F32), jax.ShapeDtypeStruct((heads, seq, qk), F32), jax.ShapeDtypeStruct((heads, seq, vdim), BF16)],
        scratch_shapes=[pltpu.VMEM((BLK, seq), BF16), pltpu.VMEM((seq, seq), BF16)],
        compiler_params=pltpu.CompilerParams(vmem_limit_bytes=56 * 1024 * 1024),
        cost_estimate=pl.CostEstimate(flops=50_000_000_000, bytes_accessed=16_000_000, transcendentals=0),
        name="attn_bwd",
    )(q, k, kt, v, do, lse, dlt)


def gather_seq(x):
    return lax.all_gather(x, 'tp', axis=0, tiled=True)


def scatter_seq(x):
    return lax.psum_scatter(x, 'tp', scatter_dimension=0, tiled=True)


def layer_pass(embedded, d_out, dy_full, w_q, w_dkv, g_kv, w_uk, w_uv, w_o, g_attn, g_mlp, w_gate, w_up, w_down):
    heads, qk = w_q.shape[1:]
    nope = w_uk.shape[2]
    vdim = w_uv.shape[2]
    scale = qk ** -0.5
    w_o2 = w_o.reshape(heads * vdim, -1)
    x_attn_loc, attn_norm_pull = jax.vjp(rms_norm, embedded.astype(F32), g_attn)
    x_attn = gather_seq(x_attn_loc)
    seq = x_attn.shape[0]
    cos_t, sin_t = rope_tables(seq, qk - nope)
    query = matmul_f32('sd,dhe->hse', x_attn, w_q).astype(BF16)
    latent = matmul_f32('sd,dc->sc', x_attn, w_dkv)
    (c_kv, k_pe), kv_pull = jax.vjp(kv_prep, latent, g_kv)
    k_nope = matmul_f32('sc,che->hse', c_kv, w_uk).astype(BF16)
    value = matmul_f32('sc,chv->hsv', c_kv, w_uv).astype(BF16)
    q_pe = apply_rope(query[..., nope:].astype(F32), cos_t, sin_t).astype(BF16)
    q_cat = jnp.concatenate([query[..., :nope], q_pe], axis=-1)
    k_cat = jnp.concatenate([k_nope, jnp.broadcast_to(k_pe[None], (heads,) + k_pe.shape)], axis=-1)
    attn_out, lse = attn_fwd(q_cat, k_cat, jnp.swapaxes(value, 1, 2), scale)
    attn_part = matmul_f32('sv,vd->sd', attn_out, w_o2).astype(BF16)
    attn_loc = scatter_seq(attn_part)
    residual = (embedded.astype(F32) + attn_loc.astype(F32)).astype(BF16)
    x_mlp_loc, mlp_norm_pull = jax.vjp(rms_norm, residual.astype(F32), g_mlp)
    x_mlp = gather_seq(x_mlp_loc)
    gate = matmul_f32('sd,df->sf', x_mlp, w_gate)
    up_proj = matmul_f32('sd,df->sf', x_mlp, w_up)
    gate_sig = jax.nn.sigmoid(gate)
    hidden = (gate * gate_sig * up_proj).astype(BF16)
    mlp_part = matmul_f32('sf,fd->sd', hidden, w_down).astype(BF16)
    mlp_loc = scatter_seq(mlp_part)
    layer_out = (residual.astype(F32) + mlp_loc.astype(F32)).astype(BF16)

    d_hidden = matmul_f32('sd,fd->sf', dy_full, w_down)
    dw_down = matmul_f32('sf,sd->fd', hidden, dy_full)
    d_up = (d_hidden * gate * gate_sig).astype(BF16)
    d_gate = (d_hidden * up_proj * gate_sig * (1.0 + gate * (1.0 - gate_sig))).astype(BF16)
    dw_gate = matmul_f32('sd,sf->df', x_mlp, d_gate)
    dw_up = matmul_f32('sd,sf->df', x_mlp, d_up)
    dx_mlp_part = (matmul_f32('sf,df->sd', d_gate, w_gate) + matmul_f32('sf,df->sd', d_up, w_up)).astype(BF16)
    dx_mlp = scatter_seq(dx_mlp_part)
    d_res_norm, dg_mlp_part = mlp_norm_pull(dx_mlp)
    d_residual = d_out.astype(F32) + d_res_norm
    d_attn_full = gather_seq(d_residual.astype(BF16))
    dw_o = matmul_f32('sv,sd->vd', attn_out, d_attn_full).reshape(w_o.shape)
    d_attn_out = matmul_f32('sd,vd->sv', d_attn_full, w_o2).astype(BF16)
    delta = jnp.sum((d_attn_out.astype(F32) * attn_out.astype(F32)).reshape(seq, heads, vdim), axis=-1).T.reshape(heads, 1, seq)
    d_qt, d_k, d_value = attn_bwd(q_cat, k_cat, jnp.swapaxes(k_cat, 1, 2), value, d_attn_out, lse, delta, scale)
    d_q = jnp.swapaxes(d_qt, 1, 2)
    d_query = jnp.concatenate([d_q[..., :nope], unapply_rope(d_q[..., nope:], cos_t, sin_t)], axis=-1).astype(BF16)
    d_knope = d_k[..., :nope].astype(BF16)
    d_kpe = jnp.sum(d_k[..., nope:], axis=0).astype(BF16)
    dw_uk = matmul_f32('sc,hse->che', c_kv, d_knope)
    dw_uv = matmul_f32('sc,hsv->chv', c_kv, d_value)
    d_ckv = (matmul_f32('hse,che->sc', d_knope, w_uk) + matmul_f32('hsv,chv->sc', d_value, w_uv)).astype(BF16)
    d_latent, dg_kv_part = kv_pull((d_ckv, d_kpe))
    d_latent = d_latent.astype(BF16)
    dw_q = matmul_f32('sd,hse->dhe', x_attn, d_query)
    dw_dkv_part = matmul_f32('sd,sc->dc', x_attn, d_latent)
    dx_attn_part = (matmul_f32('hse,dhe->sd', d_query, w_q) + matmul_f32('sc,dc->sd', d_latent, w_dkv)).astype(BF16)
    dx_attn = scatter_seq(dx_attn_part)
    d_emb_norm, dg_attn_part = attn_norm_pull(dx_attn)
    d_embed = (d_residual + d_emb_norm).astype(BF16)
    dw_dkv, dg_kv, dg_attn, dg_mlp = lax.psum((dw_dkv_part, dg_kv_part, dg_attn_part, dg_mlp_part), 'tp')
    return layer_out, d_embed, (dw_q, dw_dkv, dg_kv, dw_uk, dw_uv, dw_o, dg_attn, dg_mlp, dw_gate, dw_up, dw_down)


def solution(mesh):
    def device_step(tokens, embed_table, w_q, w_dkv, g_kv, w_uk, w_uv, w_o, g_attn, g_mlp, w_gate, w_up, w_down, d_out):
        vocab_local, model_dim = embed_table.shape
        seq = tokens.shape[1]
        dy_loc = d_out[0]
        dy_full = gather_seq(dy_loc)
        local_ids = tokens[0] - lax.axis_index('tp') * vocab_local
        owned = (local_ids >= 0) & (local_ids < vocab_local)
        slots, pos = lax.sort((jnp.where(owned, local_ids, vocab_local), lax.iota(jnp.int32, seq)), num_keys=1)
        slots = jnp.concatenate([slots, jnp.full((128,), vocab_local, jnp.int32)])
        cnt = jnp.sum(owned.astype(jnp.int32)).reshape(1)
        rows = gather_rows(slots, pos, cnt, embed_table, seq)
        embedded = scatter_seq(rows)
        layer_out, d_embed, weight_grads = layer_pass(embedded, dy_loc, dy_full, w_q, w_dkv, g_kv, w_uk, w_uv, w_o, g_attn, g_mlp, w_gate, w_up, w_down)
        de_full = gather_seq(d_embed)
        d_table = scatter_rows(slots, pos, cnt, de_full, jnp.zeros((vocab_local, model_dim), BF16))
        return (layer_out[None], d_table) + weight_grads

    row_spec = P('dp', 'tp', None)
    head_spec = P(None, 'tp', None)
    in_specs = (P('dp', None), P('tp', None), head_spec, P(None, None), P(None), head_spec, head_spec, P('tp', None, None), P(None), P(None), P(None, 'tp'), P(None, 'tp'), P('tp', None), row_spec)
    out_specs = (row_spec, P(('dp', 'tp'), None), P('dp', 'tp', None), P('dp', None), P('dp'), P('dp', 'tp', None), P('dp', 'tp', None), P(('dp', 'tp'), None, None), P('dp'), P('dp'), P('dp', 'tp'), P('dp', 'tp'), P(('dp', 'tp'), None))
    return jax.shard_map(device_step, mesh=mesh, in_specs=in_specs, out_specs=out_specs, check_vma=False)
```

```python
import functools

import jax
import jax.numpy as jnp
from jax import lax
from jax.experimental import pallas as pl
from jax.experimental.pallas import tpu as pltpu
from jax.sharding import PartitionSpec as P

EPSILON = 1e-6
ROPE_BASE = 10000.0
LOG2E = 1.4426950408889634
BLK = 256
RING = 16
F32 = jnp.float32
BF16 = jnp.bfloat16


def matmul_f32(form, lhs, rhs):
    return jnp.einsum(form, lhs, rhs, preferred_element_type=jnp.float32)


def dot_nn(a, b):
    return lax.dot_general(a, b, (((1,), (0,)), ((), ())), preferred_element_type=F32)


def dot_nt(a, b):
    return lax.dot_general(a, b, (((1,), (1,)), ((), ())), preferred_element_type=F32)


def rope_tables(seq_len, rope_dim):
    inv_freq = ROPE_BASE ** (-jnp.arange(0, rope_dim, 2, dtype=jnp.float32) / rope_dim)
    angles = jnp.arange(seq_len, dtype=jnp.float32)[:, None] * inv_freq[None, :]
    return jnp.cos(angles), jnp.sin(angles)


def apply_rope(x_in, cos_t, sin_t):
    half_dim = x_in.shape[-1] // 2
    x_lo = x_in[..., :half_dim]
    x_hi = x_in[..., half_dim:]
    return jnp.concatenate([x_lo * cos_t - x_hi * sin_t, x_hi * cos_t + x_lo * sin_t], axis=-1)


def unapply_rope(x_in, cos_t, sin_t):
    half_dim = x_in.shape[-1] // 2
    x_lo = x_in[..., :half_dim]
    x_hi = x_in[..., half_dim:]
    return jnp.concatenate([x_lo * cos_t + x_hi * sin_t, x_hi * cos_t - x_lo * sin_t], axis=-1)


def rms_norm(x_in, gain):
    inv_rms = lax.rsqrt(jnp.mean(x_in * x_in, axis=-1, keepdims=True) + EPSILON)
    return (x_in * inv_rms * gain).astype(jnp.bfloat16)


def kv_prep(latent, g_kv):
    value_a7 = g_kv.shape[0]
    cos_t, sin_t = rope_tables(latent.shape[0], latent.shape[-1] - value_a7)
    k_pe = apply_rope(latent[..., value_a7:], cos_t, sin_t).astype(jnp.bfloat16)
    return rms_norm(latent[..., :value_a7], g_kv), k_pe


def gather_body(slot_ref, pos_ref, cnt_ref, tab_ref, out_ref, buf, acc, sems):
    seq = acc.shape[0]
    cnt = cnt_ref[0]

    def fetch(k):
        blk = pl.multiple_of((slot_ref[k] // 8) * 8, 8)
        return pltpu.make_async_copy(tab_ref.at[pl.ds(blk, 8), :], buf.at[k % RING], sems.at[k % RING])

    def prime(k, c):
        fetch(k).start()
        return c

    lax.fori_loop(0, jnp.minimum(cnt, RING), prime, 0)

    def clear(i, c):
        acc[pl.ds(pl.multiple_of(i * 64, 64), 64), :] = jnp.zeros((64, acc.shape[1]), F32)
        return c

    lax.fori_loop(0, seq // 64, clear, 0)
    rows = lax.broadcasted_iota(jnp.int32, (8, acc.shape[1]), 0)

    def step(k, c):
        fetch(k).wait()
        blk = buf[k % RING].astype(F32)
        row = jnp.sum(jnp.where(rows == slot_ref[k] % 8, blk, 0.0), axis=0, keepdims=True)
        acc[pl.ds(pos_ref[k], 1), :] = row

        @pl.when(k + RING < cnt)
        def _():
            fetch(k + RING).start()

        return c

    lax.fori_loop(0, cnt, step, 0)

    def emit(i, c):
        at = pl.ds(pl.multiple_of(i * 64, 64), 64)
        out_ref[at, :] = acc[at, :].astype(BF16)
        return c

    lax.fori_loop(0, seq // 64, emit, 0)


def gather_rows(slots, pos, cnt, table, seq):
    dim = table.shape[1]
    return pl.pallas_call(
        gather_body,
        grid_spec=pltpu.PrefetchScalarGridSpec(
            num_scalar_prefetch=3,
            grid=(1,),
            in_specs=[pl.BlockSpec(memory_space=pl.ANY)],
            out_specs=pl.BlockSpec((seq, dim), lambda i, *_: (0, 0)),
            scratch_shapes=[pltpu.VMEM((RING, 8, dim), BF16), pltpu.VMEM((seq, dim), F32), pltpu.SemaphoreType.DMA((RING,))],
        ),
        out_shape=jax.ShapeDtypeStruct((seq, dim), BF16),
        compiler_params=pltpu.CompilerParams(vmem_limit_bytes=60 * 1024 * 1024),
        cost_estimate=pl.CostEstimate(flops=20_000_000_000, bytes_accessed=24_000_000, transcendentals=0),
        name="gather_rows",
    )(slots, pos, cnt, table)


def scatter_body(slot_ref, pos_ref, cnt_ref, de_ref, zero_ref, out_ref, wide, acc, stage, sems):
    seq = wide.shape[0]
    cnt = cnt_ref[0]

    def widen(i, c):
        at = pl.ds(pl.multiple_of(i * 64, 64), 64)
        wide[at, :] = de_ref[at, :].astype(F32)
        return c

    lax.fori_loop(0, seq // 64, widen, 0)

    def put(slot_blk, n):
        at = pl.multiple_of(slot_blk * 8, 8)
        return pltpu.make_async_copy(stage.at[n % RING], out_ref.at[pl.ds(at, 8), :], sems.at[n % RING])

    def step(k, carry):
        prev, n = carry
        slot = slot_ref[k]
        blk = slot // 8

        @pl.when(blk != prev)
        def _():
            acc[...] = jnp.zeros_like(acc)

        at = pl.ds(slot % 8, 1)
        acc[at, :] = acc[at, :] + wide[pl.ds(pos_ref[k], 1), :]
        last = slot_ref[k + 1] // 8 != blk

        @pl.when(last)
        def _():
            @pl.when(n >= RING)
            def _():
                put(blk, n).wait()

            stage[n % RING] = acc[...].astype(BF16)
            put(blk, n).start()

        return blk, n + last.astype(jnp.int32)

    _, total = lax.fori_loop(0, cnt, step, (jnp.int32(-1), jnp.int32(0)))

    def drain(i, c):
        put(0, i).wait()
        return c

    lax.fori_loop(jnp.maximum(total - RING, 0), total, drain, 0)


def scatter_rows(slots, pos, cnt, de, zeros):
    seq, dim = de.shape
    return pl.pallas_call(
        scatter_body,
        grid_spec=pltpu.PrefetchScalarGridSpec(
            num_scalar_prefetch=3,
            grid=(1,),
            in_specs=[pl.BlockSpec((seq, dim), lambda i, *_: (0, 0)), pl.BlockSpec(memory_space=pl.ANY)],
            out_specs=pl.BlockSpec(memory_space=pl.ANY),
            scratch_shapes=[pltpu.VMEM((seq, dim), F32), pltpu.VMEM((8, dim), F32), pltpu.VMEM((RING, 8, dim), BF16), pltpu.SemaphoreType.DMA((RING,))],
        ),
        out_shape=jax.ShapeDtypeStruct(zeros.shape, BF16),
        input_output_aliases={4: 0},
        compiler_params=pltpu.CompilerParams(vmem_limit_bytes=60 * 1024 * 1024),
        cost_estimate=pl.CostEstimate(flops=20_000_000_000, bytes_accessed=24_000_000, transcendentals=0),
        name="scatter_rows",
    )(slots, pos, cnt, de, zeros)


def attn_fwd_body(scale2, q_ref, k_ref, vt_ref, o_ref, lse_ref, s_scr):
    seq = q_ref.shape[1]
    tri = lax.broadcasted_iota(jnp.int32, (BLK, BLK), 0) <= lax.broadcasted_iota(jnp.int32, (BLK, BLK), 1)
    for i in range(seq // BLK):
        q_i = q_ref[0, i * BLK:(i + 1) * BLK, :]
        top = None
        for j in range(i + 1):
            s = dot_nt(k_ref[0, j * BLK:(j + 1) * BLK, :], q_i) * scale2
            if j == i:
                s = jnp.where(tri, s, -1e30)
            s_scr[j * BLK:(j + 1) * BLK, :] = s
            part = jnp.max(s.reshape(BLK // 8, 8, BLK), axis=0)
            top = part if top is None else jnp.maximum(top, part)
        top = jnp.max(top, axis=0, keepdims=True)
        den = None
        for j in range(i + 1):
            e = jnp.exp2(s_scr[j * BLK:(j + 1) * BLK, :] - top)
            s_scr[j * BLK:(j + 1) * BLK, :] = e
            part = jnp.sum(e.reshape(BLK // 8, 8, BLK), axis=0)
            den = part if den is None else den + part
        den = jnp.sum(den, axis=0, keepdims=True)
        inv = 1.0 / den
        out = None
        for j in range(i + 1):
            prob = (s_scr[j * BLK:(j + 1) * BLK, :] * inv).astype(BF16)
            part = dot_nn(vt_ref[0, :, j * BLK:(j + 1) * BLK], prob)
            out = part if out is None else out + part
        o_ref[i * BLK:(i + 1) * BLK, :] = out.T.astype(BF16)
        lse_ref[0, :, i * BLK:(i + 1) * BLK] = top + jnp.log2(den)


def attn_fwd(q, k, vt, scale):
    heads, seq, qk = q.shape
    vdim = vt.shape[1]
    return pl.pallas_call(
        functools.partial(attn_fwd_body, scale * LOG2E),
        grid=(heads,),
        in_specs=[pl.BlockSpec((1, seq, qk), lambda h: (h, 0, 0)), pl.BlockSpec((1, seq, qk), lambda h: (h, 0, 0)), pl.BlockSpec((1, vdim, seq), lambda h: (h, 0, 0))],
        out_specs=[pl.BlockSpec((seq, vdim), lambda h: (0, h)), pl.BlockSpec((1, 1, seq), lambda h: (h, 0, 0))],
        out_shape=[jax.ShapeDtypeStruct((seq, heads * vdim), BF16), jax.ShapeDtypeStruct((heads, 1, seq), F32)],
        scratch_shapes=[pltpu.VMEM((seq, BLK), F32)],
        compiler_params=pltpu.CompilerParams(vmem_limit_bytes=40 * 1024 * 1024),
        cost_estimate=pl.CostEstimate(flops=20_000_000_000, bytes_accessed=10_000_000, transcendentals=0),
        name="attn_fwd",
    )(q, k, vt)


def attn_bwd_body(scale2, scale, q_ref, k_ref, kt_ref, v_ref, do_ref, lse_ref, dlt_ref, dqt_ref, dk_ref, dv_ref, p_scr, ds_scr):
    seq = q_ref.shape[1]
    n = seq // BLK
    tri = lax.broadcasted_iota(jnp.int32, (BLK, BLK), 0) <= lax.broadcasted_iota(jnp.int32, (BLK, BLK), 1)
    for j in range(n):
        at_j = slice(j * BLK, (j + 1) * BLK)
        k_j = k_ref[0, at_j, :]
        v_j = v_ref[0, at_j, :]
        for i in range(j, n):
            at_i = slice(i * BLK, (i + 1) * BLK)
            s = dot_nt(k_j, q_ref[0, at_i, :])
            prob = jnp.exp2(s * scale2 - lse_ref[0, :, at_i])
            if i == j:
                prob = jnp.where(tri, prob, 0.0)
            dp = dot_nt(v_j, do_ref[at_i, :])
            p_scr[:, at_i] = prob.astype(BF16)
            ds_scr[at_j, at_i] = (prob * (dp - dlt_ref[0, :, at_i])).astype(BF16)
        dv_ref[0, at_j, :] = dot_nn(p_scr[:, j * BLK:], do_ref[j * BLK:, :]).astype(BF16)
        dk_ref[0, at_j, :] = dot_nn(ds_scr[at_j, j * BLK:], q_ref[0, j * BLK:, :]) * scale
    for i in range(n):
        at_i = slice(i * BLK, (i + 1) * BLK)
        dqt_ref[0, :, at_i] = dot_nn(kt_ref[0, :, :(i + 1) * BLK], ds_scr[:(i + 1) * BLK, at_i]) * scale


def attn_bwd(q, k, kt, v, do, lse, dlt, scale):
    heads, seq, qk = q.shape
    vdim = v.shape[2]
    per_head = lambda h: (h, 0, 0)
    return pl.pallas_call(
        functools.partial(attn_bwd_body, scale * LOG2E, scale),
        grid=(heads,),
        in_specs=[
            pl.BlockSpec((1, seq, qk), per_head),
            pl.BlockSpec((1, seq, qk), per_head),
            pl.BlockSpec((1, qk, seq), per_head),
            pl.BlockSpec((1, seq, vdim), per_head),
            pl.BlockSpec((seq, vdim), lambda h: (0, h)),
            pl.BlockSpec((1, 1, seq), per_head),
            pl.BlockSpec((1, 1, seq), per_head),
        ],
        out_specs=[pl.BlockSpec((1, qk, seq), per_head), pl.BlockSpec((1, seq, qk), per_head), pl.BlockSpec((1, seq, vdim), per_head)],
        out_shape=[jax.ShapeDtypeStruct((heads, qk, seq), F32), jax.ShapeDtypeStruct((heads, seq, qk), F32), jax.ShapeDtypeStruct((heads, seq, vdim), BF16)],
        scratch_shapes=[pltpu.VMEM((BLK, seq), BF16), pltpu.VMEM((seq, seq), BF16)],
        compiler_params=pltpu.CompilerParams(vmem_limit_bytes=56 * 1024 * 1024),
        cost_estimate=pl.CostEstimate(flops=50_000_000_000, bytes_accessed=16_000_000, transcendentals=0),
        name="attn_bwd",
    )(q, k, kt, v, do, lse, dlt)


HALF = 128
SHARD = 256
MESH = pl.DeviceIdType.MESH


def xor_bits(t, u):
    out = 0
    for b in (1, 2, 4):
        tb = (t // b) % 2
        ub = (u // b) % 2
        out = out + b * (tb + ub - 2 * tb * ub)
    return out


def greet(t):
    peers = [xor_bits(t, u) for u in (1, 2, 4)]
    barrier = pltpu.get_barrier_semaphore()
    for peer in peers:
        pl.semaphore_signal(barrier, inc=1, device_id={'tp': peer}, device_id_type=MESH)
    pl.semaphore_wait(barrier, 3)
    return peers


def half_rows(shard, half):
    return pl.ds(pl.multiple_of(shard * SHARD + half * HALF, HALF), HALF)


def ag_unit(i):
    p = i // 4
    r = i % 4
    p0 = (3 - p) // 3
    p3 = p // 3
    mid = 1 - p0 - p3
    u = p0 * (r // 2) + mid * (2 + (r % 2) * 2 + r // 2) + p3 * (6 + r // 2)
    flip = (p - 1) * mid
    return u, (r % 2) + flip * (1 - 2 * (r % 2))


def ag_run(x_ref, full, send, recv, compute):
    t = lax.axis_index('tp')
    partner, xn, yn = greet(t)

    def copy(src, shard, half, sem, u_there, dev):
        return pltpu.make_async_remote_copy(
            src_ref=src, dst_ref=full.at[half_rows(shard, half), :], send_sem=send.at[sem],
            recv_sem=recv.at[u_there, half], device_id={'tp': dev}, device_id_type=MESH)

    def mine(half):
        return x_ref.at[pl.ds(half * HALF, HALF), :]

    def held(u, half):
        return full.at[half_rows(xor_bits(t, u), half), :]

    own = [copy(mine(0), t, 0, 0, 2, xn), copy(mine(1), t, 1, 3, 4, yn), copy(mine(0), t, 0, 4, 1, partner), copy(mine(1), t, 1, 5, 1, partner),
           copy(mine(1), t, 1, 1, 2, xn), copy(mine(0), t, 0, 2, 4, yn)]
    for c in own:
        c.start()
    full[pl.ds(pl.multiple_of(t * SHARD, SHARD), SHARD), :] = x_ref[...]
    fwd_y = copy(held(2, 0), xor_bits(t, 2), 0, 6, 6, yn)
    fwd_x = copy(held(4, 1), xor_bits(t, 4), 1, 7, 6, xn)
    fwd_p = {(u, h): copy(held(u, h), xor_bits(t, u), h, 8 + (u - 2) + h, u + 1, partner) for u in (2, 4, 6) for h in (0, 1)}

    def arrive(u, h):
        copy(held(u, h), xor_bits(t, u), h, 0, u, partner).wait_recv()

    def step(i, carry):
        @pl.when(i == 2)
        def _():
            arrive(1, 0)
            arrive(1, 1)

        @pl.when(i == 4)
        def _():
            arrive(2, 0)
            fwd_y.start()
            fwd_p[2, 0].start()
            arrive(4, 1)
            fwd_x.start()
            fwd_p[4, 1].start()

        @pl.when(i == 6)
        def _():
            arrive(3, 0)
            arrive(5, 1)

        @pl.when(i == 8)
        def _():
            arrive(2, 1)
            fwd_p[2, 1].start()
            arrive(4, 0)
            fwd_p[4, 0].start()

        @pl.when(i == 10)
        def _():
            arrive(3, 1)
            arrive(5, 0)

        @pl.when(i == 12)
        def _():
            arrive(6, 0)
            fwd_p[6, 0].start()
            arrive(6, 1)
            fwd_p[6, 1].start()

        @pl.when(i == 14)
        def _():
            arrive(7, 0)
            arrive(7, 1)

        u, h = ag_unit(i)
        compute(i, xor_bits(t, u), h)
        return carry

    lax.fori_loop(0, 16, step, 0)
    for c in own + [fwd_y, fwd_x] + list(fwd_p.values()):
        c.wait_send()


AG_SEMS = [pltpu.SemaphoreType.DMA((14,)), pltpu.SemaphoreType.DMA((8, 2))]


def rs_unit(i):
    p = i // 2
    p0 = (1 - p % 2) * (1 - p // 2)
    p1 = (p % 2) * (1 - p // 2)
    p2 = (p // 2) * (1 - p % 2)
    return p0 * 6 + p1 * 2 + p2 * 4 + 1 - i % 2


def rs_run(stage, fp, fx, fy, send, recv, produce, finish):
    t = lax.axis_index('tp')
    partner, xn, yn = greet(t)

    def copy(src, dst, sem, dev):
        return pltpu.make_async_remote_copy(src_ref=src, dst_ref=dst, send_sem=send.at[sem], recv_sem=recv.at[sem], device_id={'tp': dev}, device_id_type=MESH)

    def half(h):
        return pl.ds(h * HALF, HALF)

    sx = [copy(stage.at[1, half(1), :], fx.at[0], 4, xn), copy(stage.at[3, half(1), :], fx.at[1], 5, xn), copy(stage.at[3, half(0), :], fx.at[2], 6, xn)]
    sy = [copy(stage.at[1, half(0), :], fy.at[0], 7, yn), copy(stage.at[5, half(0), :], fy.at[1], 8, yn), copy(stage.at[5, half(1), :], fy.at[2], 9, yn)]

    def add(i, first, count, src, src_first):
        def body(r, c):
            a = pl.ds(pl.multiple_of(first + r * 32, 32), 32)
            b = pl.ds(pl.multiple_of(src_first + r * 32, 32), 32)
            stage[i, a, :] = (stage[i, a, :].astype(F32) + src[b, :].astype(F32)).astype(BF16)
            return c

        lax.fori_loop(0, count // 32, body, 0)

    def step(i, carry):
        p = i // 2
        produce(i, xor_bits(t, rs_unit(i)))
        to_partner = copy(stage.at[i], fp.at[p], p, partner)

        @pl.when(i % 2 == 0)
        def _():
            to_partner.start()

        @pl.when(i % 2 == 1)
        def _():
            to_partner.wait_recv()
            add(i, 0, SHARD, fp.at[p], 0)

        @pl.when(i == 1)
        def _():
            sx[0].start()
            sy[0].start()

        @pl.when(i == 3)
        def _():
            sx[1].start()

        @pl.when(i == 5)
        def _():
            sy[1].start()
            sy[0].wait_recv()
            add(3, 0, HALF, fy.at[0], 0)
            sx[2].start()
            sx[0].wait_recv()
            add(5, HALF, HALF, fx.at[0], 0)
            sy[2].start()

        return carry

    lax.fori_loop(0, 8, step, 0)
    sy[1].wait_recv()
    sx[1].wait_recv()
    sx[2].wait_recv()
    sy[2].wait_recv()

    def last(r, c):
        lo = pl.ds(pl.multiple_of(r * 32, 32), 32)
        hi = pl.ds(pl.multiple_of(HALF + r * 32, 32), 32)
        finish(lo, (stage[7, lo, :].astype(F32) + fy[1, lo, :].astype(F32)) + fx[2, lo, :].astype(F32))
        finish(hi, (stage[7, hi, :].astype(F32) + fx[1, lo, :].astype(F32)) + fy[2, lo, :].astype(F32))
        return c

    lax.fori_loop(0, HALF // 32, last, 0)
    for q in range(4):
        copy(stage.at[2 * q], fp.at[q], q, partner).wait_send()
    for c in sx + sy:
        c.wait_send()


def rs_scratch(dim):
    return [pltpu.VMEM((8, SHARD, dim), BF16), pltpu.VMEM((4, SHARD, dim), BF16), pltpu.VMEM((3, HALF, dim), BF16), pltpu.VMEM((3, HALF, dim), BF16),
            pltpu.SemaphoreType.DMA((10,)), pltpu.SemaphoreType.DMA((10,))]


VM = pl.BlockSpec(memory_space=pltpu.VMEM)
ANY = pl.BlockSpec(memory_space=pl.ANY)


def comm_call(body, name, cid, in_specs, out_specs, out_shape, scratch, flops):
    return pl.pallas_call(
        body, name=name, in_specs=in_specs, out_specs=out_specs, out_shape=out_shape, scratch_shapes=scratch,
        compiler_params=pltpu.CompilerParams(collective_id=cid, has_side_effects=True, vmem_limit_bytes=60 * 1024 * 1024),
        cost_estimate=pl.CostEstimate(flops=flops, bytes_accessed=20_000_000, transcendentals=0),
    )


def rs_rows(rows):
    seq, dim = rows.shape

    def body(rows_ref, out_ref, stage, fp, fx, fy, send, recv, load):
        t = lax.axis_index('tp')

        def fetch(i):
            at = pl.ds(pl.multiple_of(xor_bits(t, rs_unit(i)) * SHARD, SHARD), SHARD)
            return pltpu.make_async_copy(rows_ref.at[at, :], stage.at[i], load.at[i])

        for i in range(8):
            fetch(i).start()

        def finish(at, val):
            out_ref[at, :] = val.astype(BF16)

        rs_run(stage, fp, fx, fy, send, recv, lambda i, s: fetch(i).wait(), finish)

    return comm_call(body, 'rs_rows', 0, [ANY], VM, jax.ShapeDtypeStruct((SHARD, dim), BF16), rs_scratch(dim) + [pltpu.SemaphoreType.DMA((8,))], 40_000_000_000)(rows)


def ag_proj(x, w_q, w_dkv):
    dim = x.shape[1]
    seq = 8 * SHARD
    heads, _, qk = w_q.shape
    lat = w_dkv.shape[1]

    def body(x_ref, wq_ref, wl_ref, x_out, q_ref, l_ref, full, send, recv, sem):
        def compute(i, s, h):
            at = half_rows(s, h)
            pltpu.make_async_copy(full.at[at, :], x_out.at[at, :], sem.at[i]).start()
            x_b = full[at, :]
            for hd in range(heads):
                q_ref[hd, at, :] = dot_nn(x_b, wq_ref[hd]).astype(BF16)
            l_ref[at, :] = dot_nn(x_b, wl_ref[...])

        ag_run(x_ref, full, send, recv, compute)
        for i in range(16):
            at = half_rows(i // 2, i % 2)
            pltpu.make_async_copy(full.at[at, :], x_out.at[at, :], sem.at[i]).wait()

    return comm_call(body, 'ag_proj', 1, [VM, VM, VM], [ANY, VM, VM],
                     [jax.ShapeDtypeStruct((seq, dim), BF16), jax.ShapeDtypeStruct((heads, seq, qk), BF16), jax.ShapeDtypeStruct((seq, lat), F32)],
                     [pltpu.VMEM((seq, dim), BF16)] + AG_SEMS + [pltpu.SemaphoreType.DMA((16,))], 40_000_000_000)(x, w_q, w_dkv)


def attn_out_rs(o, w_o):
    dim = w_o.shape[1]

    def body(o_ref, w_ref, out_ref, stage, fp, fx, fy, send, recv):
        def produce(i, s):
            o_b = o_ref[pl.ds(pl.multiple_of(s * SHARD, SHARD), SHARD), :]
            for n in range(dim // 256):
                cols = slice(n * 256, (n + 1) * 256)
                stage[i, :, cols] = dot_nn(o_b, w_ref[:, cols]).astype(BF16)

        def finish(at, val):
            out_ref[at, :] = val.astype(BF16)

        rs_run(stage, fp, fx, fy, send, recv, produce, finish)

    return comm_call(body, 'attn_out_rs', 2, [VM, VM], VM, jax.ShapeDtypeStruct((SHARD, dim), BF16), rs_scratch(dim), 40_000_000_000)(o, w_o)


def col_tiles(width):
    return [slice(a, min(a + 256, width)) for a in range(0, width, 256)]


def ag_mlp(z, dy, w_gate, w_up, w_down):
    dim = z.shape[1]
    seq = 8 * SHARD
    ffn = w_gate.shape[1]
    tiles = col_tiles(ffn)

    def body(z_ref, dy_ref, wg_hbm, wu_hbm, wd_hbm, z_out, hid_out, dg_out, du_out, full, wg, wu, wd, dyb, st, send, recv, zsem, wsem, dsem, osem):
        t = lax.axis_index('tp')
        loads = [pltpu.make_async_copy(a, b, wsem.at[n]) for n, (a, b) in enumerate(((wg_hbm, wg), (wu_hbm, wu), (wd_hbm, wd)))]
        for c in loads:
            c.start()

        def rows_of(i):
            u, h = ag_unit(i)
            return half_rows(xor_bits(t, u), h)

        def dy_copy(i):
            return pltpu.make_async_copy(dy_ref.at[rows_of(i), :], dyb.at[i % 2], dsem.at[i % 2])

        def z_copy(i):
            return pltpu.make_async_copy(full.at[rows_of(i), :], z_out.at[rows_of(i), :], zsem.at[i])

        def out_copies(i):
            return [pltpu.make_async_copy(st.at[n, i % 2], o.at[rows_of(i), :], osem.at[n, i % 2]) for n, o in enumerate((hid_out, dg_out, du_out))]

        dy_copy(0).start()

        def compute(i, s, h):
            @pl.when(i == 0)
            def _():
                for c in loads:
                    c.wait()

            @pl.when(i < 15)
            def _():
                dy_copy(i + 1).start()

            @pl.when(i >= 2)
            def _():
                for c in out_copies(i - 2):
                    c.wait()

            z_copy(i).start()
            dy_copy(i).wait()
            z_b = full[half_rows(s, h), :]
            dy_b = dyb[i % 2]
            for cols in tiles:
                gate = dot_nn(z_b, wg[:, cols])
                up = dot_nn(z_b, wu[:, cols])
                d_hid = dot_nt(dy_b, wd[cols, :])
                sig = jax.nn.sigmoid(gate)
                act = gate * sig
                st[0, i % 2, :, cols] = (act * up).astype(BF16)
                st[1, i % 2, :, cols] = (d_hid * up * sig * (1.0 + gate * (1.0 - sig))).astype(BF16)
                st[2, i % 2, :, cols] = (d_hid * act).astype(BF16)
            for c in out_copies(i):
                c.start()

        ag_run(z_ref, full, send, recv, compute)
        for i in (14, 15):
            for c in out_copies(i):
                c.wait()
        for i in range(16):
            z_copy(i).wait()

    act = jax.ShapeDtypeStruct((seq, ffn), BF16)
    return comm_call(body, 'ag_mlp', 3, [VM, ANY, ANY, ANY, ANY], [ANY] * 4, [jax.ShapeDtypeStruct((seq, dim), BF16), act, act, act],
                     [pltpu.VMEM((seq, dim), BF16), pltpu.VMEM((dim, ffn), BF16), pltpu.VMEM((dim, ffn), BF16), pltpu.VMEM((ffn, dim), BF16),
                      pltpu.VMEM((2, HALF, dim), BF16), pltpu.VMEM((3, 2, HALF, ffn), BF16)] + AG_SEMS
                     + [pltpu.SemaphoreType.DMA((16,)), pltpu.SemaphoreType.DMA((3,)), pltpu.SemaphoreType.DMA((2,)), pltpu.SemaphoreType.DMA((3, 2))],
                     80_000_000_000)(z, dy, w_gate, w_up, w_down)


def mlp_back_rs(d_gate, d_up, w_gate, w_up):
    ffn = d_gate.shape[1]
    dim = w_gate.shape[0]

    def body(dg_ref, du_ref, wg_hbm, wu_hbm, out_ref, stage, fp, fx, fy, send, recv, wg, wu, blk, wsem, bsem):
        t = lax.axis_index('tp')
        loads = [pltpu.make_async_copy(a, b, wsem.at[n]) for n, (a, b) in enumerate(((wg_hbm, wg), (wu_hbm, wu)))]

        def fetch(i):
            at = pl.ds(pl.multiple_of(xor_bits(t, rs_unit(i)) * SHARD, SHARD), SHARD)
            return [pltpu.make_async_copy(r.at[at, :], blk.at[n, i % 2], bsem.at[n, i % 2]) for n, r in enumerate((dg_ref, du_ref))]

        for c in fetch(0) + loads:
            c.start()

        def produce(i, s):
            @pl.when(i < 7)
            def _():
                for c in fetch(i + 1):
                    c.start()

            for c in fetch(i):
                c.wait()

            @pl.when(i == 0)
            def _():
                for c in loads:
                    c.wait()

            dg_b = blk[0, i % 2]
            du_b = blk[1, i % 2]
            for n in range(dim // 256):
                cols = slice(n * 256, (n + 1) * 256)
                stage[i, :, cols] = (dot_nt(dg_b, wg[cols, :]) + dot_nt(du_b, wu[cols, :])).astype(BF16)

        def finish(at, val):
            out_ref[at, :] = val.astype(BF16)

        rs_run(stage, fp, fx, fy, send, recv, produce, finish)

    return comm_call(body, 'mlp_back_rs', 4, [ANY] * 4, VM, jax.ShapeDtypeStruct((SHARD, dim), BF16),
                     rs_scratch(dim) + [pltpu.VMEM((dim, ffn), BF16), pltpu.VMEM((dim, ffn), BF16), pltpu.VMEM((2, 2, SHARD, ffn), BF16),
                                        pltpu.SemaphoreType.DMA((2,)), pltpu.SemaphoreType.DMA((2, 2))], 60_000_000_000)(d_gate, d_up, w_gate, w_up)


def ag_dattn(x, w_o):
    dim = x.shape[1]
    seq = 8 * SHARD
    width = w_o.shape[0]

    def body(x_ref, w_ref, x_out, do_ref, full, send, recv, sem):
        def compute(i, s, h):
            at = half_rows(s, h)
            pltpu.make_async_copy(full.at[at, :], x_out.at[at, :], sem.at[i]).start()
            do_ref[at, :] = dot_nt(full[at, :], w_ref[...]).astype(BF16)

        ag_run(x_ref, full, send, recv, compute)
        for i in range(16):
            at = half_rows(i // 2, i % 2)
            pltpu.make_async_copy(full.at[at, :], x_out.at[at, :], sem.at[i]).wait()

    return comm_call(body, 'ag_dattn', 5, [VM, VM], [ANY, VM], [jax.ShapeDtypeStruct((seq, dim), BF16), jax.ShapeDtypeStruct((seq, width), BF16)],
                     [pltpu.VMEM((seq, dim), BF16)] + AG_SEMS + [pltpu.SemaphoreType.DMA((16,))], 40_000_000_000)(x, w_o)


def attn_back_rs(d_query, d_latent, w_q, w_dkv):
    heads, dim, _ = w_q.shape

    def body(dq_ref, dl_ref, wq_ref, wl_ref, out_ref, stage, fp, fx, fy, send, recv):
        def produce(i, s):
            at = pl.ds(pl.multiple_of(s * SHARD, SHARD), SHARD)
            for n in range(dim // 256):
                cols = slice(n * 256, (n + 1) * 256)
                val = dot_nt(dl_ref[at, :], wl_ref[cols, :])
                for hd in range(heads):
                    val = val + dot_nt(dq_ref[hd, at, :], wq_ref[hd, cols, :])
                stage[i, :, cols] = val.astype(BF16)

        def finish(at, val):
            out_ref[at, :] = val.astype(BF16)

        rs_run(stage, fp, fx, fy, send, recv, produce, finish)

    return comm_call(body, 'attn_back_rs', 6, [VM] * 4, VM, jax.ShapeDtypeStruct((SHARD, dim), BF16), rs_scratch(dim), 40_000_000_000)(d_query, d_latent, w_q, w_dkv)


def gather_seq(x):
    return lax.all_gather(x, 'tp', axis=0, tiled=True)


def scatter_seq(x):
    return lax.psum_scatter(x, 'tp', scatter_dimension=0, tiled=True)


def layer_pass(embedded, d_out, dy_full, w_q, w_dkv, g_kv, w_uk, w_uv, w_o, g_attn, g_mlp, w_gate, w_up, w_down):
    heads, qk = w_q.shape[1:]
    nope = w_uk.shape[2]
    vdim = w_uv.shape[2]
    scale = qk ** -0.5
    w_o2 = w_o.reshape(heads * vdim, -1)
    x_attn_loc, attn_norm_pull = jax.vjp(rms_norm, embedded.astype(F32), g_attn)
    w_q3 = jnp.swapaxes(w_q, 0, 1)
    x_attn, query, latent = ag_proj(x_attn_loc, w_q3, w_dkv)
    seq = x_attn.shape[0]
    cos_t, sin_t = rope_tables(seq, qk - nope)
    (c_kv, k_pe), kv_pull = jax.vjp(kv_prep, latent, g_kv)
    k_nope = matmul_f32('sc,che->hse', c_kv, w_uk).astype(BF16)
    value = matmul_f32('sc,chv->hsv', c_kv, w_uv).astype(BF16)
    q_pe = apply_rope(query[..., nope:].astype(F32), cos_t, sin_t).astype(BF16)
    q_cat = jnp.concatenate([query[..., :nope], q_pe], axis=-1)
    k_cat = jnp.concatenate([k_nope, jnp.broadcast_to(k_pe[None], (heads,) + k_pe.shape)], axis=-1)
    attn_out, lse = attn_fwd(q_cat, k_cat, jnp.swapaxes(value, 1, 2), scale)
    attn_loc = attn_out_rs(attn_out, w_o2)
    residual = (embedded.astype(F32) + attn_loc.astype(F32)).astype(BF16)
    x_mlp_loc, mlp_norm_pull = jax.vjp(rms_norm, residual.astype(F32), g_mlp)
    x_mlp, hidden, d_gate, d_up = ag_mlp(x_mlp_loc, dy_full, w_gate, w_up, w_down)
    mlp_part = matmul_f32('sf,fd->sd', hidden, w_down).astype(BF16)
    mlp_loc = scatter_seq(mlp_part)
    layer_out = (residual.astype(F32) + mlp_loc.astype(F32)).astype(BF16)

    dw_down = matmul_f32('sf,sd->fd', hidden, dy_full)
    dw_gate = matmul_f32('sd,sf->df', x_mlp, d_gate)
    dw_up = matmul_f32('sd,sf->df', x_mlp, d_up)
    dx_mlp = mlp_back_rs(d_gate, d_up, w_gate, w_up)
    d_res_norm, dg_mlp_part = mlp_norm_pull(dx_mlp)
    d_residual = d_out.astype(F32) + d_res_norm
    d_attn_full, d_attn_out = ag_dattn(d_residual.astype(BF16), w_o2)
    dw_o = matmul_f32('sv,sd->vd', attn_out, d_attn_full).reshape(w_o.shape)
    delta = jnp.sum((d_attn_out.astype(F32) * attn_out.astype(F32)).reshape(seq, heads, vdim), axis=-1).T.reshape(heads, 1, seq)
    d_qt, d_k, d_value = attn_bwd(q_cat, k_cat, jnp.swapaxes(k_cat, 1, 2), value, d_attn_out, lse, delta, scale)
    d_q = jnp.swapaxes(d_qt, 1, 2)
    d_query = jnp.concatenate([d_q[..., :nope], unapply_rope(d_q[..., nope:], cos_t, sin_t)], axis=-1).astype(BF16)
    d_knope = d_k[..., :nope].astype(BF16)
    d_kpe = jnp.sum(d_k[..., nope:], axis=0).astype(BF16)
    dw_uk = matmul_f32('sc,hse->che', c_kv, d_knope)
    dw_uv = matmul_f32('sc,hsv->chv', c_kv, d_value)
    d_ckv = (matmul_f32('hse,che->sc', d_knope, w_uk) + matmul_f32('hsv,chv->sc', d_value, w_uv)).astype(BF16)
    d_latent, dg_kv_part = kv_pull((d_ckv, d_kpe))
    d_latent = d_latent.astype(BF16)
    dw_q = matmul_f32('sd,hse->dhe', x_attn, d_query)
    dw_dkv_part = matmul_f32('sd,sc->dc', x_attn, d_latent)
    dx_attn = attn_back_rs(d_query, d_latent, w_q3, w_dkv)
    d_emb_norm, dg_attn_part = attn_norm_pull(dx_attn)
    d_embed = (d_residual + d_emb_norm).astype(BF16)
    dw_dkv, dg_kv, dg_attn, dg_mlp = lax.psum((dw_dkv_part, dg_kv_part, dg_attn_part, dg_mlp_part), 'tp')
    return layer_out, d_embed, (dw_q, dw_dkv, dg_kv, dw_uk, dw_uv, dw_o, dg_attn, dg_mlp, dw_gate, dw_up, dw_down)


def solution(mesh):
    def device_step(tokens, embed_table, w_q, w_dkv, g_kv, w_uk, w_uv, w_o, g_attn, g_mlp, w_gate, w_up, w_down, d_out):
        vocab_local, model_dim = embed_table.shape
        seq = tokens.shape[1]
        dy_loc = d_out[0]
        dy_full = gather_seq(dy_loc)
        local_ids = tokens[0] - lax.axis_index('tp') * vocab_local
        owned = (local_ids >= 0) & (local_ids < vocab_local)
        slots, pos = lax.sort((jnp.where(owned, local_ids, vocab_local), lax.iota(jnp.int32, seq)), num_keys=1)
        slots = jnp.concatenate([slots, jnp.full((128,), vocab_local, jnp.int32)])
        cnt = jnp.sum(owned.astype(jnp.int32)).reshape(1)
        rows = gather_rows(slots, pos, cnt, embed_table, seq)
        embedded = rs_rows(rows)
        layer_out, d_embed, weight_grads = layer_pass(embedded, dy_loc, dy_full, w_q, w_dkv, g_kv, w_uk, w_uv, w_o, g_attn, g_mlp, w_gate, w_up, w_down)
        de_full = gather_seq(d_embed)
        d_table = scatter_rows(slots, pos, cnt, de_full, jnp.zeros((vocab_local, model_dim), BF16))
        return (layer_out[None], d_table) + weight_grads

    row_spec = P('dp', 'tp', None)
    head_spec = P(None, 'tp', None)
    in_specs = (P('dp', None), P('tp', None), head_spec, P(None, None), P(None), head_spec, head_spec, P('tp', None, None), P(None), P(None), P(None, 'tp'), P(None, 'tp'), P('tp', None), row_spec)
    out_specs = (row_spec, P(('dp', 'tp'), None), P('dp', 'tp', None), P('dp', None), P('dp'), P('dp', 'tp', None), P('dp', 'tp', None), P(('dp', 'tp'), None, None), P('dp'), P('dp'), P('dp', 'tp'), P('dp', 'tp'), P(('dp', 'tp'), None))
    return jax.shard_map(device_step, mesh=mesh, in_specs=in_specs, out_specs=out_specs, check_vma=False)
```

```python
import functools

import jax
import jax.numpy as jnp
import numpy as np
from jax import lax
from jax.experimental import pallas as pl
from jax.experimental.pallas import tpu as pltpu
from jax.sharding import PartitionSpec as P

EPSILON = 1e-6
ROPE_BASE = 10000.0
LOG2E = 1.4426950408889634
BLK = 256
RING = 16
F32 = jnp.float32
BF16 = jnp.bfloat16


def matmul_f32(form, lhs, rhs):
    return jnp.einsum(form, lhs, rhs, preferred_element_type=jnp.float32)


def dot_nn(a, b):
    return lax.dot_general(a, b, (((1,), (0,)), ((), ())), preferred_element_type=F32)


def dot_nt(a, b):
    return lax.dot_general(a, b, (((1,), (1,)), ((), ())), preferred_element_type=F32)


def rope_tables(seq_len, rope_dim):
    inv_freq = np.float32(ROPE_BASE) ** (-np.arange(0, rope_dim, 2, dtype=np.float32) / np.float32(rope_dim))
    angles = (np.arange(seq_len, dtype=np.float32)[:, None] * inv_freq[None, :]).astype(np.float64)
    cos, sin = np.cos(angles), np.sin(angles)
    return (jnp.asarray(np.concatenate([cos, cos], axis=1), dtype=F32), jnp.asarray(np.concatenate([-sin, sin], axis=1), dtype=F32))


def swap_halves(x):
    half = x.shape[1] // 2
    return jnp.concatenate([x[:, half:], x[:, :half]], axis=1)


def rope(x, cos_t, sin_t):
    return x * cos_t + swap_halves(x) * sin_t


def unrope(x, cos_t, sin_t):
    return x * cos_t - swap_halves(x) * sin_t


def rms_inv(x):
    return lax.rsqrt(jnp.mean(x * x, axis=-1, keepdims=True) + EPSILON)


def rms_back(x, gain, dy):
    inv = rms_inv(x)
    gd = dy * gain
    mix = jnp.mean(gd * x, axis=-1, keepdims=True)
    return inv * gd - x * (inv * inv * inv * mix), jnp.sum(dy * (x * inv), axis=0, keepdims=True)


def gather_body(slot_ref, pos_ref, cnt_ref, tab_ref, out_ref, buf, acc, sems):
    seq = acc.shape[0]
    cnt = cnt_ref[0]

    def fetch(k):
        blk = pl.multiple_of((slot_ref[k] // 8) * 8, 8)
        return pltpu.make_async_copy(tab_ref.at[pl.ds(blk, 8), :], buf.at[k % RING], sems.at[k % RING])

    def prime(k, c):
        fetch(k).start()
        return c

    lax.fori_loop(0, jnp.minimum(cnt, RING), prime, 0)

    def clear(i, c):
        acc[pl.ds(pl.multiple_of(i * 64, 64), 64), :] = jnp.zeros((64, acc.shape[1]), F32)
        return c

    lax.fori_loop(0, seq // 64, clear, 0)
    rows = lax.broadcasted_iota(jnp.int32, (8, acc.shape[1]), 0)

    def step(k, c):
        fetch(k).wait()
        blk = buf[k % RING].astype(F32)
        row = jnp.sum(jnp.where(rows == slot_ref[k] % 8, blk, 0.0), axis=0, keepdims=True)
        acc[pl.ds(pos_ref[k], 1), :] = row

        @pl.when(k + RING < cnt)
        def _():
            fetch(k + RING).start()

        return c

    lax.fori_loop(0, cnt, step, 0)

    def emit(i, c):
        at = pl.ds(pl.multiple_of(i * 64, 64), 64)
        out_ref[at, :] = acc[at, :].astype(BF16)
        return c

    lax.fori_loop(0, seq // 64, emit, 0)


def gather_rows(slots, pos, cnt, table, seq):
    dim = table.shape[1]
    return pl.pallas_call(
        gather_body,
        grid_spec=pltpu.PrefetchScalarGridSpec(
            num_scalar_prefetch=3,
            grid=(1,),
            in_specs=[pl.BlockSpec(memory_space=pl.ANY)],
            out_specs=pl.BlockSpec((seq, dim), lambda i, *_: (0, 0)),
            scratch_shapes=[pltpu.VMEM((RING, 8, dim), BF16), pltpu.VMEM((seq, dim), F32), pltpu.SemaphoreType.DMA((RING,))],
        ),
        out_shape=jax.ShapeDtypeStruct((seq, dim), BF16),
        compiler_params=pltpu.CompilerParams(vmem_limit_bytes=60 * 1024 * 1024),
        cost_estimate=pl.CostEstimate(flops=20_000_000_000, bytes_accessed=24_000_000, transcendentals=0),
        name="gather_rows",
    )(slots, pos, cnt, table)


def scatter_body(slot_ref, pos_ref, cnt_ref, de_ref, zero_ref, out_ref, wide, acc, stage, sems):
    seq = wide.shape[0]
    cnt = cnt_ref[0]

    def widen(i, c):
        at = pl.ds(pl.multiple_of(i * 64, 64), 64)
        wide[at, :] = de_ref[at, :].astype(F32)
        return c

    lax.fori_loop(0, seq // 64, widen, 0)

    def put(slot_blk, n):
        at = pl.multiple_of(slot_blk * 8, 8)
        return pltpu.make_async_copy(stage.at[n % RING], out_ref.at[pl.ds(at, 8), :], sems.at[n % RING])

    def step(k, carry):
        prev, n = carry
        slot = slot_ref[k]
        blk = slot // 8

        @pl.when(blk != prev)
        def _():
            acc[...] = jnp.zeros_like(acc)

        at = pl.ds(slot % 8, 1)
        acc[at, :] = acc[at, :] + wide[pl.ds(pos_ref[k], 1), :]
        last = slot_ref[k + 1] // 8 != blk

        @pl.when(last)
        def _():
            @pl.when(n >= RING)
            def _():
                put(blk, n).wait()

            stage[n % RING] = acc[...].astype(BF16)
            put(blk, n).start()

        return blk, n + last.astype(jnp.int32)

    _, total = lax.fori_loop(0, cnt, step, (jnp.int32(-1), jnp.int32(0)))

    def drain(i, c):
        put(0, i).wait()
        return c

    lax.fori_loop(jnp.maximum(total - RING, 0), total, drain, 0)


def scatter_rows(slots, pos, cnt, de, zeros):
    seq, dim = de.shape[0], zeros.shape[1]
    return pl.pallas_call(
        scatter_body,
        grid_spec=pltpu.PrefetchScalarGridSpec(
            num_scalar_prefetch=3,
            grid=(1,),
            in_specs=[pl.BlockSpec((seq, dim), lambda i, *_: (0, 0)), pl.BlockSpec(memory_space=pl.ANY)],
            out_specs=pl.BlockSpec(memory_space=pl.ANY),
            scratch_shapes=[pltpu.VMEM((seq, dim), F32), pltpu.VMEM((8, dim), F32), pltpu.VMEM((RING, 8, dim), BF16), pltpu.SemaphoreType.DMA((RING,))],
        ),
        out_shape=jax.ShapeDtypeStruct(zeros.shape, BF16),
        input_output_aliases={4: 0},
        compiler_params=pltpu.CompilerParams(vmem_limit_bytes=60 * 1024 * 1024),
        cost_estimate=pl.CostEstimate(flops=20_000_000_000, bytes_accessed=24_000_000, transcendentals=0),
        name="scatter_rows",
    )(slots, pos, cnt, de, zeros)


def zero_rows(rows, dim, after):
    step = 800

    def body(after_ref, out_ref, blank, sem):
        blank[...] = jnp.zeros_like(blank)
        copies = [pltpu.make_async_copy(blank, out_ref.at[pl.ds(n * step, step), :], sem.at[n]) for n in range(rows // step)]
        for c in copies:
            c.start()
        for c in copies:
            c.wait()

    return pl.pallas_call(
        body,
        in_specs=[pl.BlockSpec(memory_space=pl.ANY)],
        out_specs=pl.BlockSpec(memory_space=pl.ANY),
        out_shape=jax.ShapeDtypeStruct((rows, dim), BF16),
        scratch_shapes=[pltpu.VMEM((step, dim), BF16), pltpu.SemaphoreType.DMA((rows // step,))],
        cost_estimate=pl.CostEstimate(flops=15_000_000_000, bytes_accessed=52_000_000, transcendentals=0),
        name="zero_rows",
    )(after)


def attn_fwd_body(scale2, q_ref, k_ref, vt_ref, o_ref, lse_ref, s_scr):
    seq = q_ref.shape[1]
    tri = lax.broadcasted_iota(jnp.int32, (BLK, BLK), 0) <= lax.broadcasted_iota(jnp.int32, (BLK, BLK), 1)
    for i in range(seq // BLK):
        q_i = q_ref[0, i * BLK:(i + 1) * BLK, :]
        top = None
        for j in range(i + 1):
            s = dot_nt(k_ref[0, j * BLK:(j + 1) * BLK, :], q_i) * scale2
            if j == i:
                s = jnp.where(tri, s, -1e30)
            s_scr[j * BLK:(j + 1) * BLK, :] = s
            part = jnp.max(s.reshape(BLK // 8, 8, BLK), axis=0)
            top = part if top is None else jnp.maximum(top, part)
        top = jnp.max(top, axis=0, keepdims=True)
        den = None
        for j in range(i + 1):
            e = jnp.exp2(s_scr[j * BLK:(j + 1) * BLK, :] - top)
            s_scr[j * BLK:(j + 1) * BLK, :] = e
            part = jnp.sum(e.reshape(BLK // 8, 8, BLK), axis=0)
            den = part if den is None else den + part
        den = jnp.sum(den, axis=0, keepdims=True)
        inv = 1.0 / den
        out = None
        for j in range(i + 1):
            prob = (s_scr[j * BLK:(j + 1) * BLK, :] * inv).astype(BF16)
            part = dot_nn(vt_ref[0, :, j * BLK:(j + 1) * BLK], prob)
            out = part if out is None else out + part
        o_ref[i * BLK:(i + 1) * BLK, :] = out.T.astype(BF16)
        lse_ref[0, :, i * BLK:(i + 1) * BLK] = top + jnp.log2(den)


def attn_fwd(q, k, vt, scale):
    heads, seq, qk = q.shape
    vdim = vt.shape[1]
    return pl.pallas_call(
        functools.partial(attn_fwd_body, scale * LOG2E),
        grid=(heads,),
        in_specs=[pl.BlockSpec((1, seq, qk), lambda h: (h, 0, 0)), pl.BlockSpec((1, seq, qk), lambda h: (h, 0, 0)), pl.BlockSpec((1, vdim, seq), lambda h: (h, 0, 0))],
        out_specs=[pl.BlockSpec((seq, vdim), lambda h: (0, h)), pl.BlockSpec((1, 1, seq), lambda h: (h, 0, 0))],
        out_shape=[jax.ShapeDtypeStruct((seq, heads * vdim), BF16), jax.ShapeDtypeStruct((heads, 1, seq), F32)],
        scratch_shapes=[pltpu.VMEM((seq, BLK), F32)],
        compiler_params=pltpu.CompilerParams(vmem_limit_bytes=40 * 1024 * 1024),
        cost_estimate=pl.CostEstimate(flops=20_000_000_000, bytes_accessed=10_000_000, transcendentals=0),
        name="attn_fwd",
    )(q, k, vt)


def attn_bwd_body(scale2, scale, q_ref, k_ref, kt_ref, v_ref, do_ref, o_ref, lse_ref, cos_ref, sin_ref, dq_ref, dk_ref, dkp_ref, dv_ref, p_scr, ds_scr, dlt):
    seq = q_ref.shape[1]
    nope = dk_ref.shape[2]
    n = seq // BLK
    tri = lax.broadcasted_iota(jnp.int32, (BLK, BLK), 0) <= lax.broadcasted_iota(jnp.int32, (BLK, BLK), 1)
    for i in range(n):
        at_i = slice(i * BLK, (i + 1) * BLK)
        both = do_ref[at_i, :].astype(F32) * o_ref[at_i, :].astype(F32)
        dlt[:, at_i] = jnp.sum(both.T, axis=0, keepdims=True)
    for j in range(n):
        at_j = slice(j * BLK, (j + 1) * BLK)
        k_j = k_ref[0, at_j, :]
        v_j = v_ref[0, at_j, :]
        for i in range(j, n):
            at_i = slice(i * BLK, (i + 1) * BLK)
            s = dot_nt(k_j, q_ref[0, at_i, :])
            prob = jnp.exp2(s * scale2 - lse_ref[0, :, at_i])
            if i == j:
                prob = jnp.where(tri, prob, 0.0)
            dp = dot_nt(v_j, do_ref[at_i, :])
            p_scr[:, at_i] = prob.astype(BF16)
            ds_scr[at_j, at_i] = (prob * (dp - dlt[:, at_i])).astype(BF16)
        dv_ref[0, at_j, :] = dot_nn(p_scr[:, j * BLK:], do_ref[j * BLK:, :]).astype(BF16)
        dk = dot_nn(ds_scr[at_j, j * BLK:], q_ref[0, j * BLK:, :]) * scale
        dk_ref[0, at_j, :] = dk[:, :nope].astype(BF16)
        dkp_ref[0, at_j, :] = dk[:, nope:]
    for i in range(n):
        at_i = slice(i * BLK, (i + 1) * BLK)
        dq = dot_nn(kt_ref[0, :, :(i + 1) * BLK], ds_scr[:(i + 1) * BLK, at_i]) * scale
        half = (dq.shape[0] - nope) // 2
        lo, hi = dq[nope:nope + half, :], dq[nope + half:, :]
        cos_b, sin_b = cos_ref[:, at_i], sin_ref[:, at_i]
        dq_ref[0, :nope, at_i] = dq[:nope, :].astype(BF16)
        dq_ref[0, nope:nope + half, at_i] = (lo * cos_b + hi * sin_b).astype(BF16)
        dq_ref[0, nope + half:, at_i] = (hi * cos_b - lo * sin_b).astype(BF16)


def attn_bwd(q, k, kt, v, do, o, lse, cos_t, sin_t, scale):
    heads, seq, qk = q.shape
    vdim = v.shape[2]
    pe = 2 * cos_t.shape[0]
    per_head = lambda h: (h, 0, 0)
    return pl.pallas_call(
        functools.partial(attn_bwd_body, scale * LOG2E, scale),
        grid=(heads,),
        in_specs=[
            pl.BlockSpec((1, seq, qk), per_head),
            pl.BlockSpec((1, seq, qk), per_head),
            pl.BlockSpec((1, qk, seq), per_head),
            pl.BlockSpec((1, seq, vdim), per_head),
            pl.BlockSpec((seq, vdim), lambda h: (0, h)),
            pl.BlockSpec((seq, vdim), lambda h: (0, h)),
            pl.BlockSpec((1, 1, seq), per_head),
            pl.BlockSpec((pe // 2, seq), lambda h: (0, 0)),
            pl.BlockSpec((pe // 2, seq), lambda h: (0, 0)),
        ],
        out_specs=[pl.BlockSpec((1, qk, seq), per_head), pl.BlockSpec((1, seq, qk - pe), per_head), pl.BlockSpec((1, seq, pe), per_head), pl.BlockSpec((1, seq, vdim), per_head)],
        out_shape=[jax.ShapeDtypeStruct((heads, qk, seq), BF16), jax.ShapeDtypeStruct((heads, seq, qk - pe), BF16), jax.ShapeDtypeStruct((heads, seq, pe), F32), jax.ShapeDtypeStruct((heads, seq, vdim), BF16)],
        scratch_shapes=[pltpu.VMEM((BLK, seq), BF16), pltpu.VMEM((seq, seq), BF16), pltpu.VMEM((1, seq), F32)],
        compiler_params=pltpu.CompilerParams(vmem_limit_bytes=56 * 1024 * 1024),
        cost_estimate=pl.CostEstimate(flops=20_000_000_000, bytes_accessed=16_000_000, transcendentals=0),
        name="attn_bwd",
    )(q, k, kt, v, do, o, lse, cos_t, sin_t)


HALF = 128
SHARD = 256
MESH = pl.DeviceIdType.MESH


def xor_bits(t, u):
    out = 0
    for b in (1, 2, 4):
        tb = (t // b) % 2
        ub = (u // b) % 2
        out = out + b * (tb + ub - 2 * tb * ub)
    return out


def greet(t):
    peers = [xor_bits(t, u) for u in (1, 2, 4)]
    barrier = pltpu.get_barrier_semaphore()
    for peer in peers:
        pl.semaphore_signal(barrier, inc=1, device_id={'tp': peer}, device_id_type=MESH)
    pl.semaphore_wait(barrier, 3)
    return peers


def half_rows(shard, half):
    return pl.ds(pl.multiple_of(shard * SHARD + half * HALF, HALF), HALF)


def ag_unit(i):
    p = i // 4
    r = i % 4
    p0 = (3 - p) // 3
    p3 = p // 3
    mid = 1 - p0 - p3
    u = p0 * (r // 2) + mid * (2 + (r % 2) * 2 + r // 2) + p3 * (6 + r // 2)
    flip = (p - 1) * mid
    return u, (r % 2) + flip * (1 - 2 * (r % 2))


def ag_rows(t, i):
    u, h = ag_unit(i)
    return half_rows(xor_bits(t, u), h)


def ag_run(x_ref, full, send, recv, compute, before=None):
    t = lax.axis_index('tp')
    partner, xn, yn = greet(t)

    def copy(src, shard, half, sem, u_there, dev):
        return pltpu.make_async_remote_copy(
            src_ref=src, dst_ref=full.at[half_rows(shard, half), :], send_sem=send.at[sem],
            recv_sem=recv.at[u_there, half], device_id={'tp': dev}, device_id_type=MESH)

    def mine(half):
        return x_ref.at[pl.ds(half * HALF, HALF), :]

    def held(u, half):
        return full.at[half_rows(xor_bits(t, u), half), :]

    own = [copy(mine(0), t, 0, 0, 2, xn), copy(mine(1), t, 1, 3, 4, yn), copy(mine(0), t, 0, 4, 1, partner), copy(mine(1), t, 1, 5, 1, partner),
           copy(mine(1), t, 1, 1, 2, xn), copy(mine(0), t, 0, 2, 4, yn)]
    for c in own:
        c.start()
    full[pl.ds(pl.multiple_of(t * SHARD, SHARD), SHARD), :] = x_ref[...]
    fwd_y = copy(held(2, 0), xor_bits(t, 2), 0, 6, 6, yn)
    fwd_x = copy(held(4, 1), xor_bits(t, 4), 1, 7, 6, xn)
    fwd_p = {(u, h): copy(held(u, h), xor_bits(t, u), h, 8 + (u - 2) + h, u + 1, partner) for u in (2, 4, 6) for h in (0, 1)}

    def arrive(u, h):
        copy(held(u, h), xor_bits(t, u), h, 0, u, partner).wait_recv()

    def step(i, carry):
        if before is not None:
            before(i)

        @pl.when(i == 1)
        def _():
            arrive(1, 0)
            arrive(1, 1)

        @pl.when(i == 2)
        def _():
            arrive(2, 0)
            fwd_y.start()
            fwd_p[2, 0].start()
            arrive(4, 1)
            fwd_x.start()
            fwd_p[4, 1].start()

        @pl.when(i == 3)
        def _():
            arrive(3, 0)
            arrive(5, 1)

        @pl.when(i == 4)
        def _():
            arrive(2, 1)
            fwd_p[2, 1].start()
            arrive(4, 0)
            fwd_p[4, 0].start()

        @pl.when(i == 5)
        def _():
            arrive(3, 1)
            arrive(5, 0)

        @pl.when(i == 6)
        def _():
            arrive(6, 0)
            fwd_p[6, 0].start()
            arrive(6, 1)
            fwd_p[6, 1].start()

        @pl.when(i == 7)
        def _():
            arrive(7, 0)
            arrive(7, 1)

        compute(i, ag_rows(t, 2 * i), ag_rows(t, 2 * i + 1))
        return carry

    lax.fori_loop(0, 8, step, 0)
    for c in own + [fwd_y, fwd_x] + list(fwd_p.values()):
        c.wait_send()


AG_SEMS = [pltpu.SemaphoreType.DMA((14,)), pltpu.SemaphoreType.DMA((8, 2))]


def rs_run(stage, fp, fx, fy, send, recv, produce, finish, after=None):
    t = lax.axis_index('tp')
    partner, xn, yn = greet(t)

    def copy(src, dst, sem, dev):
        return pltpu.make_async_remote_copy(src_ref=src, dst_ref=dst, send_sem=send.at[sem], recv_sem=recv.at[sem], device_id={'tp': dev}, device_id_type=MESH)

    def half(h):
        return pl.ds(h * HALF, HALF)

    sx = [copy(stage.at[1, half(1), :], fx.at[0], 4, xn), copy(stage.at[3, half(0), :], fx.at[1], 5, xn), copy(stage.at[5, half(0), :], fx.at[2], 6, xn)]
    sy = [copy(stage.at[1, half(0), :], fy.at[0], 7, yn), copy(stage.at[3, half(1), :], fy.at[1], 8, yn), copy(stage.at[5, half(1), :], fy.at[2], 9, yn)]

    def add(i, first, count, src, src_first):
        def body(r, c):
            a = pl.ds(pl.multiple_of(first + r * 32, 32), 32)
            b = pl.ds(pl.multiple_of(src_first + r * 32, 32), 32)
            stage[i, a, :] = (stage[i, a, :].astype(F32) + src[b, :].astype(F32)).astype(BF16)
            return c

        lax.fori_loop(0, count // 32, body, 0)

    def step(i, carry):
        p = i // 2
        produce(i, ag_rows(t, 2 * (7 - i)), ag_rows(t, 2 * (7 - i) + 1))
        to_partner = copy(stage.at[i], fp.at[p], p, partner)

        @pl.when(i % 2 == 0)
        def _():
            to_partner.start()

        @pl.when(i % 2 == 1)
        def _():
            to_partner.wait_recv()
            add(i, 0, SHARD, fp.at[p], 0)

        @pl.when(i == 1)
        def _():
            sx[0].start()
            sy[0].start()

        @pl.when(i == 3)
        def _():
            sx[1].start()
            sy[1].start()

        @pl.when(i == 5)
        def _():
            sy[0].wait_recv()
            add(5, 0, HALF, fy.at[0], 0)
            sx[2].start()
            sx[0].wait_recv()
            add(5, HALF, HALF, fx.at[0], 0)
            sy[2].start()

        if after is not None:
            after(i)
        return carry

    lax.fori_loop(0, 8, step, 0)
    sy[1].wait_recv()
    sx[1].wait_recv()
    sx[2].wait_recv()
    sy[2].wait_recv()

    def last(r, c):
        lo = pl.ds(pl.multiple_of(r * 32, 32), 32)
        hi = pl.ds(pl.multiple_of(HALF + r * 32, 32), 32)
        finish(lo, (stage[7, lo, :].astype(F32) + fy[1, lo, :].astype(F32)) + fx[2, lo, :].astype(F32))
        finish(hi, (stage[7, hi, :].astype(F32) + fx[1, lo, :].astype(F32)) + fy[2, lo, :].astype(F32))
        return c

    lax.fori_loop(0, HALF // 32, last, 0)
    for q in range(4):
        copy(stage.at[2 * q], fp.at[q], q, partner).wait_send()
    for c in sx + sy:
        c.wait_send()


def rs_scratch(dim):
    return [pltpu.VMEM((8, SHARD, dim), BF16), pltpu.VMEM((4, SHARD, dim), BF16), pltpu.VMEM((3, HALF, dim), BF16), pltpu.VMEM((3, HALF, dim), BF16),
            pltpu.SemaphoreType.DMA((10,)), pltpu.SemaphoreType.DMA((10,))]


VM = pl.BlockSpec(memory_space=pltpu.VMEM)
ANY = pl.BlockSpec(memory_space=pl.ANY)


def comm_call(body, name, cid, in_specs, out_specs, out_shape, scratch, flops):
    return pl.pallas_call(
        body, name=name, in_specs=in_specs, out_specs=out_specs, out_shape=out_shape, scratch_shapes=scratch,
        compiler_params=pltpu.CompilerParams(collective_id=cid, has_side_effects=True, vmem_limit_bytes=60 * 1024 * 1024),
        cost_estimate=pl.CostEstimate(flops=flops, bytes_accessed=20_000_000, transcendentals=0),
    )


def rs_rows(rows, gain):
    seq, dim = rows.shape

    def body(rows_ref, g_ref, e_ref, u_ref, stage, fp, fx, fy, send, recv, load):
        t = lax.axis_index('tp')

        def fetch(i):
            return [pltpu.make_async_copy(rows_ref.at[ag_rows(t, 2 * (7 - i) + n), :], stage.at[i, n * HALF:(n + 1) * HALF, :], load.at[i, n]) for n in (0, 1)]

        for i in range(8):
            for c in fetch(i):
                c.start()

        def produce(i, r0, r1):
            for c in fetch(i):
                c.wait()

        def finish(at, val):
            e_b = val.astype(BF16)
            e_ref[at, :] = e_b
            x = e_b.astype(F32)
            u_ref[at, :] = (x * rms_inv(x) * g_ref[...]).astype(BF16)

        rs_run(stage, fp, fx, fy, send, recv, produce, finish)

    loc = jax.ShapeDtypeStruct((SHARD, dim), BF16)
    return comm_call(body, 'rs_rows', 0, [ANY, VM], [VM, VM], [loc, loc], rs_scratch(dim) + [pltpu.SemaphoreType.DMA((8, 2))], 40_000_000_000)(rows, gain)


def ag_proj(x, w_q, w_dkv, g_kv, w_uk, w_uv, cos_t, sin_t):
    dim = x.shape[1]
    seq = 8 * SHARD
    heads, qk, _ = w_q.shape
    lat = w_dkv.shape[0]
    rank, nope = w_uk.shape[1:]
    vdim = w_uv.shape[2]

    def body(x_ref, wq_ref, wl_hbm, g_ref, wk_ref, wv_ref, cos_ref, sin_ref, x_out, q_ref, l_ref, c_ref, k_ref, kt_ref, v_ref, vt_ref, full, send, recv, sem, wl, wsem):
        w_load = pltpu.make_async_copy(wl_hbm, wl, wsem.at[0])
        w_load.start()

        def compute(i, r0, r1):
            @pl.when(i == 0)
            def _():
                w_load.wait()

            x_b = jnp.concatenate([full[r0, :], full[r1, :]], axis=0)
            l_b = dot_nt(x_b, wl[...])
            kv = l_b[:, :rank]
            c_b = (kv * rms_inv(kv) * g_ref[...]).astype(BF16)
            q_all = [dot_nt(x_b, wq_ref[hd]).astype(BF16) for hd in range(heads)]
            k_all = [dot_nn(c_b, wk_ref[hd]) for hd in range(heads)]
            v_all = [dot_nn(c_b, wv_ref[hd]) for hd in range(heads)]
            for n, at in enumerate((r0, r1)):
                part = slice(n * HALF, (n + 1) * HALF)
                pltpu.make_async_copy(full.at[at, :], x_out.at[at, :], sem.at[2 * i + n]).start()
                cos_b = cos_ref[at, :]
                sin_b = sin_ref[at, :]
                l_ref[at, :] = l_b[part, :]
                c_ref[at, :] = c_b[part, :]
                pe = rope(l_b[part, rank:], cos_b, sin_b)
                for hd in range(heads):
                    q_b, k_b, v_b = q_all[hd][part, :], k_all[hd][part, :], v_all[hd][part, :]
                    q_ref[hd, at, :nope] = q_b[:, :nope]
                    q_ref[hd, at, nope:] = rope(q_b[:, nope:].astype(F32), cos_b, sin_b).astype(BF16)
                    k_ref[hd, at, :nope] = k_b.astype(BF16)
                    k_ref[hd, at, nope:] = pe.astype(BF16)
                    kt_ref[hd, :nope, at] = k_b.T.astype(BF16)
                    kt_ref[hd, nope:, at] = pe.T.astype(BF16)
                    v_ref[hd, at, :] = v_b.astype(BF16)
                    vt_ref[hd, :, at] = v_b.T.astype(BF16)

        ag_run(x_ref, full, send, recv, compute)
        for i in range(16):
            at = half_rows(i // 2, i % 2)
            pltpu.make_async_copy(full.at[at, :], x_out.at[at, :], sem.at[i]).wait()

    shapes = [((seq, dim), BF16), ((heads, seq, qk), BF16), ((seq, lat), F32), ((seq, rank), BF16), ((heads, seq, qk), BF16), ((heads, qk, seq), BF16), ((heads, seq, vdim), BF16), ((heads, vdim, seq), BF16)]
    return comm_call(body, 'ag_proj', 1, [VM, VM, ANY] + [VM] * 5, [ANY] + [VM] * 7, [jax.ShapeDtypeStruct(s, d) for s, d in shapes],
                     [pltpu.VMEM((seq, dim), BF16)] + AG_SEMS + [pltpu.SemaphoreType.DMA((16,)), pltpu.VMEM((lat, dim), BF16), pltpu.SemaphoreType.DMA((1,))], 40_000_000_000)(x, w_q, w_dkv, g_kv, w_uk, w_uv, cos_t, sin_t)


def attn_out_rs(o, w_o, e_loc, gain, dy, w_down):
    dim = w_o.shape[1]
    seq = dy.shape[0]
    ffn = w_down.shape[0]
    tiles = col_tiles(ffn)

    def body(o_ref, w_ref, e_ref, g_ref, dy_ref, wd_hbm, h_ref, z_ref, dh_ref, stage, fp, fx, fy, send, recv, wd, dyb, st, wsem, dsem, osem):
        def block(i):
            return pl.ds(pl.multiple_of(i * SHARD, SHARD), SHARD)

        def dy_copy(i):
            return pltpu.make_async_copy(dy_ref.at[block(i), :], dyb.at[i % 2], dsem.at[i % 2])

        def dh_copy(i):
            return pltpu.make_async_copy(st.at[i % 2], dh_ref.at[block(i), :], osem.at[i % 2])

        w_load = pltpu.make_async_copy(wd_hbm, wd, wsem.at[0])
        w_load.start()
        dy_copy(0).start()

        def produce(i, r0, r1):
            o_b = jnp.concatenate([o_ref[r0, :], o_ref[r1, :]], axis=0)
            for n in range(dim // 256):
                cols = slice(n * 256, (n + 1) * 256)
                stage[i, :, cols] = dot_nn(o_b, w_ref[:, cols]).astype(BF16)

        def after(i):
            @pl.when(i == 0)
            def _():
                w_load.wait()

            @pl.when(i < 7)
            def _():
                dy_copy(i + 1).start()

            @pl.when(i >= 2)
            def _():
                dh_copy(i - 2).wait()

            dy_copy(i).wait()
            dy_b = dyb[i % 2]
            for cols in tiles:
                st[i % 2, :, cols] = dot_nt(dy_b, wd[cols, :])
            dh_copy(i).start()

        def finish(at, val):
            h_b = (e_ref[at, :].astype(F32) + val.astype(BF16).astype(F32)).astype(BF16)
            h_ref[at, :] = h_b
            x = h_b.astype(F32)
            z_ref[at, :] = (x * rms_inv(x) * g_ref[...]).astype(BF16)

        rs_run(stage, fp, fx, fy, send, recv, produce, finish, after)
        dh_copy(6).wait()
        dh_copy(7).wait()

    loc = jax.ShapeDtypeStruct((SHARD, dim), BF16)
    return comm_call(body, 'attn_out_rs', 2, [VM] * 4 + [ANY] * 2, [VM, VM, ANY], [loc, loc, jax.ShapeDtypeStruct((seq, ffn), F32)],
                     rs_scratch(dim) + [pltpu.VMEM((ffn, dim), BF16), pltpu.VMEM((2, SHARD, dim), BF16), pltpu.VMEM((2, SHARD, ffn), F32),
                                        pltpu.SemaphoreType.DMA((1,)), pltpu.SemaphoreType.DMA((2,)), pltpu.SemaphoreType.DMA((2,))], 40_000_000_000)(o, w_o, e_loc, gain, dy, w_down)


def col_tiles(width):
    return [slice(a, min(a + 256, width)) for a in range(0, width, 256)]


def ag_mlp(z, dh, w_gate, w_up):
    dim = z.shape[1]
    seq = 8 * SHARD
    ffn = w_gate.shape[0]
    tiles = col_tiles(ffn)

    def body(z_ref, dh_ref, wg_hbm, wu_hbm, z_out, hid_out, dg_out, du_out, full, wg, wu, dhb, st, send, recv, zsem, wsem, dsem, osem):
        t = lax.axis_index('tp')
        loads = [pltpu.make_async_copy(a, b, wsem.at[n]) for n, (a, b) in enumerate(((wg_hbm, wg), (wu_hbm, wu)))]
        for c in loads:
            c.start()

        def dh_copies(i):
            return [pltpu.make_async_copy(dh_ref.at[ag_rows(t, 2 * i + n), :], dhb.at[i % 2, n * HALF:(n + 1) * HALF, :], dsem.at[i % 2, n]) for n in (0, 1)]

        def z_copy(i):
            return pltpu.make_async_copy(full.at[ag_rows(t, i), :], z_out.at[ag_rows(t, i), :], zsem.at[i])

        def out_copies(i):
            return [pltpu.make_async_copy(st.at[n, i % 2, m * HALF:(m + 1) * HALF, :], o.at[ag_rows(t, 2 * i + m), :], osem.at[n, i % 2, m])
                    for n, o in enumerate((hid_out, dg_out, du_out)) for m in (0, 1)]

        for c in dh_copies(0):
            c.start()

        def compute(i, r0, r1):
            @pl.when(i == 0)
            def _():
                for c in loads:
                    c.wait()

            @pl.when(i < 7)
            def _():
                for c in dh_copies(i + 1):
                    c.start()

            @pl.when(i >= 2)
            def _():
                for c in out_copies(i - 2):
                    c.wait()

            z_copy(2 * i).start()
            z_copy(2 * i + 1).start()
            for c in dh_copies(i):
                c.wait()
            z_b = jnp.concatenate([full[r0, :], full[r1, :]], axis=0)
            for cols in tiles:
                gate = dot_nt(z_b, wg[cols, :])
                up = dot_nt(z_b, wu[cols, :])
                d_hid = dhb[i % 2, :, cols]
                sig = jax.nn.sigmoid(gate)
                act = gate * sig
                st[0, i % 2, :, cols] = (act * up).astype(BF16)
                st[1, i % 2, :, cols] = (d_hid * up * sig * (1.0 + gate * (1.0 - sig))).astype(BF16)
                st[2, i % 2, :, cols] = (d_hid * act).astype(BF16)
            for c in out_copies(i):
                c.start()

        ag_run(z_ref, full, send, recv, compute)
        for i in (6, 7):
            for c in out_copies(i):
                c.wait()
        for i in range(16):
            z_copy(i).wait()

    act = jax.ShapeDtypeStruct((seq, ffn), BF16)
    return comm_call(body, 'ag_mlp', 3, [VM, ANY, ANY, ANY], [ANY] * 4, [jax.ShapeDtypeStruct((seq, dim), BF16), act, act, act],
                     [pltpu.VMEM((seq, dim), BF16), pltpu.VMEM((ffn, dim), BF16), pltpu.VMEM((ffn, dim), BF16),
                      pltpu.VMEM((2, SHARD, ffn), F32), pltpu.VMEM((3, 2, SHARD, ffn), BF16)] + AG_SEMS
                     + [pltpu.SemaphoreType.DMA((16,)), pltpu.SemaphoreType.DMA((2,)), pltpu.SemaphoreType.DMA((2, 2)), pltpu.SemaphoreType.DMA((3, 2, 2))],
                     60_000_000_000)(z, dh, w_gate, w_up)


def mlp_back_rs(d_gate, d_up, w_gate, w_up, h_loc, gain, dy):
    ffn, dim = w_gate.shape

    def body(dg_ref, du_ref, wg_hbm, wu_hbm, h_ref, g_ref, dy_ref, res_ref, resb_ref, dgain_ref, stage, fp, fx, fy, send, recv, wg, wu, blk, wsem, bsem):
        t = lax.axis_index('tp')
        loads = [pltpu.make_async_copy(a, b, wsem.at[n]) for n, (a, b) in enumerate(((wg_hbm, wg), (wu_hbm, wu)))]

        def fetch(i):
            return [pltpu.make_async_copy(r.at[ag_rows(t, 2 * (7 - i) + m), :], blk.at[n, i % 2, m * HALF:(m + 1) * HALF, :], bsem.at[n, i % 2, m])
                    for n, r in enumerate((dg_ref, du_ref)) for m in (0, 1)]

        for c in fetch(0) + loads:
            c.start()

        def produce(i, r0, r1):
            @pl.when(i < 7)
            def _():
                for c in fetch(i + 1):
                    c.start()

            for c in fetch(i):
                c.wait()

            @pl.when(i == 0)
            def _():
                for c in loads:
                    c.wait()

            dg_b = blk[0, i % 2]
            du_b = blk[1, i % 2]
            for n in range(dim // 256):
                cols = slice(n * 256, (n + 1) * 256)
                stage[i, :, cols] = (dot_nn(dg_b, wg[:, cols]) + dot_nn(du_b, wu[:, cols])).astype(BF16)

        dgain_ref[...] = jnp.zeros_like(dgain_ref)

        def finish(at, val):
            d_x, d_g = rms_back(h_ref[at, :].astype(F32), g_ref[...], val.astype(BF16).astype(F32))
            dgain_ref[...] = dgain_ref[...] + d_g
            res = dy_ref[at, :].astype(F32) + d_x
            res_ref[at, :] = res
            resb_ref[at, :] = res.astype(BF16)

        rs_run(stage, fp, fx, fy, send, recv, produce, finish)

    loc = lambda d: jax.ShapeDtypeStruct((SHARD, dim), d)
    return comm_call(body, 'mlp_back_rs', 4, [ANY] * 4 + [VM] * 3, [VM] * 3, [loc(F32), loc(BF16), jax.ShapeDtypeStruct((1, dim), F32)],
                     rs_scratch(dim) + [pltpu.VMEM((ffn, dim), BF16), pltpu.VMEM((ffn, dim), BF16), pltpu.VMEM((2, 2, SHARD, ffn), BF16),
                                        pltpu.SemaphoreType.DMA((2,)), pltpu.SemaphoreType.DMA((2, 2, 2))], 60_000_000_000)(d_gate, d_up, w_gate, w_up, h_loc, gain, dy)


def ag_dattn(x, w_o, hidden, w_down):
    dim = x.shape[1]
    seq, ffn = hidden.shape
    width = w_o.shape[0]

    def body(x_ref, w_ref, hid_ref, wd_hbm, x_out, do_ref, y_out, full, send, recv, sem, wd, hb, yb, wsem, hsem, ysem):
        def block(i):
            return pl.ds(pl.multiple_of(i * SHARD, SHARD), SHARD)

        def h_copy(i):
            return pltpu.make_async_copy(hid_ref.at[block(i), :], hb.at[i % 2], hsem.at[i % 2])

        def y_copy(i):
            return pltpu.make_async_copy(yb.at[i % 2], y_out.at[block(i), :], ysem.at[i % 2])

        w_load = pltpu.make_async_copy(wd_hbm, wd, wsem.at[0])
        w_load.start()
        h_copy(0).start()

        def before(i):
            @pl.when(i == 0)
            def _():
                w_load.wait()

            @pl.when(i < 7)
            def _():
                h_copy(i + 1).start()

            @pl.when(i >= 2)
            def _():
                y_copy(i - 2).wait()

            h_copy(i).wait()
            h_b = hb[i % 2]
            for n in range(dim // 256):
                cols = slice(n * 256, (n + 1) * 256)
                yb[i % 2, :, cols] = dot_nn(h_b, wd[:, cols]).astype(BF16)
            y_copy(i).start()

        def compute(i, r0, r1):
            x_b = jnp.concatenate([full[r0, :], full[r1, :]], axis=0)
            d_o = dot_nt(x_b, w_ref[...]).astype(BF16)
            for n, at in enumerate((r0, r1)):
                pltpu.make_async_copy(full.at[at, :], x_out.at[at, :], sem.at[2 * i + n]).start()
                do_ref[at, :] = d_o[n * HALF:(n + 1) * HALF, :]

        ag_run(x_ref, full, send, recv, compute, before)
        y_copy(6).wait()
        y_copy(7).wait()
        for i in range(16):
            at = half_rows(i // 2, i % 2)
            pltpu.make_async_copy(full.at[at, :], x_out.at[at, :], sem.at[i]).wait()

    big = jax.ShapeDtypeStruct((seq, dim), BF16)
    return comm_call(body, 'ag_dattn', 5, [VM, VM, ANY, ANY], [ANY, VM, ANY], [big, jax.ShapeDtypeStruct((seq, width), BF16), big],
                     [pltpu.VMEM((seq, dim), BF16)] + AG_SEMS + [pltpu.SemaphoreType.DMA((16,)), pltpu.VMEM((ffn, dim), BF16), pltpu.VMEM((2, SHARD, ffn), BF16),
                      pltpu.VMEM((2, SHARD, dim), BF16), pltpu.SemaphoreType.DMA((1,)), pltpu.SemaphoreType.DMA((2,)), pltpu.SemaphoreType.DMA((2,))], 40_000_000_000)(x, w_o, hidden, w_down)


def sum_small(x):
    width = x.shape[1]

    def body(x_ref, out_ref, buf, send, recv):
        t = lax.axis_index('tp')
        peers = [xor_bits(t, u) for u in range(1, 8)]
        barrier = pltpu.get_barrier_semaphore()
        for peer in peers:
            pl.semaphore_signal(barrier, inc=1, device_id={'tp': peer}, device_id_type=MESH)
        pl.semaphore_wait(barrier, 7)
        copies = [pltpu.make_async_remote_copy(src_ref=x_ref, dst_ref=buf.at[t], send_sem=send.at[n], recv_sem=recv.at[n], device_id={'tp': peer}, device_id_type=MESH)
                  for n, peer in enumerate(peers)]
        for c in copies:
            c.start()
        buf[t] = x_ref[...]
        for c in copies:
            c.wait()
        total = buf[0]
        for d in range(1, 8):
            total = total + buf[d]
        out_ref[...] = total

    return comm_call(body, 'sum_small', 7, [VM], VM, jax.ShapeDtypeStruct(x.shape, F32),
                     [pltpu.VMEM((8, 1, width), F32), pltpu.SemaphoreType.DMA((7,)), pltpu.SemaphoreType.DMA((7,))], 1_000_000_000)(x)


def attn_back_rs(d_query, d_knope, d_kpe, d_value, latent, g_kv, w_uk, w_uv, w_q, w_dkv, cos_t, sin_t, e_loc, g_attn, d_res):
    heads, _, dim = w_q.shape
    seq, lat = latent.shape
    rank = w_uk.shape[1]
    wide = -(-(dim + lat) // 128) * 128

    def body(dq_ref, dk_ref, dkp_ref, dv_ref, l_ref, gkv_ref, wk_ref, wv_ref, wq_ref, wl_ref, cos_ref, sin_ref, e_ref, g_ref, res_ref,
             de_ref, dgkv_ref, dgain_ref, stage, fp, fx, fy, send, recv):
        dgkv_ref[...] = jnp.zeros_like(dgkv_ref)
        dgain_ref[...] = jnp.zeros_like(dgain_ref)

        def produce(i, r0, r1):
            def both(ref, *lead):
                return jnp.concatenate([ref[lead + (r0, slice(None))], ref[lead + (r1, slice(None))]], axis=0)

            d_c = None
            for hd in range(heads):
                part = dot_nt(both(dk_ref, hd), wk_ref[hd]) + dot_nt(both(dv_ref, hd), wv_ref[hd])
                d_c = part if d_c is None else d_c + part
            d_kv, d_g = rms_back(both(l_ref)[:, :rank], gkv_ref[...], d_c.astype(BF16).astype(F32))
            dgkv_ref[...] = dgkv_ref[...] + d_g
            d_pe = both(dkp_ref, 0)
            for hd in range(1, heads):
                d_pe = d_pe + both(dkp_ref, hd)
            d_pe = unrope(d_pe.astype(BF16).astype(F32), both(cos_ref), both(sin_ref))
            stage[i, :, dim:dim + rank] = d_kv.astype(BF16)
            stage[i, :, dim + rank:dim + lat] = d_pe.astype(BF16)
            stage[i, :, dim + lat:] = jnp.zeros((SHARD, wide - dim - lat), BF16)
            dl_b = stage[i, :, dim:dim + lat]
            dq_b = [jnp.concatenate([dq_ref[hd, :, r].astype(F32).T for r in (r0, r1)], axis=0).astype(BF16) for hd in range(heads)]
            for n in range(dim // 256):
                cols = slice(n * 256, (n + 1) * 256)
                val = dot_nn(dl_b, wl_ref[:, cols])
                for hd in range(heads):
                    val = val + dot_nn(dq_b[hd], wq_ref[hd, :, cols])
                stage[i, :, cols] = val.astype(BF16)

        def finish(at, val):
            d_x, d_g = rms_back(e_ref[at, :].astype(F32), g_ref[...], val[:, :dim].astype(BF16).astype(F32))
            dgain_ref[...] = dgain_ref[...] + d_g
            de_ref[at, :dim] = (res_ref[at, :] + d_x).astype(BF16)
            de_ref[at, dim:] = val[:, dim:].astype(BF16)

        rs_run(stage, fp, fx, fy, send, recv, produce, finish)

    return comm_call(body, 'attn_back_rs', 6, [VM] * 15, [VM] * 3,
                     [jax.ShapeDtypeStruct((SHARD, wide), BF16), jax.ShapeDtypeStruct((1, rank), F32), jax.ShapeDtypeStruct((1, dim), F32)],
                     rs_scratch(wide), 40_000_000_000)(d_query, d_knope, d_kpe, d_value, latent, g_kv, w_uk, w_uv, w_q, w_dkv, cos_t, sin_t, e_loc, g_attn, d_res)


def gather_seq(x):
    return lax.all_gather(x, 'tp', axis=0, tiled=True)


def scatter_seq(x):
    return lax.psum_scatter(x, 'tp', scatter_dimension=0, tiled=True)


def solution(mesh):
    def device_step(tokens, embed_table, w_q, w_dkv, g_kv, w_uk, w_uv, w_o, g_attn, g_mlp, w_gate, w_up, w_down, d_out):
        vocab_local, model_dim = embed_table.shape
        seq = tokens.shape[1]
        heads, qk = w_q.shape[1:]
        vdim = w_uv.shape[2]
        scale = qk ** -0.5
        dy_loc = d_out[0]
        gkv, gat, gml = g_kv.reshape(1, -1), g_attn.reshape(1, -1), g_mlp.reshape(1, -1)
        wuk, wuv = (jnp.swapaxes(w, 0, 1) for w in (w_uk, w_uv))
        wq, wl, wg, wu = jnp.transpose(w_q, (1, 2, 0)), w_dkv.T, w_gate.T, w_up.T
        wo = w_o.reshape(heads * vdim, model_dim)
        cos_t, sin_t = rope_tables(seq, qk - w_uk.shape[2])

        dy_full = gather_seq(dy_loc)
        local_ids = tokens[0] - lax.axis_index('tp') * vocab_local
        owned = (local_ids >= 0) & (local_ids < vocab_local)
        slots, pos = lax.sort((jnp.where(owned, local_ids, vocab_local), lax.iota(jnp.int32, seq)), num_keys=1)
        slots = jnp.concatenate([slots, jnp.full((128,), vocab_local, jnp.int32)])
        cnt = jnp.sum(owned.astype(jnp.int32)).reshape(1)
        rows = gather_rows(slots, pos, cnt, embed_table, seq)
        e_loc, u_loc = rs_rows(rows, gat)
        u, q, latent, c_kv, k, kt, v, vt = ag_proj(u_loc, wq, wl, gkv, wuk, wuv, cos_t, sin_t)
        o, lse = attn_fwd(q, k, vt, scale)
        h_loc, z_loc, d_hidden = attn_out_rs(o, wo, e_loc, gml, dy_full, w_down)
        z, hidden, d_gate, d_up = ag_mlp(z_loc, d_hidden, wg, wu)
        d_res, d_res_b, dg_mlp = mlp_back_rs(d_gate, d_up, wg, wu, h_loc, gml, dy_loc)
        d_res_full, d_o, mlp_part = ag_dattn(d_res_b, wo, hidden, w_down)

        mlp_loc = scatter_seq(mlp_part)
        half = cos_t.shape[1] // 2
        d_query, d_knope, d_kpe, d_value = attn_bwd(q, k, kt, v, d_o, o, lse, cos_t[:, :half].T, sin_t[:, half:].T, scale)
        dw_gate = matmul_f32('sd,sf->df', z, d_gate)
        dw_up = matmul_f32('sd,sf->df', z, d_up)
        dw_gate, dw_up, mlp_loc, d_query = lax.optimization_barrier((dw_gate, dw_up, mlp_loc, d_query))
        layer_out = (h_loc.astype(F32) + mlp_loc.astype(F32)).astype(BF16)
        back, dg_kv, dg_attn = attn_back_rs(d_query, d_knope, d_kpe, d_value, latent, gkv, wuk, wuv, wq, wl, cos_t, sin_t, e_loc, gat, d_res)

        back_full = gather_seq(back)
        dw_down = matmul_f32('sf,sd->fd', hidden, dy_full)
        dw_q = matmul_f32('sd,hes->dhe', u, d_query)
        dw_uk = matmul_f32('sc,hse->che', c_kv, d_knope)
        dw_uv = matmul_f32('sc,hsv->chv', c_kv, d_value)
        dw_o = matmul_f32('sv,sd->vd', o, d_res_full).reshape(w_o.shape)
        gains = sum_small(jnp.concatenate([dg_kv, dg_attn, dg_mlp], axis=1))[0]
        zeros = zero_rows(vocab_local, model_dim, back)
        back_full, dw_down, dw_q, dw_uk, dw_uv, dw_o, gains, zeros = lax.optimization_barrier((back_full, dw_down, dw_q, dw_uk, dw_uv, dw_o, gains, zeros))
        dw_dkv = matmul_f32('sd,sc->dc', u, back_full[:, model_dim:model_dim + w_dkv.shape[1]])
        d_table = scatter_rows(slots, pos, cnt, back_full, zeros)
        rank = g_kv.shape[0]
        dg_kv, dg_attn, dg_mlp = gains[:rank], gains[rank:rank + model_dim], gains[rank + model_dim:]
        return layer_out[None], d_table, dw_q, dw_dkv, dg_kv, dw_uk, dw_uv, dw_o, dg_attn, dg_mlp, dw_gate, dw_up, dw_down

    row_spec = P('dp', 'tp', None)
    head_spec = P(None, 'tp', None)
    in_specs = (P('dp', None), P('tp', None), head_spec, P(None, None), P(None), head_spec, head_spec, P('tp', None, None), P(None), P(None), P(None, 'tp'), P(None, 'tp'), P('tp', None), row_spec)
    out_specs = (row_spec, P(('dp', 'tp'), None), P('dp', 'tp', None), P('dp', None), P('dp'), P('dp', 'tp', None), P('dp', 'tp', None), P(('dp', 'tp'), None, None), P('dp'), P('dp'), P('dp', 'tp'), P('dp', 'tp'), P(('dp', 'tp'), None))
    return jax.shard_map(device_step, mesh=mesh, in_specs=in_specs, out_specs=out_specs, check_vma=False)
```

```python
import functools

import jax
import jax.numpy as jnp
import numpy as np
from jax import lax
from jax.experimental import pallas as pl
from jax.experimental.pallas import tpu as pltpu
from jax.sharding import PartitionSpec as P

EPSILON = 1e-6
ROPE_BASE = 10000.0
LOG2E = 1.4426950408889634
BLK = 256
RING = 16
LANES = 128
ROWS = 64
VMEM_CAP = 60 * 1024 * 1024
BUSY = 40_000_000_000
NEG = -1e30
F32 = jnp.float32
BF16 = jnp.bfloat16


def matmul_f32(form, lhs, rhs):
    return jnp.einsum(form, lhs, rhs, preferred_element_type=jnp.float32)


def dot_nn(a, b):
    return jnp.dot(a, b, preferred_element_type=F32)


def dot_nt(a, b):
    return lax.dot_general(a, b, (((1,), (1,)), ((), ())), preferred_element_type=F32)


def tile(i):
    return slice(i * BLK, (i + 1) * BLK)


def rows_at(first, count):
    return pl.ds(pl.multiple_of(first, count), count)


def sems(*shape):
    return pltpu.SemaphoreType.DMA(shape)


def loop(count, step):
    def body(i, carry):
        step(i)
        return carry

    lax.fori_loop(0, count, body, 0)


VM = pl.BlockSpec(memory_space=pltpu.VMEM)
ANY = pl.BlockSpec(memory_space=pl.ANY)


def rope_tables(seq_len, rope_dim):
    inv_freq = np.float32(ROPE_BASE) ** (-np.arange(0, rope_dim, 2, dtype=np.float32) / np.float32(rope_dim))
    angles = (np.arange(seq_len, dtype=np.float32)[:, None] * inv_freq[None, :]).astype(np.float64)
    cos, sin = np.cos(angles), np.sin(angles)
    return (jnp.asarray(np.concatenate([cos, cos], axis=1), dtype=F32), jnp.asarray(np.concatenate([-sin, sin], axis=1), dtype=F32))


def swap_halves(x):
    half = x.shape[1] // 2
    return jnp.concatenate([x[:, half:], x[:, :half]], axis=1)


def rope(x, cos_t, sin_t):
    return x * cos_t + swap_halves(x) * sin_t


def unrope(x, cos_t, sin_t):
    return x * cos_t - swap_halves(x) * sin_t


def rms_inv(x):
    return lax.rsqrt(jnp.mean(x * x, axis=-1, keepdims=True) + EPSILON)


def rms_back(x, gain, dy):
    inv = rms_inv(x)
    gd = dy * gain
    mix = jnp.mean(gd * x, axis=-1, keepdims=True)
    return inv * gd - x * (inv * inv * inv * mix), jnp.sum(dy * (x * inv), axis=0, keepdims=True)


def gather_body(slot_ref, pos_ref, cnt_ref, tab_ref, out_ref, buf, acc, sem):
    seq, dim = acc.shape
    cnt = cnt_ref[0]

    def fetch(k):
        return pltpu.make_async_copy(tab_ref.at[rows_at(slot_ref[k] // 8 * 8, 8), :], buf.at[k % RING], sem.at[k % RING])

    loop(jnp.minimum(cnt, RING), lambda k: fetch(k).start())

    def clear(i):
        acc[rows_at(i * ROWS, ROWS), :] = jnp.zeros((ROWS, dim), F32)

    loop(seq // ROWS, clear)
    rows = lax.broadcasted_iota(jnp.int32, buf.shape[1:], 0)

    def step(k):
        fetch(k).wait()
        picked = jnp.where(rows == slot_ref[k] % 8, buf[k % RING].astype(F32), 0.0)
        acc[pl.ds(pos_ref[k], 1), :] = jnp.sum(picked, axis=0, keepdims=True)

        @pl.when(k + RING < cnt)
        def _():
            fetch(k + RING).start()

    loop(cnt, step)

    def emit(i):
        at = rows_at(i * ROWS, ROWS)
        out_ref[at, :] = acc[at, :].astype(BF16)

    loop(seq // ROWS, emit)


def local_call(body, name, out, in_specs, out_specs, scratch, scalars=0, grid=(1,), **extra):
    return pl.pallas_call(
        body, name=name, out_shape=out,
        grid_spec=pltpu.PrefetchScalarGridSpec(num_scalar_prefetch=scalars, grid=grid, in_specs=in_specs, out_specs=out_specs, scratch_shapes=scratch),
        compiler_params=pltpu.CompilerParams(vmem_limit_bytes=VMEM_CAP),
        cost_estimate=pl.CostEstimate(flops=BUSY // 2, bytes_accessed=BUSY // 2000, transcendentals=0), **extra)


def whole(*shape):
    return pl.BlockSpec(shape, lambda i, *_: (0,) * len(shape))


def gather_rows(slots, pos, cnt, table, seq):
    dim = table.shape[1]
    return local_call(gather_body, 'gather_rows', jax.ShapeDtypeStruct((seq, dim), BF16), [ANY], whole(seq, dim),
                      [pltpu.VMEM((RING, 8, dim), BF16), pltpu.VMEM((seq, dim), F32), sems(RING)], 3)(slots, pos, cnt, table)


def scatter_body(slot_ref, pos_ref, cnt_ref, de_ref, zero_ref, out_ref, wide, acc, stage, sem, near, nsem):
    seq, dim = wide.shape

    def load(i):
        at = rows_at(i * BLK, BLK)
        return pltpu.make_async_copy(de_ref.at[at, pl.ds(0, dim)], near.at[at, :], nsem.at[i])

    loop(seq // BLK, lambda i: load(i).start())

    def widen(i):
        load(i).wait()
        at = rows_at(i * BLK, BLK)
        wide[at, :] = near[at, :].astype(F32)

    loop(seq // BLK, widen)

    def put(blk, n):
        return pltpu.make_async_copy(stage.at[n % RING], out_ref.at[rows_at(blk * 8, 8), :], sem.at[n % RING])

    def step(k, carry):
        prev, n = carry
        slot = slot_ref[k]
        blk = slot // 8

        @pl.when(blk != prev)
        def _():
            acc[...] = jnp.zeros_like(acc)

        at = pl.ds(slot % 8, 1)
        acc[at, :] = acc[at, :] + wide[pl.ds(pos_ref[k], 1), :]
        last = slot_ref[k + 1] // 8 != blk

        @pl.when(last)
        def _():
            @pl.when(n >= RING)
            def _():
                put(blk, n).wait()

            stage[n % RING] = acc[...].astype(BF16)
            put(blk, n).start()

        return blk, n + last.astype(jnp.int32)

    _, total = lax.fori_loop(0, cnt_ref[0], step, (jnp.int32(-1), jnp.int32(0)))
    loop(jnp.minimum(total, RING), lambda i: put(0, total - 1 - i).wait())


def scatter_rows(slots, pos, cnt, de, zeros):
    seq, dim = de.shape[0], zeros.shape[1]
    return local_call(scatter_body, 'scatter_rows', jax.ShapeDtypeStruct(zeros.shape, BF16), [ANY, ANY], ANY,
                      [pltpu.VMEM((seq, dim), F32), pltpu.VMEM((8, dim), F32), pltpu.VMEM((RING, 8, dim), BF16), sems(RING), pltpu.VMEM((seq, dim), BF16), sems(seq // BLK)], 3, input_output_aliases={4: 0})(slots, pos, cnt, de, zeros)


def causal_tile():
    shape = (BLK, BLK)
    return lax.broadcasted_iota(jnp.int32, shape, 0) <= lax.broadcasted_iota(jnp.int32, shape, 1)


def fold(op, parts):
    total = functools.reduce(lambda a, b: a + b if op is jnp.sum else jnp.maximum(a, b), parts)
    return op(total, axis=0, keepdims=True)


def by_eight(op, x):
    return op(x.reshape(-1, 8, BLK), axis=0)


def attn_fwd_body(scale2, q_ref, k_ref, vt_ref, o_ref, lse_ref, s_scr):
    tri = causal_tile()
    for i in range(q_ref.shape[1] // BLK):
        q_i = q_ref[0, tile(i), :]
        tops = []
        for j in range(i + 1):
            s = dot_nt(k_ref[0, tile(j), :], q_i) * scale2
            if j == i:
                s = jnp.where(tri, s, NEG)
            s_scr[tile(j), :] = s
            tops.append(by_eight(jnp.max, s))
        top = fold(jnp.max, tops)
        dens = []
        for j in range(i + 1):
            e = jnp.exp2(s_scr[tile(j), :] - top)
            s_scr[tile(j), :] = e
            dens.append(by_eight(jnp.sum, e))
        den = fold(jnp.sum, dens)
        inv = 1.0 / den
        out = [dot_nn(vt_ref[0, :, tile(j)], (s_scr[tile(j), :] * inv).astype(BF16)) for j in range(i + 1)]
        o_ref[tile(i), :] = functools.reduce(jnp.add, out).T.astype(BF16)
        lse_ref[0, :, tile(i)] = top + jnp.log2(den)


def per_head(*shape):
    return pl.BlockSpec((1,) + shape, lambda h: (h, 0, 0))


def head_cols(seq, width):
    return pl.BlockSpec((seq, width), lambda h: (0, h))


def attn_fwd(q, k, vt, scale):
    heads, seq, qk = q.shape
    vdim = vt.shape[1]
    return local_call(functools.partial(attn_fwd_body, scale * LOG2E), 'attn_fwd',
                      [jax.ShapeDtypeStruct((seq, heads * vdim), BF16), jax.ShapeDtypeStruct((heads, 1, seq), F32)],
                      [per_head(seq, qk), per_head(seq, qk), per_head(vdim, seq)], [head_cols(seq, vdim), per_head(1, seq)],
                      [pltpu.VMEM((seq, BLK), F32)], grid=(heads,))(q, k, vt)


def attn_bwd_body(scale2, scale, q_ref, k_ref, kt_ref, v_ref, do_ref, o_ref, lse_ref, cos_ref, sin_ref, dq_ref, dk_ref, dkp_ref, dv_ref, zero_ref, p_scr, ds_scr, dlt, blank, zsem):
    seq = q_ref.shape[1]
    nope = dk_ref.shape[2]
    n = seq // BLK
    head = pl.program_id(0)
    size = blank.shape[0]
    fills = [pltpu.make_async_copy(blank, zero_ref.at[pl.ds(m * size, size), :], zsem.at[m]) for m in range(zsem.shape[0])]

    @pl.when(head == 0)
    def _():
        blank[...] = jnp.zeros_like(blank)
        for c in fills:
            c.start()

    tri = causal_tile()
    for i in range(n):
        both = do_ref[tile(i), :].astype(F32) * o_ref[tile(i), :].astype(F32)
        dlt[:, tile(i)] = jnp.sum(both.T, axis=0, keepdims=True)
    for j in range(n):
        k_j = k_ref[0, tile(j), :]
        v_j = v_ref[0, tile(j), :]
        for i in range(j, n):
            s = dot_nt(k_j, q_ref[0, tile(i), :])
            prob = jnp.exp2(s * scale2 - lse_ref[0, :, tile(i)])
            if i == j:
                prob = jnp.where(tri, prob, 0.0)
            dp = dot_nt(v_j, do_ref[tile(i), :])
            p_scr[:, tile(i)] = prob.astype(BF16)
            ds_scr[tile(j), tile(i)] = (prob * (dp - dlt[:, tile(i)])).astype(BF16)
        rest = slice(j * BLK, seq)
        dv_ref[0, tile(j), :] = dot_nn(p_scr[:, rest], do_ref[rest, :]).astype(BF16)
        dk = dot_nn(ds_scr[tile(j), rest], q_ref[0, rest, :]) * scale
        dk_ref[0, tile(j), :] = dk[:, :nope].astype(BF16)
        dkp_ref[0, tile(j), :] = dk[:, nope:]

    half = cos_ref.shape[0]
    for i in range(n):
        seen = slice(0, (i + 1) * BLK)
        dq = dot_nn(kt_ref[0, :, seen], ds_scr[seen, tile(i)]) * scale
        lo, hi = dq[nope:nope + half, :], dq[nope + half:, :]
        cos_b, sin_b = cos_ref[:, tile(i)], sin_ref[:, tile(i)]
        turned = jnp.concatenate([dq[:nope, :], lo * cos_b + hi * sin_b, hi * cos_b - lo * sin_b], axis=0)
        dq_ref[0, tile(i), :] = turned.T.astype(BF16)

    @pl.when(head == pl.num_programs(0) - 1)
    def _():
        for c in fills:
            c.wait()


def attn_bwd(q, k, kt, v, do, o, lse, cos_t, sin_t, scale, table):
    heads, seq, qk = q.shape
    vdim = v.shape[2]
    half = cos_t.shape[0]
    pe = half + half
    outs = [((seq, qk), BF16), ((seq, qk - pe), BF16), ((seq, pe), F32), ((seq, vdim), BF16)]
    return local_call(functools.partial(attn_bwd_body, scale * LOG2E, scale), 'attn_bwd', [jax.ShapeDtypeStruct((heads,) + s, d) for s, d in outs] + [jax.ShapeDtypeStruct(table, BF16)],
                      [per_head(seq, qk), per_head(seq, qk), per_head(qk, seq), per_head(seq, vdim), head_cols(seq, vdim), head_cols(seq, vdim), per_head(1, seq), whole(half, seq), whole(half, seq)],
                      [per_head(*s) for s, _ in outs] + [ANY],
                      [pltpu.VMEM((BLK, seq), BF16), pltpu.VMEM((seq, seq), BF16), pltpu.VMEM((1, seq), F32), pltpu.VMEM((table[0] // RING,) + table[1:], BF16), sems(RING)],
                      grid=(heads,))(q, k, kt, v, do, o, lse, cos_t, sin_t)


HALF = 128
SHARD = 256
STEPS = 8
MESH = pl.DeviceIdType.MESH


def xor_bits(t, u):
    out = 0
    for b in (1, 2, 4):
        tb = (t // b) % 2
        ub = (u // b) % 2
        out = out + b * (tb + ub - 2 * tb * ub)
    return out


def greet(t, others):
    peers = [xor_bits(t, u) for u in others]
    barrier = pltpu.get_barrier_semaphore()
    for peer in peers:
        pl.semaphore_signal(barrier, inc=1, device_id={'tp': peer}, device_id_type=MESH)
    pl.semaphore_wait(barrier, len(peers))
    return peers


def send_to(src, dst, send, recv, dev):
    return pltpu.make_async_remote_copy(src_ref=src, dst_ref=dst, send_sem=send, recv_sem=recv, device_id={'tp': dev}, device_id_type=MESH)


def piece_id(m, j):
    i = 2 * m + j // 2
    p, r = i // 4, i % 4
    first, last = (3 - p) // 3, p // 3
    mid = 1 - first - last
    u = first * (r // 2) + mid * (2 + (r % 2) * 2 + r // 2)
    h = r % 2 + (p - 1) * mid * (1 - 2 * (r % 2))
    near = 1 - last
    return u + last * (6 + j // 2), near * h + last * (j % 2), near * (j % 2) + last * (m % 2)


def piece(t, m, j):
    u, h, a = piece_id(m, j)
    return rows_at(xor_bits(t, u) * SHARD + h * HALF + a * ROWS, ROWS)


def pieces(t, m):
    return [piece(t, m, j) for j in range(4)]


def quarter(j):
    return pl.ds(j * ROWS, ROWS)


def join(ref, at, *lead):
    return jnp.concatenate([ref[lead + (r, slice(None))] for r in at], axis=0)


def begin(i, loads, ins, outs):
    @pl.when(i == 0)
    def _():
        for c in loads:
            c.wait()

    @pl.when(i < STEPS - 1)
    def _():
        for c in ins(i + 1):
            c.start()

    @pl.when(i >= 2)
    def _():
        for c in outs(i - 2):
            c.wait()

    for c in ins(i):
        c.wait()


def finish_all(outs):
    for i in (STEPS - 2, STEPS - 1):
        for c in outs(i):
            c.wait()


def ag_run(x_ref, full, send, recv, compute, before=None):
    t = lax.axis_index('tp')
    partner, xn, yn = greet(t, (1, 2, 4))
    sends = []

    def copy(src, shard, first, count, u_there, dev):
        place = rows_at(shard * SHARD + first, count)
        slot = first // ROWS
        c = send_to(src, full.at[place, :], send.at[len(sends)], recv.at[u_there, slot], dev)
        sends.append(c)
        return c

    def mine(h, u, dev):
        return copy(x_ref.at[pl.ds(h * HALF, HALF), :], t, h * HALF, HALF, u, dev)

    def relay(u, first, count, u_there, dev):
        shard = xor_bits(t, u)
        return copy(full.at[rows_at(shard * SHARD + first, count), :], shard, first, count, u_there, dev)

    for h, u, dev in ((0, 2, xn), (1, 4, yn), (0, 1, partner), (1, 1, partner), (1, 2, xn), (0, 4, yn)):
        mine(h, u, dev).start()
    full[rows_at(t * SHARD, SHARD), :] = x_ref[...]
    onward = {(u, h): [relay(u, h * HALF, HALF, u + 1, partner)] for u in (2, 4) for h in (0, 1)}
    for a in (0, 1):
        onward[2, 0].append(relay(2, a * ROWS, ROWS, 6, yn))
        onward[4, 1].append(relay(4, HALF + a * ROWS, ROWS, 6, xn))
    far = {(h, a): relay(6, h * HALF + a * ROWS, ROWS, 7, partner) for h in (0, 1) for a in (0, 1)}

    def arrive(u, first, count):
        place = full.at[rows_at(xor_bits(t, u) * SHARD + first, count), :]
        send_to(place, place, send.at[0], recv.at[u, first // ROWS], partner).wait_recv()

    def step(i):
        if before is not None:
            before(i)
        for m in range(1, 6):
            @pl.when(i == m)
            def _(m=m):
                for j in (0, 2):
                    u, h, _ = piece_id(m, j)
                    arrive(u, h * HALF, HALF)
                    for c in onward.get((u, h), ()):
                        c.start()

        for a in (0, 1):
            @pl.when(i == 6 + a)
            def _(a=a):
                for h in (0, 1):
                    arrive(6, h * HALF + a * ROWS, ROWS)
                    far[h, a].start()
                for h in (0, 1):
                    arrive(7, h * HALF + a * ROWS, ROWS)

        compute(i, pieces(t, i))

    loop(STEPS, step)
    for c in sends:
        c.wait_send()


AG_SEMS = [sems(18), sems(8, 4)]


def rs_run(stage, fp, fx, fy, send, recv, produce, finish, after=None, others=(1, 2, 4)):
    t = lax.axis_index('tp')
    partner, xn, yn, *_ = greet(t, others)
    sends = []

    def copy(src, dst, dev):
        n = len(sends)
        c = send_to(src, dst, send.at[n], recv.at[n], dev)
        sends.append(c)
        return c

    first, second = pl.ds(0, HALF), pl.ds(HALF, HALF)
    swap = [copy(stage.at[k, second, :], fp.at[0, pl.ds(k * HALF, HALF), :], partner) for k in (0, 1)]
    swap += [copy(stage.at[2 * p], fp.at[p], partner) for p in (1, 2, 3)]
    far_y = [copy(stage.at[k, quarter(0), :], fy.at[0, quarter(1 - k), :], yn) for k in (0, 1)]
    far_x = [copy(stage.at[k, quarter(1), :], fx.at[0, quarter(1 - k), :], xn) for k in (0, 1)]
    near_x, near_y = copy(stage.at[3, first, :], fx.at[1], xn), copy(stage.at[3, second, :], fy.at[1], yn)
    via_x, via_y = copy(stage.at[5, first, :], fx.at[2], xn), copy(stage.at[5, second, :], fy.at[2], yn)

    def add(i, start, count, src, src_start):
        def body(r):
            a = rows_at(start + r * 32, 32)
            stage[i, a, :] = (stage[i, a, :].astype(F32) + src[rows_at(src_start + r * 32, 32), :].astype(F32)).astype(BF16)

        loop(count // 32, body)

    def step(i):
        produce(i, pieces(t, STEPS - 1 - i))
        for k in (0, 1):
            @pl.when(i == k)
            def _(k=k):
                swap[k].start()
                swap[k].wait_recv()
                add(k, 0, HALF, fp.at[0], k * HALF)
                far_x[k].start()
                far_y[k].start()

        for p in (1, 2, 3):
            @pl.when(i == 2 * p)
            def _(p=p):
                swap[p + 1].start()

            @pl.when(i == 2 * p + 1)
            def _(p=p):
                swap[p + 1].wait_recv()
                add(2 * p + 1, 0, SHARD, fp.at[p], 0)

        @pl.when(i == 3)
        def _():
            near_x.start()
            near_y.start()

        @pl.when(i == 5)
        def _():
            for c in far_y:
                c.wait_recv()
            add(5, 0, HALF, fy.at[0], 0)
            via_x.start()
            for c in far_x:
                c.wait_recv()
            add(5, HALF, HALF, fx.at[0], 0)
            via_y.start()

        if after is not None:
            @pl.when(i >= 1)
            def _():
                after(i - 1)

    loop(STEPS, step)
    if after is not None:
        after(STEPS - 1)
    for c in (near_x, near_y, via_x, via_y):
        c.wait_recv()

    def last(r):
        lo, hi = rows_at(r * 32, 32), rows_at(HALF + r * 32, 32)
        finish(lo, (stage[7, lo, :].astype(F32) + fy[1, lo, :].astype(F32)) + fx[2, lo, :].astype(F32))
        finish(hi, (stage[7, hi, :].astype(F32) + fx[1, lo, :].astype(F32)) + fy[2, lo, :].astype(F32))

    loop(HALF // 32, last)
    for c in sends:
        c.wait_send()


def rs_scratch(dim):
    return [pltpu.VMEM((n, rows, dim), BF16) for n, rows in ((STEPS, SHARD), (4, SHARD), (3, HALF), (3, HALF))] + [sems(13), sems(13)]


def comm_call(body, name, cid, in_specs, out_specs, out_shape, scratch):
    return pl.pallas_call(
        body, name=name, in_specs=in_specs, out_specs=out_specs, out_shape=out_shape, scratch_shapes=scratch,
        compiler_params=pltpu.CompilerParams(collective_id=cid, has_side_effects=True, vmem_limit_bytes=VMEM_CAP),
        cost_estimate=pl.CostEstimate(flops=BUSY, bytes_accessed=BUSY // 2000, transcendentals=0))


def col_tiles(width):
    return [slice(a, min(a + BLK, width)) for a in range(0, width, BLK)]


def struct(dtype, *shape):
    return jax.ShapeDtypeStruct(shape, dtype)


def back_rms_rows(x_ref, g_ref, dgain_ref, at, dy):
    d_x, d_g = rms_back(x_ref[at, :].astype(F32), g_ref[...], dy.astype(BF16).astype(F32))
    dgain_ref[...] = dgain_ref[...] + d_g
    return d_x


def rs_rows(rows, gain):
    dim = rows.shape[1]

    def body(rows_ref, g_ref, e_ref, u_ref, stage, fp, fx, fy, send, recv, load):
        t = lax.axis_index('tp')

        def fetch(i):
            return [pltpu.make_async_copy(rows_ref.at[at, :], stage.at[i, quarter(j), :], load.at[i, j]) for j, at in enumerate(pieces(t, STEPS - 1 - i))]

        for i in range(STEPS):
            for c in fetch(i):
                c.start()

        def produce(i, at):
            for c in fetch(i):
                c.wait()

        def finish(at, val):
            e_b = val.astype(BF16)
            e_ref[at, :] = e_b
            x = e_b.astype(F32)
            u_ref[at, :] = (x * rms_inv(x) * g_ref[...]).astype(BF16)

        rs_run(stage, fp, fx, fy, send, recv, produce, finish)

    loc = struct(BF16, SHARD, dim)
    return comm_call(body, 'rs_rows', 0, [ANY, VM], [VM, VM], [loc, loc], rs_scratch(dim) + [sems(STEPS, 4)])(rows, gain)


def ag_proj(x, w_q, w_dkv, g_kv, w_uk, w_uv, cos_t, sin_t):
    seq = cos_t.shape[0]
    heads, qk, dim = w_q.shape
    lat = w_dkv.shape[0]
    rank, nope = w_uk.shape[1:]
    vdim = w_uv.shape[2]

    def body(x_ref, wq_ref, wl_hbm, g_ref, wk_ref, wv_ref, cos_ref, sin_ref, x_out, q_ref, l_ref, c_ref, k_ref, kt_ref, v_ref, vt_ref, full, send, recv, sem, wl, wsem):
        t = lax.axis_index('tp')
        w_load = pltpu.make_async_copy(wl_hbm, wl, wsem)
        w_load.start()

        def x_copies(i):
            return [pltpu.make_async_copy(full.at[at, :], x_out.at[at, :], sem.at[i, j]) for j, at in enumerate(pieces(t, i))]

        def turn(m, j):
            u, h, _ = piece_id(m, j)
            at = rows_at(xor_bits(t, u) * SHARD + h * HALF, HALF)
            for hd in range(heads):
                kt_ref[hd, :, at] = k_ref[hd, at, :].astype(F32).T.astype(BF16)
                vt_ref[hd, :, at] = v_ref[hd, at, :].astype(F32).T.astype(BF16)

        def compute(i, rows):
            @pl.when(i == 0)
            def _():
                w_load.wait()

            for c in x_copies(i):
                c.start()
            x_b = join(full, rows)
            l_b = dot_nt(x_b, wl[...])
            kv = l_b[:, :rank]
            c_b = (kv * rms_inv(kv) * g_ref[...]).astype(BF16)
            cos_b, sin_b = join(cos_ref, rows), join(sin_ref, rows)
            pe_b = rope(l_b[:, rank:], cos_b, sin_b).astype(BF16)

            def put(ref, val, *lead, cols=slice(None)):
                for j, at in enumerate(rows):
                    ref[lead + (at, cols)] = val[j * ROWS:(j + 1) * ROWS, :]

            put(l_ref, l_b)
            put(c_ref, c_b)
            for hd in range(heads):
                q_b = dot_nt(x_b, wq_ref[hd]).astype(BF16)
                put(q_ref, q_b[:, :nope], hd, cols=slice(0, nope))
                put(q_ref, rope(q_b[:, nope:].astype(F32), cos_b, sin_b).astype(BF16), hd, cols=slice(nope, qk))
                put(k_ref, dot_nn(c_b, wk_ref[hd]).astype(BF16), hd, cols=slice(0, nope))
                put(k_ref, pe_b, hd, cols=slice(nope, qk))
                put(v_ref, dot_nn(c_b, wv_ref[hd]).astype(BF16), hd)

            @pl.when(i < 6)
            def _():
                turn(i, 0)
                turn(i, 2)

            @pl.when(i == STEPS - 1)
            def _():
                for j in range(4):
                    turn(STEPS - 1, j)

        ag_run(x_ref, full, send, recv, compute)
        for i in range(STEPS):
            for c in x_copies(i):
                c.wait()

    per = [struct(BF16, heads, seq, qk), struct(F32, seq, lat), struct(BF16, seq, rank), struct(BF16, heads, seq, qk), struct(BF16, heads, qk, seq), struct(BF16, heads, seq, vdim), struct(BF16, heads, vdim, seq)]
    return comm_call(body, 'ag_proj', 1, [VM, VM, ANY] + [VM] * 5, [ANY] + [VM] * len(per), [struct(BF16, seq, dim)] + per,
                     [pltpu.VMEM((seq, dim), BF16)] + AG_SEMS + [sems(STEPS, 4), pltpu.VMEM((lat, dim), BF16), pltpu.SemaphoreType.DMA])(x, w_q, w_dkv, g_kv, w_uk, w_uv, cos_t, sin_t)


def shard_rows(i):
    return rows_at(i * SHARD, SHARD)


def stream_copies(ref, buf, sem, out=False):
    def copies(i):
        a, b = ref.at[shard_rows(i), :], buf.at[i % 2]
        return [pltpu.make_async_copy(b, a, sem.at[i % 2]) if out else pltpu.make_async_copy(a, b, sem.at[i % 2])]

    return copies


def attn_out_rs(o, w_o, e_loc, gain, dy, w_down):
    seq, dim = dy.shape
    ffn = w_down.shape[0]

    def body(o_ref, w_ref, e_ref, g_ref, dy_ref, wd_hbm, h_ref, z_ref, dh_ref, stage, fp, fx, fy, send, recv, wd, dyb, st, wsem, dsem, osem):
        ins, outs = stream_copies(dy_ref, dyb, dsem), stream_copies(dh_ref, st, osem, True)
        w_load = pltpu.make_async_copy(wd_hbm, wd, wsem)
        for c in ins(0) + [w_load]:
            c.start()

        def produce(i, at):
            o_b = join(o_ref, at)
            for cols in col_tiles(dim):
                stage[i, :, cols] = dot_nn(o_b, w_ref[:, cols]).astype(BF16)

        def after(i):
            begin(i, [w_load], ins, outs)
            dy_b = dyb[i % 2]
            for cols in col_tiles(ffn):
                st[i % 2, :, cols] = dot_nt(dy_b, wd[cols, :])
            for c in outs(i):
                c.start()

        def finish(at, val):
            h_b = (e_ref[at, :].astype(F32) + val.astype(BF16).astype(F32)).astype(BF16)
            h_ref[at, :] = h_b
            x = h_b.astype(F32)
            z_ref[at, :] = (x * rms_inv(x) * g_ref[...]).astype(BF16)

        rs_run(stage, fp, fx, fy, send, recv, produce, finish, after)
        finish_all(outs)

    loc = struct(BF16, SHARD, dim)
    return comm_call(body, 'attn_out_rs', 2, [VM] * 4 + [ANY] * 2, [VM, VM, ANY], [loc, loc, struct(F32, seq, ffn)],
                     rs_scratch(dim) + [pltpu.VMEM((ffn, dim), BF16), pltpu.VMEM((2, SHARD, dim), BF16), pltpu.VMEM((2, SHARD, ffn), F32),
                                        pltpu.SemaphoreType.DMA, sems(2), sems(2)])(o, w_o, e_loc, gain, dy, w_down)


def ag_mlp(z, dh, w_gate, w_up):
    seq, ffn = dh.shape
    dim = z.shape[1]

    def body(z_ref, dh_ref, wg_hbm, wu_hbm, z_out, hid_out, dg_out, du_out, full, wg, wu, dhb, st, send, recv, zsem, wsem, dsem, osem):
        t = lax.axis_index('tp')
        loads = [pltpu.make_async_copy(a, b, wsem.at[n]) for n, (a, b) in enumerate(((wg_hbm, wg), (wu_hbm, wu)))]

        def ins(i):
            return [pltpu.make_async_copy(dh_ref.at[at, :], dhb.at[i % 2, quarter(j), :], dsem.at[i % 2, j]) for j, at in enumerate(pieces(t, i))]

        def z_copies(i):
            return [pltpu.make_async_copy(full.at[at, :], z_out.at[at, :], zsem.at[i, j]) for j, at in enumerate(pieces(t, i))]

        def outs(i):
            return [pltpu.make_async_copy(st.at[n, i % 2, quarter(j), :], o.at[at, :], osem.at[n, i % 2, j])
                    for n, o in enumerate((hid_out, dg_out, du_out)) for j, at in enumerate(pieces(t, i))]

        for c in loads + ins(0):
            c.start()

        def compute(i, rows):
            begin(i, loads, ins, outs)
            for c in z_copies(i):
                c.start()
            z_b = join(full, rows)
            for cols in col_tiles(ffn):
                gate = dot_nt(z_b, wg[cols, :])
                up = dot_nt(z_b, wu[cols, :])
                d_hid = dhb[i % 2, :, cols]
                sig = jax.nn.sigmoid(gate)
                act = gate * sig
                for n, val in enumerate((act * up, d_hid * up * sig * (1.0 + gate * (1.0 - sig)), d_hid * act)):
                    st[n, i % 2, :, cols] = val.astype(BF16)
            for c in outs(i):
                c.start()

        ag_run(z_ref, full, send, recv, compute)
        finish_all(outs)
        for i in range(STEPS):
            for c in z_copies(i):
                c.wait()

    act = struct(BF16, seq, ffn)
    weight = pltpu.VMEM((ffn, dim), BF16)
    return comm_call(body, 'ag_mlp', 3, [VM, ANY, ANY, ANY], [ANY] * 4, [struct(BF16, seq, dim), act, act, act],
                     [pltpu.VMEM((seq, dim), BF16), weight, weight, pltpu.VMEM((2, SHARD, ffn), F32), pltpu.VMEM((3, 2, SHARD, ffn), BF16)] + AG_SEMS
                     + [sems(STEPS, 4), sems(2), sems(2, 4), sems(3, 2, 4)])(z, dh, w_gate, w_up)


def mlp_back_rs(d_gate, d_up, w_gate, w_up, h_loc, gain, dy):
    ffn, dim = w_gate.shape

    def body(dg_ref, du_ref, wg_hbm, wu_hbm, h_ref, g_ref, dy_ref, res_ref, resb_ref, dgain_ref, stage, fp, fx, fy, send, recv, wg, wu, blk, wsem, bsem):
        t = lax.axis_index('tp')
        loads = [pltpu.make_async_copy(a, b, wsem.at[n]) for n, (a, b) in enumerate(((wg_hbm, wg), (wu_hbm, wu)))]

        def ins(i):
            return [pltpu.make_async_copy(r.at[at, :], blk.at[n, i % 2, quarter(j), :], bsem.at[n, i % 2, j])
                    for n, r in enumerate((dg_ref, du_ref)) for j, at in enumerate(pieces(t, STEPS - 1 - i))]

        for c in ins(0) + loads:
            c.start()

        def produce(i, at):
            begin(i, loads, ins, lambda i: [])
            dg_b = blk[0, i % 2]
            du_b = blk[1, i % 2]
            for cols in col_tiles(dim):
                stage[i, :, cols] = (dot_nn(dg_b, wg[:, cols]) + dot_nn(du_b, wu[:, cols])).astype(BF16)

        dgain_ref[...] = jnp.zeros_like(dgain_ref)

        def finish(at, val):
            res = dy_ref[at, :].astype(F32) + back_rms_rows(h_ref, g_ref, dgain_ref, at, val)
            res_ref[at, :] = res
            resb_ref[at, :] = res.astype(BF16)

        rs_run(stage, fp, fx, fy, send, recv, produce, finish)

    weight = pltpu.VMEM((ffn, dim), BF16)
    return comm_call(body, 'mlp_back_rs', 4, [ANY] * 4 + [VM] * 3, [VM] * 3, [struct(F32, SHARD, dim), struct(BF16, SHARD, dim), struct(F32, *gain.shape)],
                     rs_scratch(dim) + [weight, weight, pltpu.VMEM((2, 2, SHARD, ffn), BF16), sems(2), sems(2, 2, 4)])(d_gate, d_up, w_gate, w_up, h_loc, gain, dy)


def ag_dattn(x, w_o, hidden, w_down):
    seq, ffn = hidden.shape
    width, dim = w_o.shape

    def body(x_ref, w_ref, hid_ref, wd_hbm, x_out, do_ref, y_out, full, send, recv, sem, wd, hb, yb, wsem, hsem, ysem):
        t = lax.axis_index('tp')
        ins, outs = stream_copies(hid_ref, hb, hsem), stream_copies(y_out, yb, ysem, True)
        w_load = pltpu.make_async_copy(wd_hbm, wd, wsem)
        for c in ins(0) + [w_load]:
            c.start()

        def x_copies(i):
            return [pltpu.make_async_copy(full.at[at, :], x_out.at[at, :], sem.at[i, j]) for j, at in enumerate(pieces(t, i))]

        def before(i):
            begin(i, [w_load], ins, outs)
            h_b = hb[i % 2]
            for cols in col_tiles(dim):
                yb[i % 2, :, cols] = dot_nn(h_b, wd[:, cols]).astype(BF16)
            for c in outs(i):
                c.start()

        def compute(i, rows):
            for c in x_copies(i):
                c.start()
            d_o = dot_nt(join(full, rows), w_ref[...]).astype(BF16)
            for j, at in enumerate(rows):
                do_ref[at, :] = d_o[j * ROWS:(j + 1) * ROWS, :]

        ag_run(x_ref, full, send, recv, compute, before)
        finish_all(outs)
        for i in range(STEPS):
            for c in x_copies(i):
                c.wait()

    big = struct(BF16, seq, dim)
    return comm_call(body, 'ag_dattn', 5, [VM, VM, ANY, ANY], [ANY, VM, ANY], [big, struct(BF16, seq, width), big],
                     [pltpu.VMEM((seq, dim), BF16)] + AG_SEMS + [sems(STEPS, 4), pltpu.VMEM((ffn, dim), BF16), pltpu.VMEM((2, SHARD, ffn), BF16),
                      pltpu.VMEM((2, SHARD, dim), BF16), pltpu.SemaphoreType.DMA, sems(2), sems(2)])(x, w_o, hidden, w_down)


def attn_back_rs(d_query, d_knope, d_kpe, d_value, latent, g_kv, w_uk, w_uv, w_q, w_dkv, cos_t, sin_t, e_loc, g_attn, d_res, dg_mlp):
    heads, _, dim = w_q.shape
    lat = latent.shape[1]
    rank = w_uk.shape[1]
    wide = -(-(dim + lat) // LANES) * LANES
    others = (1, 2, 4, 3, 5, 6, 7)
    total = (1, g_kv.shape[1] + g_attn.shape[1] + dg_mlp.shape[1])

    def body(dq_ref, dk_ref, dkp_ref, dv_ref, l_ref, gkv_ref, wk_ref, wv_ref, wq_ref, wl_ref, cos_ref, sin_ref, e_ref, g_ref, res_ref, dgm_ref,
             de_ref, sum_ref, stage, fp, fx, fy, send, recv, parts, dgkv_ref, dgain_ref, gsend, grecv):
        t = lax.axis_index('tp')
        dgkv_ref[...] = jnp.zeros_like(dgkv_ref)
        dgain_ref[...] = jnp.zeros_like(dgain_ref)

        def produce(i, at):
            d_c = functools.reduce(jnp.add, [dot_nt(join(r, at, hd), w[hd]) for hd in range(heads) for r, w in ((dk_ref, wk_ref), (dv_ref, wv_ref))])
            d_kv, d_g = rms_back(join(l_ref, at)[:, :rank], gkv_ref[...], d_c.astype(BF16).astype(F32))
            dgkv_ref[...] = dgkv_ref[...] + d_g
            d_pe = functools.reduce(jnp.add, [join(dkp_ref, at, hd) for hd in range(heads)])
            d_pe = unrope(d_pe.astype(BF16).astype(F32), join(cos_ref, at), join(sin_ref, at))
            stage[i, :, dim:dim + rank] = d_kv.astype(BF16)
            stage[i, :, dim + rank:dim + lat] = d_pe.astype(BF16)
            stage[i, :, dim + lat:] = jnp.zeros((SHARD, wide - dim - lat), BF16)
            dl_b = stage[i, :, dim:dim + lat]
            dq_b = [join(dq_ref, at, hd) for hd in range(heads)]
            for cols in col_tiles(dim):
                val = dot_nn(dl_b, wl_ref[:, cols])
                for hd in range(heads):
                    val = val + dot_nn(dq_b[hd], wq_ref[hd, :, cols])
                stage[i, :, cols] = val.astype(BF16)

        def finish(at, val):
            d_x = back_rms_rows(e_ref, g_ref, dgain_ref, at, val[:, :dim])
            de_ref[at, :dim] = (res_ref[at, :] + d_x).astype(BF16)
            de_ref[at, dim:] = val[:, dim:].astype(BF16)

        rs_run(stage, fp, fx, fy, send, recv, produce, finish, others=others)
        first = 0
        for ref in (dgkv_ref, dgain_ref, dgm_ref):
            parts[t, :, first:first + ref.shape[1]] = ref[...]
            first += ref.shape[1]
        copies = [send_to(parts.at[t], parts.at[t], gsend.at[n], grecv.at[n], xor_bits(t, u)) for n, u in enumerate(others)]
        for c in copies:
            c.start()
        for c in copies:
            c.wait()
        sum_ref[...] = functools.reduce(jnp.add, [parts[d] for d in range(STEPS)])

    count = len(others)
    return comm_call(body, 'attn_back_rs', 6, [VM] * 16, [VM] * 2, [struct(BF16, SHARD, wide), struct(F32, *total)],
                     rs_scratch(wide) + [pltpu.VMEM((STEPS,) + total, F32), pltpu.VMEM(g_kv.shape, F32), pltpu.VMEM(g_attn.shape, F32), sems(count), sems(count)])(
                         d_query, d_knope, d_kpe, d_value, latent, g_kv, w_uk, w_uv, w_q, w_dkv, cos_t, sin_t, e_loc, g_attn, d_res, dg_mlp)


def gather_seq(x):
    return lax.all_gather(x, 'tp', axis=0, tiled=True)


def scatter_seq(x):
    return lax.psum_scatter(x, 'tp', scatter_dimension=0, tiled=True)


def solution(mesh):
    def device_step(tokens, embed_table, w_q, w_dkv, g_kv, w_uk, w_uv, w_o, g_attn, g_mlp, w_gate, w_up, w_down, d_out):
        vocab_local, model_dim = embed_table.shape
        seq = tokens.shape[1]
        heads, qk = w_q.shape[1:]
        vdim = w_uv.shape[2]
        scale = qk ** -0.5
        dy_loc = d_out[0]
        gkv, gat, gml = g_kv.reshape(1, -1), g_attn.reshape(1, -1), g_mlp.reshape(1, -1)
        wuk, wuv, wq = (jnp.moveaxis(w, 1, 0) for w in (w_uk, w_uv, w_q))
        wq, wl, wg, wu = jnp.swapaxes(wq, 1, 2), w_dkv.T, w_gate.T, w_up.T
        wo = w_o.reshape(heads * vdim, model_dim)
        cos_t, sin_t = rope_tables(seq, qk - w_uk.shape[2])

        dy_full = gather_seq(dy_loc)
        local_ids = tokens[0] - lax.axis_index('tp') * vocab_local
        owned = (local_ids >= 0) & (local_ids < vocab_local)
        slots, pos = lax.sort((jnp.where(owned, local_ids, vocab_local), lax.iota(jnp.int32, seq)), num_keys=1)
        slots = jnp.concatenate([slots, jnp.full((128,), vocab_local, jnp.int32)])
        cnt = jnp.sum(owned.astype(jnp.int32)).reshape(1)
        rows = gather_rows(slots, pos, cnt, embed_table, seq)
        e_loc, u_loc = rs_rows(rows, gat)
        u, q, latent, c_kv, k, kt, v, vt = ag_proj(u_loc, wq, wl, gkv, wuk, wuv, cos_t, sin_t)
        o, lse = attn_fwd(q, k, vt, scale)
        h_loc, z_loc, d_hidden = attn_out_rs(o, wo, e_loc, gml, dy_full, w_down)
        z, hidden, d_gate, d_up = ag_mlp(z_loc, d_hidden, wg, wu)
        d_res, d_res_b, dg_mlp = mlp_back_rs(d_gate, d_up, wg, wu, h_loc, gml, dy_loc)
        d_res_full, d_o, mlp_part = ag_dattn(d_res_b, wo, hidden, w_down)

        mlp_loc = scatter_seq(mlp_part)
        half = cos_t.shape[1] // 2
        d_query, d_knope, d_kpe, d_value, zeros = attn_bwd(q, k, kt, v, d_o, o, lse, cos_t[:, :half].T, sin_t[:, half:].T, scale, embed_table.shape)
        dw_up = matmul_f32('sf,sd->fd', d_up, z)
        dw_up, d_query = lax.optimization_barrier((dw_up, d_query))
        layer_out = (h_loc.astype(F32) + mlp_loc.astype(F32)).astype(BF16)
        back, gains = attn_back_rs(d_query, d_knope, d_kpe, d_value, latent, gkv, wuk, wuv, wq, wl, cos_t, sin_t, e_loc, gat, d_res, dg_mlp)

        back_full = gather_seq(back)
        dw_gate = matmul_f32('sf,sd->fd', d_gate, z)
        dw_down = matmul_f32('sf,sd->fd', hidden, dy_full)
        dw_q = matmul_f32('sd,hse->dhe', u, d_query)
        dw_uk = matmul_f32('sc,hse->che', c_kv, d_knope)
        dw_uv = matmul_f32('sc,hsv->chv', c_kv, d_value)
        dw_o = matmul_f32('sv,sd->vd', o, d_res_full).reshape(w_o.shape)
        back_full, dw_gate, dw_down, dw_q, dw_uk, dw_uv, dw_o = lax.optimization_barrier((back_full, dw_gate, dw_down, dw_q, dw_uk, dw_uv, dw_o))
        dw_gate, dw_up = dw_gate.T, dw_up.T
        dw_dkv = matmul_f32('sc,sd->cd', back_full[:, model_dim:model_dim + w_dkv.shape[1]], u).T
        d_table = scatter_rows(slots, pos, cnt, back_full, zeros)
        gains = gains[0]
        rank = g_kv.shape[0]
        dg_kv, dg_attn, dg_mlp = gains[:rank], gains[rank:rank + model_dim], gains[rank + model_dim:]
        return layer_out[None], d_table, dw_q, dw_dkv, dg_kv, dw_uk, dw_uv, dw_o, dg_attn, dg_mlp, dw_gate, dw_up, dw_down

    row_spec = P('dp', 'tp', None)
    head_spec = P(None, 'tp', None)
    in_specs = (P('dp', None), P('tp', None), head_spec, P(None, None), P(None), head_spec, head_spec, P('tp', None, None), P(None), P(None), P(None, 'tp'), P(None, 'tp'), P('tp', None), row_spec)
    out_specs = (row_spec, P(('dp', 'tp'), None), P('dp', 'tp', None), P('dp', None), P('dp'), P('dp', 'tp', None), P('dp', 'tp', None), P(('dp', 'tp'), None, None), P('dp'), P('dp'), P('dp', 'tp'), P('dp', 'tp'), P(('dp', 'tp'), None))
    return jax.shard_map(device_step, mesh=mesh, in_specs=in_specs, out_specs=out_specs, check_vma=False)
```

```python
import functools

import jax
import jax.numpy as jnp
import numpy as np
from jax import lax
from jax.experimental import pallas as pl
from jax.experimental.pallas import tpu as pltpu
from jax.sharding import PartitionSpec as P

EPSILON = 1e-6
ROPE_BASE = 10000.0
LOG2E = 1.4426950408889634
BLK = 256
RING = 16
LANES = 128
ROWS = 64
VMEM_CAP = 60 * 1024 * 1024
BUSY = 40_000_000_000
NEG = -1e30
F32 = jnp.float32
BF16 = jnp.bfloat16


def matmul_f32(form, lhs, rhs):
    return jnp.einsum(form, lhs, rhs, preferred_element_type=jnp.float32)


def dot_nn(a, b):
    return jnp.dot(a, b, preferred_element_type=F32)


def dot_nt(a, b):
    return lax.dot_general(a, b, (((1,), (1,)), ((), ())), preferred_element_type=F32)


def tile(i):
    return slice(i * BLK, (i + 1) * BLK)


def rows_at(first, count):
    return pl.ds(pl.multiple_of(first, count), count)


def sems(*shape):
    return pltpu.SemaphoreType.DMA(shape)


def loop(count, step):
    def body(i, carry):
        step(i)
        return carry

    lax.fori_loop(0, count, body, 0)


VM = pl.BlockSpec(memory_space=pltpu.VMEM)
ANY = pl.BlockSpec(memory_space=pl.ANY)


def rope_tables(seq_len, rope_dim):
    inv_freq = np.float32(ROPE_BASE) ** (-np.arange(0, rope_dim, 2, dtype=np.float32) / np.float32(rope_dim))
    angles = (np.arange(seq_len, dtype=np.float32)[:, None] * inv_freq[None, :]).astype(np.float64)
    cos, sin = np.cos(angles), np.sin(angles)
    return (jnp.asarray(np.concatenate([cos, cos], axis=1), dtype=F32), jnp.asarray(np.concatenate([-sin, sin], axis=1), dtype=F32))


def swap_halves(x):
    half = x.shape[1] // 2
    return jnp.concatenate([x[:, half:], x[:, :half]], axis=1)


def rope(x, cos_t, sin_t):
    return x * cos_t + swap_halves(x) * sin_t


def unrope(x, cos_t, sin_t):
    return x * cos_t - swap_halves(x) * sin_t


def rms_inv(x):
    return lax.rsqrt(jnp.mean(x * x, axis=-1, keepdims=True) + EPSILON)


def rms_back(x, gain, dy):
    inv = rms_inv(x)
    gd = dy * gain
    mix = jnp.mean(gd * x, axis=-1, keepdims=True)
    return inv * gd - x * (inv * inv * inv * mix), jnp.sum(dy * (x * inv), axis=0, keepdims=True)


def gather_body(slot_ref, pos_ref, cnt_ref, tab_ref, out_ref, buf, acc, sem):
    seq, dim = acc.shape
    cnt = cnt_ref[0]

    def fetch(k):
        return pltpu.make_async_copy(tab_ref.at[rows_at(slot_ref[k] // 8 * 8, 8), :], buf.at[k % RING], sem.at[k % RING])

    loop(jnp.minimum(cnt, RING), lambda k: fetch(k).start())

    def clear(i):
        acc[rows_at(i * ROWS, ROWS), :] = jnp.zeros((ROWS, dim), F32)

    loop(seq // ROWS, clear)
    rows = lax.broadcasted_iota(jnp.int32, buf.shape[1:], 0)

    def step(k):
        fetch(k).wait()
        picked = jnp.where(rows == slot_ref[k] % 8, buf[k % RING].astype(F32), 0.0)
        acc[pl.ds(pos_ref[k], 1), :] = jnp.sum(picked, axis=0, keepdims=True)

        @pl.when(k + RING < cnt)
        def _():
            fetch(k + RING).start()

    loop(cnt, step)

    def emit(i):
        at = rows_at(i * ROWS, ROWS)
        out_ref[at, :] = acc[at, :].astype(BF16)

    loop(seq // ROWS, emit)


def local_call(body, name, out, in_specs, out_specs, scratch, scalars=0, grid=(1,), **extra):
    return pl.pallas_call(
        body, name=name, out_shape=out,
        grid_spec=pltpu.PrefetchScalarGridSpec(num_scalar_prefetch=scalars, grid=grid, in_specs=in_specs, out_specs=out_specs, scratch_shapes=scratch),
        compiler_params=pltpu.CompilerParams(vmem_limit_bytes=VMEM_CAP),
        cost_estimate=pl.CostEstimate(flops=BUSY // 2, bytes_accessed=BUSY // 2000, transcendentals=0), **extra)


def whole(*shape):
    return pl.BlockSpec(shape, lambda i, *_: (0,) * len(shape))


def gather_rows(slots, pos, cnt, table, seq):
    dim = table.shape[1]
    return local_call(gather_body, 'gather_rows', jax.ShapeDtypeStruct((seq, dim), BF16), [ANY], whole(seq, dim),
                      [pltpu.VMEM((RING, 8, dim), BF16), pltpu.VMEM((seq, dim), F32), sems(RING)], 3)(slots, pos, cnt, table)


def scatter_body(slot_ref, pos_ref, cnt_ref, de_ref, zero_ref, out_ref, wide, acc, stage, sem, near, nsem):
    seq, dim = wide.shape

    def load(i):
        at = rows_at(i * BLK, BLK)
        return pltpu.make_async_copy(de_ref.at[at, pl.ds(0, dim)], near.at[at, :], nsem.at[i])

    loop(seq // BLK, lambda i: load(i).start())

    def widen(i):
        load(i).wait()
        at = rows_at(i * BLK, BLK)
        wide[at, :] = near[at, :].astype(F32)

    loop(seq // BLK, widen)

    def put(blk, n):
        return pltpu.make_async_copy(stage.at[n % RING], out_ref.at[rows_at(blk * 8, 8), :], sem.at[n % RING])

    def step(k, carry):
        prev, n = carry
        slot = slot_ref[k]
        blk = slot // 8

        @pl.when(blk != prev)
        def _():
            acc[...] = jnp.zeros_like(acc)

        at = pl.ds(slot % 8, 1)
        acc[at, :] = acc[at, :] + wide[pl.ds(pos_ref[k], 1), :]
        last = slot_ref[k + 1] // 8 != blk

        @pl.when(last)
        def _():
            @pl.when(n >= RING)
            def _():
                put(blk, n).wait()

            stage[n % RING] = acc[...].astype(BF16)
            put(blk, n).start()

        return blk, n + last.astype(jnp.int32)

    _, total = lax.fori_loop(0, cnt_ref[0], step, (jnp.int32(-1), jnp.int32(0)))
    loop(jnp.minimum(total, RING), lambda i: put(0, total - 1 - i).wait())


def scatter_rows(slots, pos, cnt, de, zeros):
    seq, dim = de.shape[0], zeros.shape[1]
    return local_call(scatter_body, 'scatter_rows', jax.ShapeDtypeStruct(zeros.shape, BF16), [ANY, ANY], ANY,
                      [pltpu.VMEM((seq, dim), F32), pltpu.VMEM((8, dim), F32), pltpu.VMEM((RING, 8, dim), BF16), sems(RING), pltpu.VMEM((seq, dim), BF16), sems(seq // BLK)], 3, input_output_aliases={4: 0})(slots, pos, cnt, de, zeros)


def causal_tile():
    shape = (BLK, BLK)
    return lax.broadcasted_iota(jnp.int32, shape, 0) <= lax.broadcasted_iota(jnp.int32, shape, 1)


def fold(op, parts):
    total = functools.reduce(lambda a, b: a + b if op is jnp.sum else jnp.maximum(a, b), parts)
    return op(total, axis=0, keepdims=True)


def by_eight(op, x):
    return op(x.reshape(-1, 8, BLK), axis=0)


def attn_fwd_body(scale2, q_ref, k_ref, vt_ref, o_ref, lse_ref, s_scr):
    tri = causal_tile()
    for i in range(q_ref.shape[1] // BLK):
        q_i = q_ref[0, tile(i), :]
        tops = []
        for j in range(i + 1):
            s = dot_nt(k_ref[0, tile(j), :], q_i) * scale2
            if j == i:
                s = jnp.where(tri, s, NEG)
            s_scr[tile(j), :] = s
            tops.append(by_eight(jnp.max, s))
        top = fold(jnp.max, tops)
        dens = []
        for j in range(i + 1):
            e = jnp.exp2(s_scr[tile(j), :] - top)
            s_scr[tile(j), :] = e
            dens.append(by_eight(jnp.sum, e))
        den = fold(jnp.sum, dens)
        inv = 1.0 / den
        out = [dot_nn(vt_ref[0, :, tile(j)], (s_scr[tile(j), :] * inv).astype(BF16)) for j in range(i + 1)]
        o_ref[tile(i), :] = functools.reduce(jnp.add, out).T.astype(BF16)
        lse_ref[0, :, tile(i)] = top + jnp.log2(den)


def per_head(*shape):
    return pl.BlockSpec((1,) + shape, lambda h: (h, 0, 0))


def head_cols(seq, width):
    return pl.BlockSpec((seq, width), lambda h: (0, h))


def attn_fwd(q, k, vt, scale):
    heads, seq, qk = q.shape
    vdim = vt.shape[1]
    return local_call(functools.partial(attn_fwd_body, scale * LOG2E), 'attn_fwd',
                      [jax.ShapeDtypeStruct((seq, heads * vdim), BF16), jax.ShapeDtypeStruct((heads, 1, seq), F32)],
                      [per_head(seq, qk), per_head(seq, qk), per_head(vdim, seq)], [head_cols(seq, vdim), per_head(1, seq)],
                      [pltpu.VMEM((seq, BLK), F32)], grid=(heads,))(q, k, vt)


def attn_bwd_body(scale2, scale, q_ref, k_ref, kt_ref, v_ref, do_ref, o_ref, lse_ref, cos_ref, sin_ref, dq_ref, dk_ref, dkp_ref, dv_ref, zero_ref, p_scr, ds_scr, dlt, blank, zsem):
    seq = q_ref.shape[1]
    nope = dk_ref.shape[2]
    n = seq // BLK
    head = pl.program_id(0)
    size = blank.shape[0]
    fills = [pltpu.make_async_copy(blank, zero_ref.at[pl.ds(m * size, size), :], zsem.at[m]) for m in range(zsem.shape[0])]

    @pl.when(head == 0)
    def _():
        blank[...] = jnp.zeros_like(blank)
        for c in fills:
            c.start()

    tri = causal_tile()
    for i in range(n):
        both = do_ref[tile(i), :].astype(F32) * o_ref[tile(i), :].astype(F32)
        dlt[:, tile(i)] = jnp.sum(both.T, axis=0, keepdims=True)
    for j in range(n):
        k_j = k_ref[0, tile(j), :]
        v_j = v_ref[0, tile(j), :]
        for i in range(j, n):
            s = dot_nt(k_j, q_ref[0, tile(i), :])
            prob = jnp.exp2(s * scale2 - lse_ref[0, :, tile(i)])
            if i == j:
                prob = jnp.where(tri, prob, 0.0)
            dp = dot_nt(v_j, do_ref[tile(i), :])
            p_scr[:, tile(i)] = prob.astype(BF16)
            ds_scr[tile(j), tile(i)] = (prob * (dp - dlt[:, tile(i)])).astype(BF16)
        rest = slice(j * BLK, seq)
        dv_ref[0, tile(j), :] = dot_nn(p_scr[:, rest], do_ref[rest, :]).astype(BF16)
        dk = dot_nn(ds_scr[tile(j), rest], q_ref[0, rest, :]) * scale
        dk_ref[0, tile(j), :] = dk[:, :nope].astype(BF16)
        dkp_ref[0, tile(j), :] = dk[:, nope:]

    half = cos_ref.shape[0]
    for i in range(n):
        seen = slice(0, (i + 1) * BLK)
        dq = dot_nn(kt_ref[0, :, seen], ds_scr[seen, tile(i)]) * scale
        lo, hi = dq[nope:nope + half, :], dq[nope + half:, :]
        cos_b, sin_b = cos_ref[:, tile(i)], sin_ref[:, tile(i)]
        turned = jnp.concatenate([dq[:nope, :], lo * cos_b + hi * sin_b, hi * cos_b - lo * sin_b], axis=0)
        dq_ref[0, tile(i), :] = turned.T.astype(BF16)

    @pl.when(head == pl.num_programs(0) - 1)
    def _():
        for c in fills:
            c.wait()


def attn_bwd(q, k, kt, v, do, o, lse, cos_t, sin_t, scale, table):
    heads, seq, qk = q.shape
    vdim = v.shape[2]
    half = cos_t.shape[0]
    pe = half + half
    outs = [((seq, qk), BF16), ((seq, qk - pe), BF16), ((seq, pe), F32), ((seq, vdim), BF16)]
    return local_call(functools.partial(attn_bwd_body, scale * LOG2E, scale), 'attn_bwd', [jax.ShapeDtypeStruct((heads,) + s, d) for s, d in outs] + [jax.ShapeDtypeStruct(table, BF16)],
                      [per_head(seq, qk), per_head(seq, qk), per_head(qk, seq), per_head(seq, vdim), head_cols(seq, vdim), head_cols(seq, vdim), per_head(1, seq), whole(half, seq), whole(half, seq)],
                      [per_head(*s) for s, _ in outs] + [ANY],
                      [pltpu.VMEM((BLK, seq), BF16), pltpu.VMEM((seq, seq), BF16), pltpu.VMEM((1, seq), F32), pltpu.VMEM((table[0] // RING,) + table[1:], BF16), sems(RING)],
                      grid=(heads,))(q, k, kt, v, do, o, lse, cos_t, sin_t)


HALF = 128
SHARD = 256
STEPS = 8
PEERS = (1, 2, 4)
MESH = pl.DeviceIdType.MESH


def xor_bits(t, u):
    out = 0
    for b in (1, 2, 4):
        tb = (t // b) % 2
        ub = (u // b) % 2
        out = out + b * (tb + ub - 2 * tb * ub)
    return out


def greet(t, others):
    peers = [xor_bits(t, u) for u in others]
    barrier = pltpu.get_barrier_semaphore()
    for peer in peers:
        pl.semaphore_signal(barrier, inc=1, device_id={'tp': peer}, device_id_type=MESH)
    pl.semaphore_wait(barrier, len(peers))
    return peers


def send_to(src, dst, send, recv, dev):
    return pltpu.make_async_remote_copy(src_ref=src, dst_ref=dst, send_sem=send, recv_sem=recv, device_id={'tp': dev}, device_id_type=MESH)


def piece_id(m, j):
    i = 2 * m + j // 2
    p, r = i // 4, i % 4
    first, last = (3 - p) // 3, p // 3
    mid = 1 - first - last
    u = first * (r // 2) + mid * (2 + (r % 2) * 2 + r // 2)
    h = r % 2 + (p - 1) * mid * (1 - 2 * (r % 2))
    near = 1 - last
    return u + last * (6 + j // 2), near * h + last * (j % 2), near * (j % 2) + last * (m % 2)


def piece(t, m, j):
    u, h, a = piece_id(m, j)
    return rows_at(xor_bits(t, u) * SHARD + h * HALF + a * ROWS, ROWS)


def pieces(t, m):
    return [piece(t, m, j) for j in range(4)]


def quarter(j):
    return pl.ds(j * ROWS, ROWS)


def join(ref, at, *lead):
    return jnp.concatenate([ref[lead + (r, slice(None))] for r in at], axis=0)


def begin(i, loads, ins, outs):
    @pl.when(i == 0)
    def _():
        for c in loads:
            c.wait()

    @pl.when(i < STEPS - 1)
    def _():
        for c in ins(i + 1):
            c.start()

    @pl.when(i >= 2)
    def _():
        for c in outs(i - 2):
            c.wait()

    for c in ins(i):
        c.wait()


def finish_all(outs):
    for i in (STEPS - 2, STEPS - 1):
        for c in outs(i):
            c.wait()


def ag_run(x_ref, full, send, recv, compute, before=None, peers=None):
    t = lax.axis_index('tp')
    partner, xn, yn = peers or greet(t, PEERS)
    sends = []

    def copy(src, shard, first, count, u_there, dev):
        place = rows_at(shard * SHARD + first, count)
        slot = first // ROWS
        c = send_to(src, full.at[place, :], send.at[len(sends)], recv.at[u_there, slot], dev)
        sends.append(c)
        return c

    def mine(h, u, dev):
        return copy(x_ref.at[pl.ds(h * HALF, HALF), :], t, h * HALF, HALF, u, dev)

    def relay(u, first, count, u_there, dev):
        shard = xor_bits(t, u)
        return copy(full.at[rows_at(shard * SHARD + first, count), :], shard, first, count, u_there, dev)

    for h, u, dev in ((0, 2, xn), (1, 4, yn), (0, 1, partner), (1, 1, partner), (1, 2, xn), (0, 4, yn)):
        mine(h, u, dev).start()
    full[rows_at(t * SHARD, SHARD), :] = x_ref[...]
    onward = {(u, h): [relay(u, h * HALF, HALF, u + 1, partner)] for u in (2, 4) for h in (0, 1)}
    for a in (0, 1):
        onward[2, 0].append(relay(2, a * ROWS, ROWS, 6, yn))
        onward[4, 1].append(relay(4, HALF + a * ROWS, ROWS, 6, xn))
    far = {(h, a): relay(6, h * HALF + a * ROWS, ROWS, 7, partner) for h in (0, 1) for a in (0, 1)}

    def arrive(u, first, count):
        place = full.at[rows_at(xor_bits(t, u) * SHARD + first, count), :]
        send_to(place, place, send.at[0], recv.at[u, first // ROWS], partner).wait_recv()

    def step(i):
        if before is not None:
            before(i)
        for m in range(1, 6):
            @pl.when(i == m)
            def _(m=m):
                for j in (0, 2):
                    u, h, _ = piece_id(m, j)
                    arrive(u, h * HALF, HALF)
                    for c in onward.get((u, h), ()):
                        c.start()

        for a in (0, 1):
            @pl.when(i == 6 + a)
            def _(a=a):
                for h in (0, 1):
                    arrive(6, h * HALF + a * ROWS, ROWS)
                    far[h, a].start()
                for h in (0, 1):
                    arrive(7, h * HALF + a * ROWS, ROWS)

        compute(i, pieces(t, i))

    loop(STEPS, step)
    for c in sends:
        c.wait_send()


AG_SEMS = [sems(18), sems(8, 4)]


def rs_run(stage, fp, fx, fy, send, recv, produce, finish, after=None, others=PEERS, peers=None):
    t = lax.axis_index('tp')
    partner, xn, yn, *_ = peers or greet(t, others)
    sends = []

    def copy(src, dst, dev):
        n = len(sends)
        c = send_to(src, dst, send.at[n], recv.at[n], dev)
        sends.append(c)
        return c

    first, second = pl.ds(0, HALF), pl.ds(HALF, HALF)
    swap = [copy(stage.at[k, second, :], fp.at[0, pl.ds(k * HALF, HALF), :], partner) for k in (0, 1)]
    swap += [copy(stage.at[2 * p], fp.at[p], partner) for p in (1, 2, 3)]
    far_y = [copy(stage.at[k, quarter(0), :], fy.at[0, quarter(1 - k), :], yn) for k in (0, 1)]
    far_x = [copy(stage.at[k, quarter(1), :], fx.at[0, quarter(1 - k), :], xn) for k in (0, 1)]
    near_x, near_y = copy(stage.at[3, first, :], fx.at[1], xn), copy(stage.at[3, second, :], fy.at[1], yn)
    via_x, via_y = copy(stage.at[5, first, :], fx.at[2], xn), copy(stage.at[5, second, :], fy.at[2], yn)

    def add(i, start, count, src, src_start):
        def body(r):
            a = rows_at(start + r * 32, 32)
            stage[i, a, :] = (stage[i, a, :].astype(F32) + src[rows_at(src_start + r * 32, 32), :].astype(F32)).astype(BF16)

        loop(count // 32, body)

    def step(i):
        produce(i, pieces(t, STEPS - 1 - i))
        for k in (0, 1):
            @pl.when(i == k)
            def _(k=k):
                swap[k].start()
                swap[k].wait_recv()
                add(k, 0, HALF, fp.at[0], k * HALF)
                far_x[k].start()
                far_y[k].start()

        for p in (1, 2, 3):
            @pl.when(i == 2 * p)
            def _(p=p):
                swap[p + 1].start()

            @pl.when(i == 2 * p + 1)
            def _(p=p):
                swap[p + 1].wait_recv()
                add(2 * p + 1, 0, SHARD, fp.at[p], 0)

        @pl.when(i == 3)
        def _():
            near_x.start()
            near_y.start()

        @pl.when(i == 5)
        def _():
            for c in far_y:
                c.wait_recv()
            add(5, 0, HALF, fy.at[0], 0)
            via_x.start()
            for c in far_x:
                c.wait_recv()
            add(5, HALF, HALF, fx.at[0], 0)
            via_y.start()

        if after is not None:
            @pl.when(i >= 1)
            def _():
                after(i - 1)

    loop(STEPS, step)
    if after is not None:
        after(STEPS - 1)
    for c in (near_x, near_y, via_x, via_y):
        c.wait_recv()

    def last(r):
        lo, hi = rows_at(r * 32, 32), rows_at(HALF + r * 32, 32)
        finish(lo, (stage[7, lo, :].astype(F32) + fy[1, lo, :].astype(F32)) + fx[2, lo, :].astype(F32))
        finish(hi, (stage[7, hi, :].astype(F32) + fx[1, lo, :].astype(F32)) + fy[2, lo, :].astype(F32))

    loop(HALF // 32, last)
    for c in sends:
        c.wait_send()


def rs_scratch(dim):
    return [pltpu.VMEM((n, rows, dim), BF16) for n, rows in ((STEPS, SHARD), (4, SHARD), (3, HALF), (3, HALF))] + [sems(13), sems(13)]


def comm_call(body, name, cid, in_specs, out_specs, out_shape, scratch):
    return pl.pallas_call(
        body, name=name, in_specs=in_specs, out_specs=out_specs, out_shape=out_shape, scratch_shapes=scratch,
        compiler_params=pltpu.CompilerParams(collective_id=cid, has_side_effects=True, vmem_limit_bytes=VMEM_CAP),
        cost_estimate=pl.CostEstimate(flops=BUSY, bytes_accessed=BUSY // 2000, transcendentals=0))


def col_tiles(width):
    return [slice(a, min(a + BLK, width)) for a in range(0, width, BLK)]


def struct(dtype, *shape):
    return jax.ShapeDtypeStruct(shape, dtype)


def back_rms_rows(x_ref, g_ref, dgain_ref, at, dy):
    d_x, d_g = rms_back(x_ref[at, :].astype(F32), g_ref[...], dy.astype(BF16).astype(F32))
    dgain_ref[...] = dgain_ref[...] + d_g
    return d_x


def rs_rows(rows, gain):
    dim = rows.shape[1]

    def body(rows_ref, g_ref, e_ref, u_ref, stage, fp, fx, fy, send, recv, load):
        t = lax.axis_index('tp')

        def fetch(i):
            return [pltpu.make_async_copy(rows_ref.at[at, :], stage.at[i, quarter(j), :], load.at[i, j]) for j, at in enumerate(pieces(t, STEPS - 1 - i))]

        for i in range(STEPS):
            for c in fetch(i):
                c.start()

        def produce(i, at):
            for c in fetch(i):
                c.wait()

        def finish(at, val):
            e_b = val.astype(BF16)
            e_ref[at, :] = e_b
            x = e_b.astype(F32)
            u_ref[at, :] = (x * rms_inv(x) * g_ref[...]).astype(BF16)

        rs_run(stage, fp, fx, fy, send, recv, produce, finish)

    loc = struct(BF16, SHARD, dim)
    return comm_call(body, 'rs_rows', 0, [ANY, VM], [VM, VM], [loc, loc], rs_scratch(dim) + [sems(STEPS, 4)])(rows, gain)


def ag_proj(x, w_q, w_dkv, g_kv, w_uk, w_uv, cos_t, sin_t):
    seq = cos_t.shape[0]
    heads, qk, dim = w_q.shape
    lat = w_dkv.shape[0]
    rank, nope = w_uk.shape[1:]
    vdim = w_uv.shape[2]

    def body(x_ref, wq_ref, wl_hbm, g_ref, wk_ref, wv_ref, cos_ref, sin_ref, x_out, q_ref, l_ref, c_ref, k_ref, kt_ref, v_ref, vt_ref, full, send, recv, sem, wl, wsem):
        t = lax.axis_index('tp')
        w_load = pltpu.make_async_copy(wl_hbm, wl, wsem)
        w_load.start()

        def x_copies(i):
            return [pltpu.make_async_copy(full.at[at, :], x_out.at[at, :], sem.at[i, j]) for j, at in enumerate(pieces(t, i))]

        def turn(m, j):
            u, h, _ = piece_id(m, j)
            at = rows_at(xor_bits(t, u) * SHARD + h * HALF, HALF)
            for hd in range(heads):
                kt_ref[hd, :, at] = k_ref[hd, at, :].astype(F32).T.astype(BF16)
                vt_ref[hd, :, at] = v_ref[hd, at, :].astype(F32).T.astype(BF16)

        def compute(i, rows):
            @pl.when(i == 0)
            def _():
                w_load.wait()

            for c in x_copies(i):
                c.start()
            x_b = join(full, rows)
            l_b = dot_nt(x_b, wl[...])
            kv = l_b[:, :rank]
            c_b = (kv * rms_inv(kv) * g_ref[...]).astype(BF16)
            cos_b, sin_b = join(cos_ref, rows), join(sin_ref, rows)
            pe_b = rope(l_b[:, rank:], cos_b, sin_b).astype(BF16)

            def put(ref, val, *lead, cols=slice(None)):
                for j, at in enumerate(rows):
                    ref[lead + (at, cols)] = val[j * ROWS:(j + 1) * ROWS, :]

            put(l_ref, l_b)
            put(c_ref, c_b)
            for hd in range(heads):
                q_b = dot_nt(x_b, wq_ref[hd]).astype(BF16)
                put(q_ref, q_b[:, :nope], hd, cols=slice(0, nope))
                put(q_ref, rope(q_b[:, nope:].astype(F32), cos_b, sin_b).astype(BF16), hd, cols=slice(nope, qk))
                put(k_ref, dot_nn(c_b, wk_ref[hd]).astype(BF16), hd, cols=slice(0, nope))
                put(k_ref, pe_b, hd, cols=slice(nope, qk))
                put(v_ref, dot_nn(c_b, wv_ref[hd]).astype(BF16), hd)

            @pl.when(i < 6)
            def _():
                turn(i, 0)
                turn(i, 2)

            @pl.when(i == STEPS - 1)
            def _():
                for j in range(4):
                    turn(STEPS - 1, j)

        ag_run(x_ref, full, send, recv, compute)
        for i in range(STEPS):
            for c in x_copies(i):
                c.wait()

    per = [struct(BF16, heads, seq, qk), struct(F32, seq, lat), struct(BF16, seq, rank), struct(BF16, heads, seq, qk), struct(BF16, heads, qk, seq), struct(BF16, heads, seq, vdim), struct(BF16, heads, vdim, seq)]
    return comm_call(body, 'ag_proj', 1, [VM, VM, ANY] + [VM] * 5, [ANY] + [VM] * len(per), [struct(BF16, seq, dim)] + per,
                     [pltpu.VMEM((seq, dim), BF16)] + AG_SEMS + [sems(STEPS, 4), pltpu.VMEM((lat, dim), BF16), pltpu.SemaphoreType.DMA])(x, w_q, w_dkv, g_kv, w_uk, w_uv, cos_t, sin_t)


def shard_rows(i):
    return rows_at(i * SHARD, SHARD)


def stream_copies(ref, buf, sem, out=False):
    def copies(i):
        a, b = ref.at[shard_rows(i), :], buf.at[i % 2]
        return [pltpu.make_async_copy(b, a, sem.at[i % 2]) if out else pltpu.make_async_copy(a, b, sem.at[i % 2])]

    return copies


def attn_out_rs(o, w_o, e_loc, gain, dy, w_down):
    seq, dim = dy.shape
    ffn = w_down.shape[0]

    def body(o_ref, w_ref, e_ref, g_ref, dy_ref, wd_hbm, h_ref, z_ref, dh_ref, stage, fp, fx, fy, send, recv, wd, dyb, st, wsem, dsem, osem):
        ins, outs = stream_copies(dy_ref, dyb, dsem), stream_copies(dh_ref, st, osem, True)
        w_load = pltpu.make_async_copy(wd_hbm, wd, wsem)
        for c in ins(0) + [w_load]:
            c.start()

        def produce(i, at):
            o_b = join(o_ref, at)
            for cols in col_tiles(dim):
                stage[i, :, cols] = dot_nn(o_b, w_ref[:, cols]).astype(BF16)

        def after(i):
            begin(i, [w_load], ins, outs)
            dy_b = dyb[i % 2]
            for cols in col_tiles(ffn):
                st[i % 2, :, cols] = dot_nt(dy_b, wd[cols, :])
            for c in outs(i):
                c.start()

        def finish(at, val):
            h_b = (e_ref[at, :].astype(F32) + val.astype(BF16).astype(F32)).astype(BF16)
            h_ref[at, :] = h_b
            x = h_b.astype(F32)
            z_ref[at, :] = (x * rms_inv(x) * g_ref[...]).astype(BF16)

        rs_run(stage, fp, fx, fy, send, recv, produce, finish, after)
        finish_all(outs)

    loc = struct(BF16, SHARD, dim)
    return comm_call(body, 'attn_out_rs', 2, [VM] * 4 + [ANY] * 2, [VM, VM, ANY], [loc, loc, struct(F32, seq, ffn)],
                     rs_scratch(dim) + [pltpu.VMEM((ffn, dim), BF16), pltpu.VMEM((2, SHARD, dim), BF16), pltpu.VMEM((2, SHARD, ffn), F32),
                                        pltpu.SemaphoreType.DMA, sems(2), sems(2)])(o, w_o, e_loc, gain, dy, w_down)


def mlp_block(z, dh, w_gate, w_up, h_loc, gain, dy):
    seq, ffn = dh.shape
    dim = z.shape[1]

    def body(z_ref, dh_ref, wg_hbm, wu_hbm, h_ref, g_ref, dy_ref, z_out, hid_out, dg_out, du_out, res_ref, resb_ref, dgain_ref,
             full, wg, wu, dhb, st, dg, du, wsem, dsem, osem, gsem, send, recv, stage, fp, fx, fy, rs_send, rs_recv):
        t = lax.axis_index('tp')
        peers = greet(t, PEERS)
        loads = [pltpu.make_async_copy(a, b, wsem.at[n]) for n, (a, b) in enumerate(((wg_hbm, wg), (wu_hbm, wu)))]

        def ins(i):
            return [pltpu.make_async_copy(dh_ref.at[at, :], dhb.at[i % 2, quarter(j), :], dsem.at[i % 2, j]) for j, at in enumerate(pieces(t, i))]

        def outs(i):
            return [pltpu.make_async_copy(st.at[i % 2, quarter(j), :], hid_out.at[at, :], osem.at[i % 2, j]) for j, at in enumerate(pieces(t, i))]

        def kept(i):
            return [pltpu.make_async_copy(a.at[at, :], b.at[at, :], gsem.at[n, i, j])
                    for n, (a, b) in enumerate(((full, z_out), (dg, dg_out), (du, du_out))) for j, at in enumerate(pieces(t, i))]

        for c in loads + ins(0):
            c.start()
        dgain_ref[...] = jnp.zeros_like(dgain_ref)

        def compute(i, rows):
            begin(i, loads, ins, outs)
            z_b = join(full, rows)
            for cols in col_tiles(ffn):
                gate = dot_nt(z_b, wg[cols, :])
                up = dot_nt(z_b, wu[cols, :])
                d_hid = dhb[i % 2, :, cols]
                sig = jax.nn.sigmoid(gate)
                act = gate * sig
                st[i % 2, :, cols] = (act * up).astype(BF16)
                for ref, val in ((dg, d_hid * up * sig * (1.0 + gate * (1.0 - sig))), (du, d_hid * act)):
                    for j, at in enumerate(rows):
                        ref[at, cols] = val[j * ROWS:(j + 1) * ROWS, :].astype(BF16)
            for c in outs(i) + kept(i):
                c.start()

        ag_run(z_ref, full, send, recv, compute, peers=peers)

        def produce(i, at):
            dg_b, du_b = join(dg, at), join(du, at)
            for cols in col_tiles(dim):
                stage[i, :, cols] = (dot_nn(dg_b, wg[:, cols]) + dot_nn(du_b, wu[:, cols])).astype(BF16)

        def finish(at, val):
            res = dy_ref[at, :].astype(F32) + back_rms_rows(h_ref, g_ref, dgain_ref, at, val)
            res_ref[at, :] = res
            resb_ref[at, :] = res.astype(BF16)

        rs_run(stage, fp, fx, fy, rs_send, rs_recv, produce, finish, peers=peers)
        finish_all(outs)
        for i in range(STEPS):
            for c in kept(i):
                c.wait()

    act = struct(BF16, seq, ffn)
    weight, wide = pltpu.VMEM((ffn, dim), BF16), pltpu.VMEM((seq, ffn), BF16)
    return comm_call(body, 'mlp_block', 3, [VM] + [ANY] * 3 + [VM] * 3, [ANY] * 4 + [VM] * 3,
                     [struct(BF16, seq, dim), act, act, act, struct(F32, SHARD, dim), struct(BF16, SHARD, dim), struct(F32, *gain.shape)],
                     [pltpu.VMEM((seq, dim), BF16), weight, weight, pltpu.VMEM((2, SHARD, ffn), F32), pltpu.VMEM((2, SHARD, ffn), BF16), wide, wide,
                      sems(2), sems(2, 4), sems(2, 4), sems(3, STEPS, 4)] + AG_SEMS + rs_scratch(dim))(z, dh, w_gate, w_up, h_loc, gain, dy)


def ag_dattn(x, w_o, hidden, w_down):
    seq, ffn = hidden.shape
    width, dim = w_o.shape

    def body(x_ref, w_ref, hid_ref, wd_hbm, x_out, do_ref, y_out, full, send, recv, sem, wd, hb, yb, wsem, hsem, ysem):
        t = lax.axis_index('tp')
        ins, outs = stream_copies(hid_ref, hb, hsem), stream_copies(y_out, yb, ysem, True)
        w_load = pltpu.make_async_copy(wd_hbm, wd, wsem)
        for c in ins(0) + [w_load]:
            c.start()

        def x_copies(i):
            return [pltpu.make_async_copy(full.at[at, :], x_out.at[at, :], sem.at[i, j]) for j, at in enumerate(pieces(t, i))]

        def before(i):
            begin(i, [w_load], ins, outs)
            h_b = hb[i % 2]
            for cols in col_tiles(dim):
                yb[i % 2, :, cols] = dot_nn(h_b, wd[:, cols]).astype(BF16)
            for c in outs(i):
                c.start()

        def compute(i, rows):
            for c in x_copies(i):
                c.start()
            d_o = dot_nt(join(full, rows), w_ref[...]).astype(BF16)
            for j, at in enumerate(rows):
                do_ref[at, :] = d_o[j * ROWS:(j + 1) * ROWS, :]

        ag_run(x_ref, full, send, recv, compute, before)
        finish_all(outs)
        for i in range(STEPS):
            for c in x_copies(i):
                c.wait()

    big = struct(BF16, seq, dim)
    return comm_call(body, 'ag_dattn', 5, [VM, VM, ANY, ANY], [ANY, VM, ANY], [big, struct(BF16, seq, width), big],
                     [pltpu.VMEM((seq, dim), BF16)] + AG_SEMS + [sems(STEPS, 4), pltpu.VMEM((ffn, dim), BF16), pltpu.VMEM((2, SHARD, ffn), BF16),
                      pltpu.VMEM((2, SHARD, dim), BF16), pltpu.SemaphoreType.DMA, sems(2), sems(2)])(x, w_o, hidden, w_down)


def attn_back_rs(d_query, d_knope, d_kpe, d_value, latent, g_kv, w_uk, w_uv, w_q, w_dkv, cos_t, sin_t, e_loc, g_attn, d_res, dg_mlp):
    heads, _, dim = w_q.shape
    lat = latent.shape[1]
    rank = w_uk.shape[1]
    wide = -(-(dim + lat) // LANES) * LANES
    others = (1, 2, 4, 3, 5, 6, 7)
    total = (1, g_kv.shape[1] + g_attn.shape[1] + dg_mlp.shape[1])

    def body(dq_ref, dk_ref, dkp_ref, dv_ref, l_ref, gkv_ref, wk_ref, wv_ref, wq_ref, wl_ref, cos_ref, sin_ref, e_ref, g_ref, res_ref, dgm_ref,
             de_ref, sum_ref, stage, fp, fx, fy, send, recv, parts, dgkv_ref, dgain_ref, gsend, grecv):
        t = lax.axis_index('tp')
        dgkv_ref[...] = jnp.zeros_like(dgkv_ref)
        dgain_ref[...] = jnp.zeros_like(dgain_ref)

        def produce(i, at):
            d_c = functools.reduce(jnp.add, [dot_nt(join(r, at, hd), w[hd]) for hd in range(heads) for r, w in ((dk_ref, wk_ref), (dv_ref, wv_ref))])
            d_kv, d_g = rms_back(join(l_ref, at)[:, :rank], gkv_ref[...], d_c.astype(BF16).astype(F32))
            dgkv_ref[...] = dgkv_ref[...] + d_g
            d_pe = functools.reduce(jnp.add, [join(dkp_ref, at, hd) for hd in range(heads)])
            d_pe = unrope(d_pe.astype(BF16).astype(F32), join(cos_ref, at), join(sin_ref, at))
            stage[i, :, dim:dim + rank] = d_kv.astype(BF16)
            stage[i, :, dim + rank:dim + lat] = d_pe.astype(BF16)
            stage[i, :, dim + lat:] = jnp.zeros((SHARD, wide - dim - lat), BF16)
            dl_b = stage[i, :, dim:dim + lat]
            dq_b = [join(dq_ref, at, hd) for hd in range(heads)]
            for cols in col_tiles(dim):
                val = dot_nn(dl_b, wl_ref[:, cols])
                for hd in range(heads):
                    val = val + dot_nn(dq_b[hd], wq_ref[hd, :, cols])
                stage[i, :, cols] = val.astype(BF16)

        def finish(at, val):
            d_x = back_rms_rows(e_ref, g_ref, dgain_ref, at, val[:, :dim])
            de_ref[at, :dim] = (res_ref[at, :] + d_x).astype(BF16)
            de_ref[at, dim:] = val[:, dim:].astype(BF16)

        rs_run(stage, fp, fx, fy, send, recv, produce, finish, others=others)
        first = 0
        for ref in (dgkv_ref, dgain_ref, dgm_ref):
            parts[t, :, first:first + ref.shape[1]] = ref[...]
            first += ref.shape[1]
        copies = [send_to(parts.at[t], parts.at[t], gsend.at[n], grecv.at[n], xor_bits(t, u)) for n, u in enumerate(others)]
        for c in copies:
            c.start()
        for c in copies:
            c.wait()
        sum_ref[...] = functools.reduce(jnp.add, [parts[d] for d in range(STEPS)])

    count = len(others)
    return comm_call(body, 'attn_back_rs', 6, [VM] * 16, [VM] * 2, [struct(BF16, SHARD, wide), struct(F32, *total)],
                     rs_scratch(wide) + [pltpu.VMEM((STEPS,) + total, F32), pltpu.VMEM(g_kv.shape, F32), pltpu.VMEM(g_attn.shape, F32), sems(count), sems(count)])(
                         d_query, d_knope, d_kpe, d_value, latent, g_kv, w_uk, w_uv, w_q, w_dkv, cos_t, sin_t, e_loc, g_attn, d_res, dg_mlp)


def gather_seq(x):
    return lax.all_gather(x, 'tp', axis=0, tiled=True)


def scatter_seq(x):
    return lax.psum_scatter(x, 'tp', scatter_dimension=0, tiled=True)


def solution(mesh):
    def device_step(tokens, embed_table, w_q, w_dkv, g_kv, w_uk, w_uv, w_o, g_attn, g_mlp, w_gate, w_up, w_down, d_out):
        vocab_local, model_dim = embed_table.shape
        seq = tokens.shape[1]
        heads, qk = w_q.shape[1:]
        vdim = w_uv.shape[2]
        scale = qk ** -0.5
        dy_loc = d_out[0]
        gkv, gat, gml = g_kv.reshape(1, -1), g_attn.reshape(1, -1), g_mlp.reshape(1, -1)
        wuk, wuv, wq = (jnp.moveaxis(w, 1, 0) for w in (w_uk, w_uv, w_q))
        wq, wl, wg, wu = jnp.swapaxes(wq, 1, 2), w_dkv.T, w_gate.T, w_up.T
        wo = w_o.reshape(heads * vdim, model_dim)
        cos_t, sin_t = rope_tables(seq, qk - w_uk.shape[2])

        dy_full = gather_seq(dy_loc)
        local_ids = tokens[0] - lax.axis_index('tp') * vocab_local
        owned = (local_ids >= 0) & (local_ids < vocab_local)
        slots, pos = lax.sort((jnp.where(owned, local_ids, vocab_local), lax.iota(jnp.int32, seq)), num_keys=1)
        slots = jnp.concatenate([slots, jnp.full((128,), vocab_local, jnp.int32)])
        cnt = jnp.sum(owned.astype(jnp.int32)).reshape(1)
        rows = gather_rows(slots, pos, cnt, embed_table, seq)
        e_loc, u_loc = rs_rows(rows, gat)
        u, q, latent, c_kv, k, kt, v, vt = ag_proj(u_loc, wq, wl, gkv, wuk, wuv, cos_t, sin_t)
        o, lse = attn_fwd(q, k, vt, scale)
        h_loc, z_loc, d_hidden = attn_out_rs(o, wo, e_loc, gml, dy_full, w_down)
        z, hidden, d_gate, d_up, d_res, d_res_b, dg_mlp = mlp_block(z_loc, d_hidden, wg, wu, h_loc, gml, dy_loc)
        d_res_full, d_o, mlp_part = ag_dattn(d_res_b, wo, hidden, w_down)

        mlp_loc = scatter_seq(mlp_part)
        half = cos_t.shape[1] // 2
        d_query, d_knope, d_kpe, d_value, zeros = attn_bwd(q, k, kt, v, d_o, o, lse, cos_t[:, :half].T, sin_t[:, half:].T, scale, embed_table.shape)
        dw_up = matmul_f32('sf,sd->fd', d_up, z)
        dw_up, d_query = lax.optimization_barrier((dw_up, d_query))
        layer_out = (h_loc.astype(F32) + mlp_loc.astype(F32)).astype(BF16)
        back, gains = attn_back_rs(d_query, d_knope, d_kpe, d_value, latent, gkv, wuk, wuv, wq, wl, cos_t, sin_t, e_loc, gat, d_res, dg_mlp)

        back_full = gather_seq(back)
        dw_gate = matmul_f32('sf,sd->fd', d_gate, z)
        dw_down = matmul_f32('sf,sd->fd', hidden, dy_full)
        dw_q = matmul_f32('sd,hse->dhe', u, d_query)
        dw_uk = matmul_f32('sc,hse->che', c_kv, d_knope)
        dw_uv = matmul_f32('sc,hsv->chv', c_kv, d_value)
        dw_o = matmul_f32('sv,sd->vd', o, d_res_full).reshape(w_o.shape)
        back_full, dw_gate, dw_down, dw_q, dw_o = lax.optimization_barrier((back_full, dw_gate, dw_down, dw_q, dw_o))
        dw_gate, dw_up = dw_gate.T, dw_up.T
        dw_dkv = matmul_f32('sc,sd->cd', back_full[:, model_dim:model_dim + w_dkv.shape[1]], u).T
        d_table = scatter_rows(slots, pos, cnt, back_full, zeros)
        gains = gains[0]
        rank = g_kv.shape[0]
        dg_kv, dg_attn, dg_mlp = gains[:rank], gains[rank:rank + model_dim], gains[rank + model_dim:]
        return layer_out[None], d_table, dw_q, dw_dkv, dg_kv, dw_uk, dw_uv, dw_o, dg_attn, dg_mlp, dw_gate, dw_up, dw_down

    row_spec = P('dp', 'tp', None)
    head_spec = P(None, 'tp', None)
    in_specs = (P('dp', None), P('tp', None), head_spec, P(None, None), P(None), head_spec, head_spec, P('tp', None, None), P(None), P(None), P(None, 'tp'), P(None, 'tp'), P('tp', None), row_spec)
    out_specs = (row_spec, P(('dp', 'tp'), None), P('dp', 'tp', None), P('dp', None), P('dp'), P('dp', 'tp', None), P('dp', 'tp', None), P(('dp', 'tp'), None, None), P('dp'), P('dp'), P('dp', 'tp'), P('dp', 'tp'), P(('dp', 'tp'), None))
    return jax.shard_map(device_step, mesh=mesh, in_specs=in_specs, out_specs=out_specs, check_vma=False)
```

```python
import functools

import jax
import jax.numpy as jnp
import numpy as np
from jax import lax
from jax.experimental import pallas as pl
from jax.experimental.pallas import tpu as pltpu
from jax.sharding import PartitionSpec as P

EPSILON = 1e-6
ROPE_BASE = 10000.0
LOG2E = 1.4426950408889634
BLK = 256
RING = 16
LANES = 128
ROWS = 64
VMEM_CAP = 60 * 1024 * 1024
BUSY = 40_000_000_000
NEG = -1e30
F32 = jnp.float32
BF16 = jnp.bfloat16


def matmul_f32(form, lhs, rhs):
    return jnp.einsum(form, lhs, rhs, preferred_element_type=jnp.float32)


def dot_nn(a, b):
    return jnp.dot(a, b, preferred_element_type=F32)


def dot_nt(a, b):
    return lax.dot_general(a, b, (((1,), (1,)), ((), ())), preferred_element_type=F32)


def tile(i):
    return slice(i * BLK, (i + 1) * BLK)


def rows_at(first, count):
    return pl.ds(pl.multiple_of(first, count), count)


def sems(*shape):
    return pltpu.SemaphoreType.DMA(shape)


def loop(count, step):
    def body(i, carry):
        step(i)
        return carry

    lax.fori_loop(0, count, body, 0)


VM = pl.BlockSpec(memory_space=pltpu.VMEM)
ANY = pl.BlockSpec(memory_space=pl.ANY)


def rope_tables(seq_len, rope_dim):
    inv_freq = np.float32(ROPE_BASE) ** (-np.arange(0, rope_dim, 2, dtype=np.float32) / np.float32(rope_dim))
    angles = (np.arange(seq_len, dtype=np.float32)[:, None] * inv_freq[None, :]).astype(np.float64)
    cos, sin = np.cos(angles), np.sin(angles)
    return (jnp.asarray(np.concatenate([cos, cos], axis=1), dtype=F32), jnp.asarray(np.concatenate([-sin, sin], axis=1), dtype=F32))


def swap_halves(x):
    half = x.shape[1] // 2
    return jnp.concatenate([x[:, half:], x[:, :half]], axis=1)


def rope(x, cos_t, sin_t):
    return x * cos_t + swap_halves(x) * sin_t


def unrope(x, cos_t, sin_t):
    return x * cos_t - swap_halves(x) * sin_t


def rms_inv(x):
    return lax.rsqrt(jnp.mean(x * x, axis=-1, keepdims=True) + EPSILON)


def rms_back(x, gain, dy):
    inv = rms_inv(x)
    gd = dy * gain
    mix = jnp.mean(gd * x, axis=-1, keepdims=True)
    return inv * gd - x * (inv * inv * inv * mix), jnp.sum(dy * (x * inv), axis=0, keepdims=True)


def gather_body(slot_ref, pos_ref, cnt_ref, tab_ref, out_ref, buf, acc, sem):
    seq, dim = acc.shape
    cnt = cnt_ref[0]

    def fetch(k):
        return pltpu.make_async_copy(tab_ref.at[rows_at(slot_ref[k] // 8 * 8, 8), :], buf.at[k % RING], sem.at[k % RING])

    loop(jnp.minimum(cnt, RING), lambda k: fetch(k).start())

    def clear(i):
        acc[rows_at(i * ROWS, ROWS), :] = jnp.zeros((ROWS, dim), F32)

    loop(seq // ROWS, clear)
    rows = lax.broadcasted_iota(jnp.int32, buf.shape[1:], 0)

    def step(k):
        fetch(k).wait()
        picked = jnp.where(rows == slot_ref[k] % 8, buf[k % RING].astype(F32), 0.0)
        acc[pl.ds(pos_ref[k], 1), :] = jnp.sum(picked, axis=0, keepdims=True)

        @pl.when(k + RING < cnt)
        def _():
            fetch(k + RING).start()

    loop(cnt, step)

    def emit(i):
        at = rows_at(i * ROWS, ROWS)
        out_ref[at, :] = acc[at, :].astype(BF16)

    loop(seq // ROWS, emit)


def local_call(body, name, out, in_specs, out_specs, scratch, scalars=0, grid=(1,), **extra):
    return pl.pallas_call(
        body, name=name, out_shape=out,
        grid_spec=pltpu.PrefetchScalarGridSpec(num_scalar_prefetch=scalars, grid=grid, in_specs=in_specs, out_specs=out_specs, scratch_shapes=scratch),
        compiler_params=pltpu.CompilerParams(vmem_limit_bytes=VMEM_CAP),
        cost_estimate=pl.CostEstimate(flops=BUSY // 2, bytes_accessed=BUSY // 2000, transcendentals=0), **extra)


def whole(*shape):
    return pl.BlockSpec(shape, lambda i, *_: (0,) * len(shape))


def gather_rows(slots, pos, cnt, table, seq):
    dim = table.shape[1]
    return local_call(gather_body, 'gather_rows', jax.ShapeDtypeStruct((seq, dim), BF16), [ANY], whole(seq, dim),
                      [pltpu.VMEM((RING, 8, dim), BF16), pltpu.VMEM((seq, dim), F32), sems(RING)], 3)(slots, pos, cnt, table)


def scatter_body(slot_ref, pos_ref, cnt_ref, de_ref, zero_ref, out_ref, wide, acc, stage, sem, near, nsem):
    seq, dim = wide.shape

    def load(i):
        at = rows_at(i * BLK, BLK)
        return pltpu.make_async_copy(de_ref.at[at, pl.ds(0, dim)], near.at[at, :], nsem.at[i])

    loop(seq // BLK, lambda i: load(i).start())

    def widen(i):
        load(i).wait()
        at = rows_at(i * BLK, BLK)
        wide[at, :] = near[at, :].astype(F32)

    loop(seq // BLK, widen)

    def put(blk, n):
        return pltpu.make_async_copy(stage.at[n % RING], out_ref.at[rows_at(blk * 8, 8), :], sem.at[n % RING])

    def step(k, carry):
        prev, n = carry
        slot = slot_ref[k]
        blk = slot // 8

        @pl.when(blk != prev)
        def _():
            acc[...] = jnp.zeros_like(acc)

        at = pl.ds(slot % 8, 1)
        acc[at, :] = acc[at, :] + wide[pl.ds(pos_ref[k], 1), :]
        last = slot_ref[k + 1] // 8 != blk

        @pl.when(last)
        def _():
            @pl.when(n >= RING)
            def _():
                put(blk, n).wait()

            stage[n % RING] = acc[...].astype(BF16)
            put(blk, n).start()

        return blk, n + last.astype(jnp.int32)

    _, total = lax.fori_loop(0, cnt_ref[0], step, (jnp.int32(-1), jnp.int32(0)))
    loop(jnp.minimum(total, RING), lambda i: put(0, total - 1 - i).wait())


def scatter_rows(slots, pos, cnt, de, zeros):
    seq, dim = de.shape[0], zeros.shape[1]
    return local_call(scatter_body, 'scatter_rows', jax.ShapeDtypeStruct(zeros.shape, BF16), [ANY, ANY], ANY,
                      [pltpu.VMEM((seq, dim), F32), pltpu.VMEM((8, dim), F32), pltpu.VMEM((RING, 8, dim), BF16), sems(RING), pltpu.VMEM((seq, dim), BF16), sems(seq // BLK)], 3, input_output_aliases={4: 0})(slots, pos, cnt, de, zeros)


def causal_tile():
    shape = (BLK, BLK)
    return lax.broadcasted_iota(jnp.int32, shape, 0) <= lax.broadcasted_iota(jnp.int32, shape, 1)


def fold(op, parts):
    total = functools.reduce(lambda a, b: a + b if op is jnp.sum else jnp.maximum(a, b), parts)
    return op(total, axis=0, keepdims=True)


def by_eight(op, x):
    return op(x.reshape(-1, 8, BLK), axis=0)


def attn_fwd_body(scale2, q_ref, k_ref, vt_ref, o_ref, lse_ref, s_scr):
    tri = causal_tile()
    for i in range(q_ref.shape[1] // BLK):
        q_i = q_ref[0, tile(i), :]
        tops = []
        for j in range(i + 1):
            s = dot_nt(k_ref[0, tile(j), :], q_i) * scale2
            if j == i:
                s = jnp.where(tri, s, NEG)
            s_scr[tile(j), :] = s
            tops.append(by_eight(jnp.max, s))
        top = fold(jnp.max, tops)
        dens = []
        for j in range(i + 1):
            e = jnp.exp2(s_scr[tile(j), :] - top)
            s_scr[tile(j), :] = e
            dens.append(by_eight(jnp.sum, e))
        den = fold(jnp.sum, dens)
        inv = 1.0 / den
        out = [dot_nn(vt_ref[0, :, tile(j)], (s_scr[tile(j), :] * inv).astype(BF16)) for j in range(i + 1)]
        o_ref[tile(i), :] = functools.reduce(jnp.add, out).T.astype(BF16)
        lse_ref[0, :, tile(i)] = top + jnp.log2(den)


def per_head(*shape):
    return pl.BlockSpec((1,) + shape, lambda h: (h, 0, 0))


def head_cols(seq, width):
    return pl.BlockSpec((seq, width), lambda h: (0, h))


def attn_fwd(q, k, vt, scale):
    heads, seq, qk = q.shape
    vdim = vt.shape[1]
    return local_call(functools.partial(attn_fwd_body, scale * LOG2E), 'attn_fwd',
                      [jax.ShapeDtypeStruct((seq, heads * vdim), BF16), jax.ShapeDtypeStruct((heads, 1, seq), F32)],
                      [per_head(seq, qk), per_head(seq, qk), per_head(vdim, seq)], [head_cols(seq, vdim), per_head(1, seq)],
                      [pltpu.VMEM((seq, BLK), F32)], grid=(heads,))(q, k, vt)


def attn_bwd_body(scale2, scale, q_ref, k_ref, kt_ref, v_ref, do_ref, o_ref, lse_ref, cos_ref, sin_ref, dq_ref, dk_ref, dkp_ref, dv_ref, zero_ref, p_scr, ds_scr, dlt, blank, zsem):
    seq = q_ref.shape[1]
    nope = dk_ref.shape[2]
    n = seq // BLK
    head = pl.program_id(0)
    size = blank.shape[0]
    fills = [pltpu.make_async_copy(blank, zero_ref.at[pl.ds(m * size, size), :], zsem.at[m]) for m in range(zsem.shape[0])]

    @pl.when(head == 0)
    def _():
        blank[...] = jnp.zeros_like(blank)
        for c in fills:
            c.start()

    tri = causal_tile()
    for i in range(n):
        both = do_ref[tile(i), :].astype(F32) * o_ref[tile(i), :].astype(F32)
        dlt[:, tile(i)] = jnp.sum(both.T, axis=0, keepdims=True)
    for j in range(n):
        k_j = k_ref[0, tile(j), :]
        v_j = v_ref[0, tile(j), :]
        for i in range(j, n):
            s = dot_nt(k_j, q_ref[0, tile(i), :])
            prob = jnp.exp2(s * scale2 - lse_ref[0, :, tile(i)])
            if i == j:
                prob = jnp.where(tri, prob, 0.0)
            dp = dot_nt(v_j, do_ref[tile(i), :])
            p_scr[:, tile(i)] = prob.astype(BF16)
            ds_scr[tile(j), tile(i)] = (prob * (dp - dlt[:, tile(i)])).astype(BF16)
        rest = slice(j * BLK, seq)
        dv_ref[0, tile(j), :] = dot_nn(p_scr[:, rest], do_ref[rest, :]).astype(BF16)
        dk = dot_nn(ds_scr[tile(j), rest], q_ref[0, rest, :]) * scale
        dk_ref[0, tile(j), :] = dk[:, :nope].astype(BF16)
        dkp_ref[0, tile(j), :] = dk[:, nope:]

    half = cos_ref.shape[0]
    for i in range(n):
        seen = slice(0, (i + 1) * BLK)
        dq = dot_nn(kt_ref[0, :, seen], ds_scr[seen, tile(i)]) * scale
        lo, hi = dq[nope:nope + half, :], dq[nope + half:, :]
        cos_b, sin_b = cos_ref[:, tile(i)], sin_ref[:, tile(i)]
        turned = jnp.concatenate([dq[:nope, :], lo * cos_b + hi * sin_b, hi * cos_b - lo * sin_b], axis=0)
        dq_ref[0, tile(i), :] = turned.T.astype(BF16)

    @pl.when(head == pl.num_programs(0) - 1)
    def _():
        for c in fills:
            c.wait()


def attn_bwd(q, k, kt, v, do, o, lse, cos_t, sin_t, scale, table):
    heads, seq, qk = q.shape
    vdim = v.shape[2]
    half = cos_t.shape[0]
    pe = half + half
    outs = [((seq, qk), BF16), ((seq, qk - pe), BF16), ((seq, pe), F32), ((seq, vdim), BF16)]
    return local_call(functools.partial(attn_bwd_body, scale * LOG2E, scale), 'attn_bwd', [jax.ShapeDtypeStruct((heads,) + s, d) for s, d in outs] + [jax.ShapeDtypeStruct(table, BF16)],
                      [per_head(seq, qk), per_head(seq, qk), per_head(qk, seq), per_head(seq, vdim), head_cols(seq, vdim), head_cols(seq, vdim), per_head(1, seq), whole(half, seq), whole(half, seq)],
                      [per_head(*s) for s, _ in outs] + [ANY],
                      [pltpu.VMEM((BLK, seq), BF16), pltpu.VMEM((seq, seq), BF16), pltpu.VMEM((1, seq), F32), pltpu.VMEM((table[0] // RING,) + table[1:], BF16), sems(RING)],
                      grid=(heads,))(q, k, kt, v, do, o, lse, cos_t, sin_t)


HALF = 128
SHARD = 256
STEPS = 8
PEERS = (1, 2, 4)
MESH = pl.DeviceIdType.MESH


def xor_bits(t, u):
    out = 0
    for b in (1, 2, 4):
        tb = (t // b) % 2
        ub = (u // b) % 2
        out = out + b * (tb + ub - 2 * tb * ub)
    return out


def greet(t, others):
    peers = [xor_bits(t, u) for u in others]
    barrier = pltpu.get_barrier_semaphore()
    for peer in peers:
        pl.semaphore_signal(barrier, inc=1, device_id={'tp': peer}, device_id_type=MESH)
    pl.semaphore_wait(barrier, len(peers))
    return peers


def send_to(src, dst, send, recv, dev):
    return pltpu.make_async_remote_copy(src_ref=src, dst_ref=dst, send_sem=send, recv_sem=recv, device_id={'tp': dev}, device_id_type=MESH)


def piece_id(m, j):
    i = 2 * m + j // 2
    p, r = i // 4, i % 4
    first, last = (3 - p) // 3, p // 3
    mid = 1 - first - last
    u = first * (r // 2) + mid * (2 + (r % 2) * 2 + r // 2)
    h = r % 2 + (p - 1) * mid * (1 - 2 * (r % 2))
    near = 1 - last
    return u + last * (6 + j // 2), near * h + last * (j % 2), near * (j % 2) + last * (m % 2)


def piece(t, m, j):
    u, h, a = piece_id(m, j)
    return rows_at(xor_bits(t, u) * SHARD + h * HALF + a * ROWS, ROWS)


def pieces(t, m):
    return [piece(t, m, j) for j in range(4)]


def quarter(j):
    return pl.ds(j * ROWS, ROWS)


def join(ref, at, *lead):
    return jnp.concatenate([ref[lead + (r, slice(None))] for r in at], axis=0)


def begin(i, loads, ins, outs):
    @pl.when(i == 0)
    def _():
        for c in loads:
            c.wait()

    @pl.when(i < STEPS - 1)
    def _():
        for c in ins(i + 1):
            c.start()

    @pl.when(i >= 2)
    def _():
        for c in outs(i - 2):
            c.wait()

    for c in ins(i):
        c.wait()


def finish_all(outs):
    for i in (STEPS - 2, STEPS - 1):
        for c in outs(i):
            c.wait()


def ag_run(x_ref, full, send, recv, compute, before=None, peers=None):
    t = lax.axis_index('tp')
    partner, xn, yn = peers or greet(t, PEERS)
    sends = []

    def copy(src, shard, first, count, u_there, dev):
        place = rows_at(shard * SHARD + first, count)
        slot = first // ROWS
        c = send_to(src, full.at[place, :], send.at[len(sends)], recv.at[u_there, slot], dev)
        sends.append(c)
        return c

    def mine(h, u, dev):
        return copy(x_ref.at[pl.ds(h * HALF, HALF), :], t, h * HALF, HALF, u, dev)

    def relay(u, first, count, u_there, dev):
        shard = xor_bits(t, u)
        return copy(full.at[rows_at(shard * SHARD + first, count), :], shard, first, count, u_there, dev)

    for h, u, dev in ((0, 2, xn), (1, 4, yn), (0, 1, partner), (1, 1, partner), (1, 2, xn), (0, 4, yn)):
        mine(h, u, dev).start()
    full[rows_at(t * SHARD, SHARD), :] = x_ref[...]
    onward = {(u, h): [relay(u, h * HALF, HALF, u + 1, partner)] for u in (2, 4) for h in (0, 1)}
    for a in (0, 1):
        onward[2, 0].append(relay(2, a * ROWS, ROWS, 6, yn))
        onward[4, 1].append(relay(4, HALF + a * ROWS, ROWS, 6, xn))
    far = {(h, a): relay(6, h * HALF + a * ROWS, ROWS, 7, partner) for h in (0, 1) for a in (0, 1)}

    def arrive(u, first, count):
        place = full.at[rows_at(xor_bits(t, u) * SHARD + first, count), :]
        send_to(place, place, send.at[0], recv.at[u, first // ROWS], partner).wait_recv()

    def step(i):
        if before is not None:
            before(i)
        for m in range(1, 6):
            @pl.when(i == m)
            def _(m=m):
                for j in (0, 2):
                    u, h, _ = piece_id(m, j)
                    arrive(u, h * HALF, HALF)
                    for c in onward.get((u, h), ()):
                        c.start()

        for a in (0, 1):
            @pl.when(i == 6 + a)
            def _(a=a):
                for h in (0, 1):
                    arrive(6, h * HALF + a * ROWS, ROWS)
                    far[h, a].start()
                for h in (0, 1):
                    arrive(7, h * HALF + a * ROWS, ROWS)

        compute(i, pieces(t, i))

    loop(STEPS, step)
    for c in sends:
        c.wait_send()


AG_SEMS = [sems(18), sems(8, 4)]


def rs_run(stage, fp, fx, fy, send, recv, produce, finish, after=None, others=PEERS, peers=None):
    t = lax.axis_index('tp')
    partner, xn, yn, *_ = peers or greet(t, others)
    sends = []

    def copy(src, dst, dev):
        n = len(sends)
        c = send_to(src, dst, send.at[n], recv.at[n], dev)
        sends.append(c)
        return c

    first, second = pl.ds(0, HALF), pl.ds(HALF, HALF)
    swap = [copy(stage.at[k, second, :], fp.at[0, pl.ds(k * HALF, HALF), :], partner) for k in (0, 1)]
    swap += [copy(stage.at[2 * p], fp.at[p], partner) for p in (1, 2, 3)]
    far_y = [copy(stage.at[k, quarter(0), :], fy.at[0, quarter(1 - k), :], yn) for k in (0, 1)]
    far_x = [copy(stage.at[k, quarter(1), :], fx.at[0, quarter(1 - k), :], xn) for k in (0, 1)]
    near_x, near_y = copy(stage.at[3, first, :], fx.at[1], xn), copy(stage.at[3, second, :], fy.at[1], yn)
    via_x, via_y = copy(stage.at[5, first, :], fx.at[2], xn), copy(stage.at[5, second, :], fy.at[2], yn)

    def add(i, start, count, src, src_start):
        def body(r):
            a = rows_at(start + r * 32, 32)
            stage[i, a, :] = (stage[i, a, :].astype(F32) + src[rows_at(src_start + r * 32, 32), :].astype(F32)).astype(BF16)

        loop(count // 32, body)

    def step(i):
        produce(i, pieces(t, STEPS - 1 - i))
        for k in (0, 1):
            @pl.when(i == k)
            def _(k=k):
                swap[k].start()
                swap[k].wait_recv()
                add(k, 0, HALF, fp.at[0], k * HALF)
                far_x[k].start()
                far_y[k].start()

        for p in (1, 2, 3):
            @pl.when(i == 2 * p)
            def _(p=p):
                swap[p + 1].start()

            @pl.when(i == 2 * p + 1)
            def _(p=p):
                swap[p + 1].wait_recv()
                add(2 * p + 1, 0, SHARD, fp.at[p], 0)

        @pl.when(i == 3)
        def _():
            near_x.start()
            near_y.start()

        @pl.when(i == 5)
        def _():
            for c in far_y:
                c.wait_recv()
            add(5, 0, HALF, fy.at[0], 0)
            via_x.start()
            for c in far_x:
                c.wait_recv()
            add(5, HALF, HALF, fx.at[0], 0)
            via_y.start()

        if after is not None:
            @pl.when(i >= 1)
            def _():
                after(i - 1)

    loop(STEPS, step)
    if after is not None:
        after(STEPS - 1)
    for c in (near_x, near_y, via_x, via_y):
        c.wait_recv()

    def last(r):
        lo, hi = rows_at(r * 32, 32), rows_at(HALF + r * 32, 32)
        finish(lo, (stage[7, lo, :].astype(F32) + fy[1, lo, :].astype(F32)) + fx[2, lo, :].astype(F32))
        finish(hi, (stage[7, hi, :].astype(F32) + fx[1, lo, :].astype(F32)) + fy[2, lo, :].astype(F32))

    loop(HALF // 32, last)
    for c in sends:
        c.wait_send()


def rs_scratch(dim):
    return [pltpu.VMEM((n, rows, dim), BF16) for n, rows in ((STEPS, SHARD), (4, SHARD), (3, HALF), (3, HALF))] + [sems(13), sems(13)]


def comm_call(body, name, cid, in_specs, out_specs, out_shape, scratch):
    return pl.pallas_call(
        body, name=name, in_specs=in_specs, out_specs=out_specs, out_shape=out_shape, scratch_shapes=scratch,
        compiler_params=pltpu.CompilerParams(collective_id=cid, has_side_effects=True, vmem_limit_bytes=VMEM_CAP),
        cost_estimate=pl.CostEstimate(flops=BUSY, bytes_accessed=BUSY // 2000, transcendentals=0))


def col_tiles(width):
    return [slice(a, min(a + BLK, width)) for a in range(0, width, BLK)]


def struct(dtype, *shape):
    return jax.ShapeDtypeStruct(shape, dtype)


def back_rms_rows(x_ref, g_ref, dgain_ref, at, dy):
    d_x, d_g = rms_back(x_ref[at, :].astype(F32), g_ref[...], dy.astype(BF16).astype(F32))
    dgain_ref[...] = dgain_ref[...] + d_g
    return d_x


def embed_proj(rows, g_attn, w_q, w_dkv, g_kv, w_uk, w_uv, cos_t, sin_t):
    seq = cos_t.shape[0]
    heads, qk, dim = w_q.shape
    lat = w_dkv.shape[0]
    rank, nope = w_uk.shape[1:]
    vdim = w_uv.shape[2]

    def body(rows_ref, ga_ref, wq_ref, wl_hbm, g_ref, wk_ref, wv_ref, cos_ref, sin_ref, x_out, e_ref, q_ref, l_ref, c_ref, k_ref, kt_ref, v_ref, vt_ref,
             full, send, recv, sem, wl, wsem, u_ref, load, stage, fp, fx, fy, rs_send, rs_recv):
        t = lax.axis_index('tp')

        def fetch(i):
            return [pltpu.make_async_copy(rows_ref.at[at, :], stage.at[i, quarter(j), :], load.at[i, j]) for j, at in enumerate(pieces(t, STEPS - 1 - i))]

        for i in range(STEPS):
            for c in fetch(i):
                c.start()
        w_load = pltpu.make_async_copy(wl_hbm, wl, wsem)
        w_load.start()
        peers = greet(t, PEERS)

        def produce(i, at):
            for c in fetch(i):
                c.wait()

        def finish(at, val):
            e_b = val.astype(BF16)
            e_ref[at, :] = e_b
            x = e_b.astype(F32)
            u_ref[at, :] = (x * rms_inv(x) * ga_ref[...]).astype(BF16)

        rs_run(stage, fp, fx, fy, rs_send, rs_recv, produce, finish, peers=peers)

        def x_copies(i):
            return [pltpu.make_async_copy(full.at[at, :], x_out.at[at, :], sem.at[i, j]) for j, at in enumerate(pieces(t, i))]

        def turn(m, j):
            u, h, _ = piece_id(m, j)
            at = rows_at(xor_bits(t, u) * SHARD + h * HALF, HALF)
            for hd in range(heads):
                kt_ref[hd, :, at] = k_ref[hd, at, :].astype(F32).T.astype(BF16)
                vt_ref[hd, :, at] = v_ref[hd, at, :].astype(F32).T.astype(BF16)

        def compute(i, rows):
            @pl.when(i == 0)
            def _():
                w_load.wait()

            for c in x_copies(i):
                c.start()
            x_b = join(full, rows)
            l_b = dot_nt(x_b, wl[...])
            kv = l_b[:, :rank]
            c_b = (kv * rms_inv(kv) * g_ref[...]).astype(BF16)
            cos_b, sin_b = join(cos_ref, rows), join(sin_ref, rows)
            pe_b = rope(l_b[:, rank:], cos_b, sin_b).astype(BF16)

            def put(ref, val, *lead, cols=slice(None)):
                for j, at in enumerate(rows):
                    ref[lead + (at, cols)] = val[j * ROWS:(j + 1) * ROWS, :]

            put(l_ref, l_b)
            put(c_ref, c_b)
            for hd in range(heads):
                q_b = dot_nt(x_b, wq_ref[hd]).astype(BF16)
                put(q_ref, q_b[:, :nope], hd, cols=slice(0, nope))
                put(q_ref, rope(q_b[:, nope:].astype(F32), cos_b, sin_b).astype(BF16), hd, cols=slice(nope, qk))
                put(k_ref, dot_nn(c_b, wk_ref[hd]).astype(BF16), hd, cols=slice(0, nope))
                put(k_ref, pe_b, hd, cols=slice(nope, qk))
                put(v_ref, dot_nn(c_b, wv_ref[hd]).astype(BF16), hd)

            @pl.when(i < 6)
            def _():
                turn(i, 0)
                turn(i, 2)

            @pl.when(i == STEPS - 1)
            def _():
                for j in range(4):
                    turn(STEPS - 1, j)

        ag_run(u_ref, full, send, recv, compute, peers=peers)
        for i in range(STEPS):
            for c in x_copies(i):
                c.wait()

    per = [struct(BF16, SHARD, dim), struct(BF16, heads, seq, qk), struct(F32, seq, lat), struct(BF16, seq, rank), struct(BF16, heads, seq, qk), struct(BF16, heads, qk, seq), struct(BF16, heads, seq, vdim), struct(BF16, heads, vdim, seq)]
    return comm_call(body, 'embed_proj', 1, [ANY, VM, VM, ANY] + [VM] * 5, [ANY] + [VM] * len(per), [struct(BF16, seq, dim)] + per,
                     [pltpu.VMEM((seq, dim), BF16)] + AG_SEMS + [sems(STEPS, 4), pltpu.VMEM((lat, dim), BF16), pltpu.SemaphoreType.DMA, pltpu.VMEM((SHARD, dim), BF16), sems(STEPS, 4)] + rs_scratch(dim))(
                         rows, g_attn, w_q, w_dkv, g_kv, w_uk, w_uv, cos_t, sin_t)


def shard_rows(i):
    return rows_at(i * SHARD, SHARD)


def stream_copies(ref, buf, sem, out=False):
    def copies(i):
        a, b = ref.at[shard_rows(i), :], buf.at[i % 2]
        return [pltpu.make_async_copy(b, a, sem.at[i % 2]) if out else pltpu.make_async_copy(a, b, sem.at[i % 2])]

    return copies


def attn_out_rs(o, w_o, e_loc, gain, dy, w_down):
    seq, dim = dy.shape
    ffn = w_down.shape[0]

    def body(o_ref, w_ref, e_ref, g_ref, dy_ref, wd_hbm, h_ref, z_ref, dh_ref, stage, fp, fx, fy, send, recv, wd, dyb, st, wsem, dsem, osem):
        ins, outs = stream_copies(dy_ref, dyb, dsem), stream_copies(dh_ref, st, osem, True)
        w_load = pltpu.make_async_copy(wd_hbm, wd, wsem)
        for c in ins(0) + [w_load]:
            c.start()

        def produce(i, at):
            o_b = join(o_ref, at)
            for cols in col_tiles(dim):
                stage[i, :, cols] = dot_nn(o_b, w_ref[:, cols]).astype(BF16)

        def after(i):
            begin(i, [w_load], ins, outs)
            dy_b = dyb[i % 2]
            for cols in col_tiles(ffn):
                st[i % 2, :, cols] = dot_nt(dy_b, wd[cols, :])
            for c in outs(i):
                c.start()

        def finish(at, val):
            h_b = (e_ref[at, :].astype(F32) + val.astype(BF16).astype(F32)).astype(BF16)
            h_ref[at, :] = h_b
            x = h_b.astype(F32)
            z_ref[at, :] = (x * rms_inv(x) * g_ref[...]).astype(BF16)

        rs_run(stage, fp, fx, fy, send, recv, produce, finish, after)
        finish_all(outs)

    loc = struct(BF16, SHARD, dim)
    return comm_call(body, 'attn_out_rs', 2, [VM] * 4 + [ANY] * 2, [VM, VM, ANY], [loc, loc, struct(F32, seq, ffn)],
                     rs_scratch(dim) + [pltpu.VMEM((ffn, dim), BF16), pltpu.VMEM((2, SHARD, dim), BF16), pltpu.VMEM((2, SHARD, ffn), F32),
                                        pltpu.SemaphoreType.DMA, sems(2), sems(2)])(o, w_o, e_loc, gain, dy, w_down)


def mlp_block(z, dh, w_gate, w_up, h_loc, gain, dy):
    seq, ffn = dh.shape
    dim = z.shape[1]

    def body(z_ref, dh_ref, wg_hbm, wu_hbm, h_ref, g_ref, dy_ref, z_out, hid_out, dg_out, du_out, res_ref, resb_ref, dgain_ref,
             full, wg, wu, dhb, st, dg, du, wsem, dsem, osem, gsem, send, recv, stage, fp, fx, fy, rs_send, rs_recv):
        t = lax.axis_index('tp')
        peers = greet(t, PEERS)
        loads = [pltpu.make_async_copy(a, b, wsem.at[n]) for n, (a, b) in enumerate(((wg_hbm, wg), (wu_hbm, wu)))]

        def ins(i):
            return [pltpu.make_async_copy(dh_ref.at[at, :], dhb.at[i % 2, quarter(j), :], dsem.at[i % 2, j]) for j, at in enumerate(pieces(t, i))]

        def outs(i):
            return [pltpu.make_async_copy(st.at[i % 2, quarter(j), :], hid_out.at[at, :], osem.at[i % 2, j]) for j, at in enumerate(pieces(t, i))]

        def kept(i):
            return [pltpu.make_async_copy(a.at[at, :], b.at[at, :], gsem.at[n, i, j])
                    for n, (a, b) in enumerate(((full, z_out), (dg, dg_out), (du, du_out))) for j, at in enumerate(pieces(t, i))]

        for c in loads + ins(0):
            c.start()
        dgain_ref[...] = jnp.zeros_like(dgain_ref)

        def compute(i, rows):
            begin(i, loads, ins, outs)
            z_b = join(full, rows)
            for cols in col_tiles(ffn):
                gate = dot_nt(z_b, wg[cols, :])
                up = dot_nt(z_b, wu[cols, :])
                d_hid = dhb[i % 2, :, cols]
                sig = jax.nn.sigmoid(gate)
                act = gate * sig
                st[i % 2, :, cols] = (act * up).astype(BF16)
                for ref, val in ((dg, d_hid * up * sig * (1.0 + gate * (1.0 - sig))), (du, d_hid * act)):
                    for j, at in enumerate(rows):
                        ref[at, cols] = val[j * ROWS:(j + 1) * ROWS, :].astype(BF16)
            for c in outs(i) + kept(i):
                c.start()

        ag_run(z_ref, full, send, recv, compute, peers=peers)

        def produce(i, at):
            dg_b, du_b = join(dg, at), join(du, at)
            for cols in col_tiles(dim):
                stage[i, :, cols] = (dot_nn(dg_b, wg[:, cols]) + dot_nn(du_b, wu[:, cols])).astype(BF16)

        def finish(at, val):
            res = dy_ref[at, :].astype(F32) + back_rms_rows(h_ref, g_ref, dgain_ref, at, val)
            res_ref[at, :] = res
            resb_ref[at, :] = res.astype(BF16)

        rs_run(stage, fp, fx, fy, rs_send, rs_recv, produce, finish, peers=peers)
        finish_all(outs)
        for i in range(STEPS):
            for c in kept(i):
                c.wait()

    act = struct(BF16, seq, ffn)
    weight, wide = pltpu.VMEM((ffn, dim), BF16), pltpu.VMEM((seq, ffn), BF16)
    return comm_call(body, 'mlp_block', 3, [VM] + [ANY] * 3 + [VM] * 3, [ANY] * 4 + [VM] * 3,
                     [struct(BF16, seq, dim), act, act, act, struct(F32, SHARD, dim), struct(BF16, SHARD, dim), struct(F32, *gain.shape)],
                     [pltpu.VMEM((seq, dim), BF16), weight, weight, pltpu.VMEM((2, SHARD, ffn), F32), pltpu.VMEM((2, SHARD, ffn), BF16), wide, wide,
                      sems(2), sems(2, 4), sems(2, 4), sems(3, STEPS, 4)] + AG_SEMS + rs_scratch(dim))(z, dh, w_gate, w_up, h_loc, gain, dy)


def ag_dattn(x, w_o, hidden, w_down):
    seq, ffn = hidden.shape
    width, dim = w_o.shape

    def body(x_ref, w_ref, hid_ref, wd_hbm, x_out, do_ref, y_out, full, send, recv, sem, wd, hb, yb, wsem, hsem, ysem):
        t = lax.axis_index('tp')
        ins, outs = stream_copies(hid_ref, hb, hsem), stream_copies(y_out, yb, ysem, True)
        w_load = pltpu.make_async_copy(wd_hbm, wd, wsem)
        for c in ins(0) + [w_load]:
            c.start()

        def x_copies(i):
            return [pltpu.make_async_copy(full.at[at, :], x_out.at[at, :], sem.at[i, j]) for j, at in enumerate(pieces(t, i))]

        def before(i):
            begin(i, [w_load], ins, outs)
            h_b = hb[i % 2]
            for cols in col_tiles(dim):
                yb[i % 2, :, cols] = dot_nn(h_b, wd[:, cols]).astype(BF16)
            for c in outs(i):
                c.start()

        def compute(i, rows):
            for c in x_copies(i):
                c.start()
            d_o = dot_nt(join(full, rows), w_ref[...]).astype(BF16)
            for j, at in enumerate(rows):
                do_ref[at, :] = d_o[j * ROWS:(j + 1) * ROWS, :]

        ag_run(x_ref, full, send, recv, compute, before)
        finish_all(outs)
        for i in range(STEPS):
            for c in x_copies(i):
                c.wait()

    big = struct(BF16, seq, dim)
    return comm_call(body, 'ag_dattn', 5, [VM, VM, ANY, ANY], [ANY, VM, ANY], [big, struct(BF16, seq, width), big],
                     [pltpu.VMEM((seq, dim), BF16)] + AG_SEMS + [sems(STEPS, 4), pltpu.VMEM((ffn, dim), BF16), pltpu.VMEM((2, SHARD, ffn), BF16),
                      pltpu.VMEM((2, SHARD, dim), BF16), pltpu.SemaphoreType.DMA, sems(2), sems(2)])(x, w_o, hidden, w_down)


def attn_back_rs(d_query, d_knope, d_kpe, d_value, latent, g_kv, w_uk, w_uv, w_q, w_dkv, cos_t, sin_t, e_loc, g_attn, d_res, dg_mlp):
    heads, _, dim = w_q.shape
    lat = latent.shape[1]
    rank = w_uk.shape[1]
    wide = -(-(dim + lat) // LANES) * LANES
    others = (1, 2, 4, 3, 5, 6, 7)
    total = (1, g_kv.shape[1] + g_attn.shape[1] + dg_mlp.shape[1])

    def body(dq_ref, dk_ref, dkp_ref, dv_ref, l_ref, gkv_ref, wk_ref, wv_ref, wq_ref, wl_ref, cos_ref, sin_ref, e_ref, g_ref, res_ref, dgm_ref,
             de_ref, sum_ref, stage, fp, fx, fy, send, recv, parts, dgkv_ref, dgain_ref, gsend, grecv):
        t = lax.axis_index('tp')
        dgkv_ref[...] = jnp.zeros_like(dgkv_ref)
        dgain_ref[...] = jnp.zeros_like(dgain_ref)

        def produce(i, at):
            d_c = functools.reduce(jnp.add, [dot_nt(join(r, at, hd), w[hd]) for hd in range(heads) for r, w in ((dk_ref, wk_ref), (dv_ref, wv_ref))])
            d_kv, d_g = rms_back(join(l_ref, at)[:, :rank], gkv_ref[...], d_c.astype(BF16).astype(F32))
            dgkv_ref[...] = dgkv_ref[...] + d_g
            d_pe = functools.reduce(jnp.add, [join(dkp_ref, at, hd) for hd in range(heads)])
            d_pe = unrope(d_pe.astype(BF16).astype(F32), join(cos_ref, at), join(sin_ref, at))
            stage[i, :, dim:dim + rank] = d_kv.astype(BF16)
            stage[i, :, dim + rank:dim + lat] = d_pe.astype(BF16)
            stage[i, :, dim + lat:] = jnp.zeros((SHARD, wide - dim - lat), BF16)
            dl_b = stage[i, :, dim:dim + lat]
            dq_b = [join(dq_ref, at, hd) for hd in range(heads)]
            for cols in col_tiles(dim):
                val = dot_nn(dl_b, wl_ref[:, cols])
                for hd in range(heads):
                    val = val + dot_nn(dq_b[hd], wq_ref[hd, :, cols])
                stage[i, :, cols] = val.astype(BF16)

        def finish(at, val):
            d_x = back_rms_rows(e_ref, g_ref, dgain_ref, at, val[:, :dim])
            de_ref[at, :dim] = (res_ref[at, :] + d_x).astype(BF16)
            de_ref[at, dim:] = val[:, dim:].astype(BF16)

        rs_run(stage, fp, fx, fy, send, recv, produce, finish, others=others)
        first = 0
        for ref in (dgkv_ref, dgain_ref, dgm_ref):
            parts[t, :, first:first + ref.shape[1]] = ref[...]
            first += ref.shape[1]
        copies = [send_to(parts.at[t], parts.at[t], gsend.at[n], grecv.at[n], xor_bits(t, u)) for n, u in enumerate(others)]
        for c in copies:
            c.start()
        for c in copies:
            c.wait()
        sum_ref[...] = functools.reduce(jnp.add, [parts[d] for d in range(STEPS)])

    count = len(others)
    return comm_call(body, 'attn_back_rs', 6, [VM] * 16, [VM] * 2, [struct(BF16, SHARD, wide), struct(F32, *total)],
                     rs_scratch(wide) + [pltpu.VMEM((STEPS,) + total, F32), pltpu.VMEM(g_kv.shape, F32), pltpu.VMEM(g_attn.shape, F32), sems(count), sems(count)])(
                         d_query, d_knope, d_kpe, d_value, latent, g_kv, w_uk, w_uv, w_q, w_dkv, cos_t, sin_t, e_loc, g_attn, d_res, dg_mlp)


def gather_seq(x):
    return lax.all_gather(x, 'tp', axis=0, tiled=True)


def scatter_seq(x):
    return lax.psum_scatter(x, 'tp', scatter_dimension=0, tiled=True)


def solution(mesh):
    def device_step(tokens, embed_table, w_q, w_dkv, g_kv, w_uk, w_uv, w_o, g_attn, g_mlp, w_gate, w_up, w_down, d_out):
        vocab_local, model_dim = embed_table.shape
        seq = tokens.shape[1]
        heads, qk = w_q.shape[1:]
        vdim = w_uv.shape[2]
        scale = qk ** -0.5
        dy_loc = d_out[0]
        gkv, gat, gml = g_kv.reshape(1, -1), g_attn.reshape(1, -1), g_mlp.reshape(1, -1)
        wuk, wuv, wq = (jnp.moveaxis(w, 1, 0) for w in (w_uk, w_uv, w_q))
        wq, wl, wg, wu = jnp.swapaxes(wq, 1, 2), w_dkv.T, w_gate.T, w_up.T
        wo = w_o.reshape(heads * vdim, model_dim)
        cos_t, sin_t = rope_tables(seq, qk - w_uk.shape[2])

        dy_full = gather_seq(dy_loc)
        local_ids = tokens[0] - lax.axis_index('tp') * vocab_local
        owned = (local_ids >= 0) & (local_ids < vocab_local)
        slots, pos = lax.sort((jnp.where(owned, local_ids, vocab_local), lax.iota(jnp.int32, seq)), num_keys=1)
        slots = jnp.concatenate([slots, jnp.full((128,), vocab_local, jnp.int32)])
        cnt = jnp.sum(owned.astype(jnp.int32)).reshape(1)
        rows = gather_rows(slots, pos, cnt, embed_table, seq)
        u, e_loc, q, latent, c_kv, k, kt, v, vt = embed_proj(rows, gat, wq, wl, gkv, wuk, wuv, cos_t, sin_t)
        o, lse = attn_fwd(q, k, vt, scale)
        h_loc, z_loc, d_hidden = attn_out_rs(o, wo, e_loc, gml, dy_full, w_down)
        z, hidden, d_gate, d_up, d_res, d_res_b, dg_mlp = mlp_block(z_loc, d_hidden, wg, wu, h_loc, gml, dy_loc)
        d_res_full, d_o, mlp_part = ag_dattn(d_res_b, wo, hidden, w_down)

        mlp_loc = scatter_seq(mlp_part)
        half = cos_t.shape[1] // 2
        d_query, d_knope, d_kpe, d_value, zeros = attn_bwd(q, k, kt, v, d_o, o, lse, cos_t[:, :half].T, sin_t[:, half:].T, scale, embed_table.shape)
        dw_up = matmul_f32('sf,sd->fd', d_up, z)
        dw_up, d_query = lax.optimization_barrier((dw_up, d_query))
        layer_out = (h_loc.astype(F32) + mlp_loc.astype(F32)).astype(BF16)
        back, gains = attn_back_rs(d_query, d_knope, d_kpe, d_value, latent, gkv, wuk, wuv, wq, wl, cos_t, sin_t, e_loc, gat, d_res, dg_mlp)

        back_full = gather_seq(back)
        dw_gate = matmul_f32('sf,sd->fd', d_gate, z)
        dw_down = matmul_f32('sf,sd->fd', hidden, dy_full)
        dw_q = matmul_f32('sd,hse->dhe', u, d_query)
        dw_uk = matmul_f32('sc,hse->che', c_kv, d_knope)
        dw_uv = matmul_f32('sc,hsv->chv', c_kv, d_value)
        dw_o = matmul_f32('sv,sd->vd', o, d_res_full).reshape(w_o.shape)
        back_full, dw_gate, dw_down, dw_q, dw_o = lax.optimization_barrier((back_full, dw_gate, dw_down, dw_q, dw_o))
        dw_gate, dw_up = dw_gate.T, dw_up.T
        dw_dkv = matmul_f32('sc,sd->cd', back_full[:, model_dim:model_dim + w_dkv.shape[1]], u).T
        d_table = scatter_rows(slots, pos, cnt, back_full, zeros)
        gains = gains[0]
        rank = g_kv.shape[0]
        dg_kv, dg_attn, dg_mlp = gains[:rank], gains[rank:rank + model_dim], gains[rank + model_dim:]
        return layer_out[None], d_table, dw_q, dw_dkv, dg_kv, dw_uk, dw_uv, dw_o, dg_attn, dg_mlp, dw_gate, dw_up, dw_down

    row_spec = P('dp', 'tp', None)
    head_spec = P(None, 'tp', None)
    in_specs = (P('dp', None), P('tp', None), head_spec, P(None, None), P(None), head_spec, head_spec, P('tp', None, None), P(None), P(None), P(None, 'tp'), P(None, 'tp'), P('tp', None), row_spec)
    out_specs = (row_spec, P(('dp', 'tp'), None), P('dp', 'tp', None), P('dp', None), P('dp'), P('dp', 'tp', None), P('dp', 'tp', None), P(('dp', 'tp'), None, None), P('dp'), P('dp'), P('dp', 'tp'), P('dp', 'tp'), P(('dp', 'tp'), None))
    return jax.shard_map(device_step, mesh=mesh, in_specs=in_specs, out_specs=out_specs, check_vma=False)
```
